256 devices in a mesh: gx: 8 (over y, core), gy: 16 (over x_lo, z), gz: 2 (over x_hi).
Axes of the slice: x: 4 (x_hi: 2, x_lo: 2; x = x_hi * 2 + x_lo), y: 4, z: 8, core: 2. Of those that a mesh axis runs over, the one named last changes fastest.
Arguments:
- permittivity: float32 [64, 512, 256], P('gx', 'gy', 'gz'), may hold values from 1 to 9
- loss: float32 [64, 512, 256], P('gx', 'gy', 'gz'), may hold values from 0 to 0.2
- fwd_electric: float32 [3, 64, 512, 256], P(None, 'gx', 'gy', 'gz'), may hold values from -6 to 6
- fwd_magnetic: float32 [3, 64, 512, 256], P(None, 'gx', 'gy', 'gz'), may hold values from -6 to 6
- adj_electric: float32 [3, 64, 512, 256], P(None, 'gx', 'gy', 'gz'), may hold values from -200 to 200
- adj_magnetic: float32 [3, 64, 512, 256], P(None, 'gx', 'gy', 'gz'), may hold values from -200 to 200
- wavelet: float32 [64], replicated, may hold values from -6 to 6
- residuals: float32 [2048, 64], P(('gx', 'gy', 'gz')), may hold values from -24 to 24
- source_cell: int32 [1], replicated, may hold values from 0 to 8388607
- receiver_cells: int32 [2048], replicated, may hold values from 0 to 8388607
- start_step: int32 [1], replicated, may hold values from 0 to 60
Outputs:
- direction: float32 [64, 512, 256], P('gx', 'gy', 'gz')
- grad_rms: float32 [], replicated
The draws below stay inside these ranges and needn't reach their ends.
Inputs may be any that keep to these rules, and one draw needn't show every extreme that they name: source_cell[0] is a flat index of a cell. receiver_cells[r] is the flat index of receiver r's cell; several receivers may share a cell. Samples start_step to start_step + 3 exist in every trace.
All inputs are finite; a program needn't handle non-finite values.
Results may differ from the reference program's by a relative error of at most 0.0003.
Values sent between devices are 32-bit elements; how exact they have to be, the bound alone decides.
A program may use at most 128 MiB of HBM per device.

```python
import math
import jax
import jax.numpy as jnp
from jax import lax

STEPS = 4
TRACE = 64
NREC = 2048
NX = 64
NY = 512
NZ = 256


def adjoint_field(key):
    keys = jax.random.split(key, 4)
    ramp = 3.0 ** (jnp.arange(NX, dtype=jnp.float32) / NX)
    scale_x = ramp
    scale_y = jnp.exp(jax.random.uniform(keys[2], (NY,), jnp.float32, 0.0, math.log(4.0)))
    scale_z = jnp.exp(jax.random.uniform(keys[3], (NZ,), jnp.float32, 0.0, math.log(2.0)))
    base = jnp.clip(jax.random.normal(keys[0], (3, NX, NY, NZ), jnp.float32), -6.0, 6.0)
    return base * scale_x[None, :, None, None] * scale_y[None, None, :, None] * scale_z[None, None, None, :]


def draw_adj_electric(key, part):
    return adjoint_field(jax.random.fold_in(key, 11))


def draw_adj_magnetic(key, part):
    return adjoint_field(jax.random.fold_in(key, 23))


def place_ends(values, rng, low, high):
    longest = values.shape.index(max(values.shape))
    spots = []
    for shift in (0, 1):
        where = [jax.random.randint(jax.random.fold_in(rng, axis), (), 0, length) for axis, length in enumerate(values.shape)]
        where[longest] = (where[longest] + shift) % values.shape[longest]
        spots.append(tuple(where))
    return values.at[spots[0]].set(low).at[spots[1]].set(high)


def levels(stream_key, shape, cuts, low, largest):
    def one(dim, parts):
        steps = jax.random.uniform(jax.random.fold_in(jax.random.fold_in(stream_key, 6), dim), (parts,), jnp.float32, low / len(cuts), largest / len(cuts))
        return jnp.repeat(jnp.exp(steps), shape[dim] // parts).reshape((-1,) + (1,) * (len(shape) - dim - 1))

    gain = one(*cuts[0])
    for cut in cuts[1:]:
        gain = gain * one(*cut)
    return gain


def normal_values(stream_key, dims, spread, limit, shards=(), kind=jnp.bfloat16):
    values = spread * jax.random.normal(stream_key, dims, jnp.float32)
    if shards:
        values = values * levels(stream_key, dims, shards, -0.22, 0.18)
    return jnp.clip(values, -limit, limit).astype(kind)


def setup_inputs(seed: int = 0) -> dict:
    seeds = jax.random.split(jax.random.key(seed), 12)
    return {
        "permittivity": jnp.clip(jnp.exp(math.log(9.0) - 2.1972246 * jax.random.uniform(seeds[0], (NX, NY, NZ), jnp.float32) ** levels(seeds[0], (NX, NY, NZ), ((0, 8), (1, 16), (2, 2)), -0.2, 0.2)), 1.0, 9.0),
        "loss": jnp.clip(0.2 * jax.random.uniform(seeds[1], (NX, NY, NZ), jnp.float32) ** levels(seeds[1], (NX, NY, NZ), ((0, 8), (1, 16), (2, 2)), -0.2, 0.2), 0.0, 0.2),
        "fwd_electric": normal_values(seeds[2], (3, NX, NY, NZ), 1.0, 6.0, ((1, 8), (2, 16), (3, 2)), jnp.float32),
        "fwd_magnetic": normal_values(seeds[3], (3, NX, NY, NZ), 1.0, 6.0, ((1, 8), (2, 16), (3, 2)), jnp.float32),
        "adj_electric": draw_adj_electric(jax.random.fold_in(seeds[11], 71), 0),
        "adj_magnetic": draw_adj_magnetic(jax.random.fold_in(seeds[11], 71), 0),
        "wavelet": normal_values(seeds[6], (TRACE,), 1.0, 6.0, (), jnp.float32),
        "residuals": normal_values(seeds[7], (NREC, TRACE), 4.0, 24.0, ((0, 256),), jnp.float32),
        "source_cell": jax.random.randint(seeds[8], (1,), 0, NX * NY * NZ).astype(jnp.int32),
        "receiver_cells": place_ends(jax.random.randint(seeds[9], (NREC,), 0, NX * NY * NZ), jax.random.fold_in(seeds[9], 1), 0, (NX * NY * NZ) - 1).astype(jnp.int32),
        "start_step": jax.random.randint(seeds[10], (1,), 0, TRACE - STEPS + 1).astype(jnp.int32),
    }


def shifted_above(field, axis):
    rest = lax.slice_in_dim(field, 1, field.shape[axis], axis=axis)
    edge = jnp.zeros_like(lax.slice_in_dim(field, 0, 1, axis=axis))
    return jnp.concatenate([rest, edge], axis)

def shifted_below(field, axis):
    rest = lax.slice_in_dim(field, 0, field.shape[axis] - 1, axis=axis)
    edge = jnp.zeros_like(lax.slice_in_dim(field, 0, 1, axis=axis))
    return jnp.concatenate([edge, rest], axis)

def yee_step(electric, magnetic, keep, curl):
    electric_x, electric_y, electric_z = electric
    magnetic_x, magnetic_y, magnetic_z = magnetic
    magnetic_x = magnetic_x - 0.5 * (shifted_above(electric_z, 1) - electric_z - (shifted_above(electric_y, 2) - electric_y))
    magnetic_y = magnetic_y - 0.5 * (shifted_above(electric_x, 2) - electric_x - (shifted_above(electric_z, 0) - electric_z))
    magnetic_z = magnetic_z - 0.5 * (shifted_above(electric_y, 0) - electric_y - (shifted_above(electric_x, 1) - electric_x))
    electric_x = keep * electric_x + curl * (magnetic_z - shifted_below(magnetic_z, 1) - (magnetic_y - shifted_below(magnetic_y, 2)))
    electric_y = keep * electric_y + curl * (magnetic_x - shifted_below(magnetic_x, 2) - (magnetic_z - shifted_below(magnetic_z, 0)))
    electric_z = keep * electric_z + curl * (magnetic_y - shifted_below(magnetic_y, 0) - (magnetic_x - shifted_below(magnetic_x, 1)))
    return ((electric_x, electric_y, electric_z), (magnetic_x, magnetic_y, magnetic_z))

def split_index(flat):
    first = flat // (NY * NZ)
    second = flat // NZ % NY
    third = flat % NZ
    return (first, second, third)

def reference(permittivity, loss, fwd_electric, fwd_magnetic, adj_electric, adj_magnetic, wavelet, residuals, source_cell, receiver_cells, start_step):
    keep = (1.0 - loss) / (1.0 + loss)
    curl = 0.5 / (permittivity * (1.0 + loss))
    start = start_step[0]
    zero_index = jnp.zeros((), jnp.int32)
    src_i, src_j, src_k = split_index(source_cell[0])
    rec_i, rec_j, rec_k = split_index(receiver_cells)
    electric = (fwd_electric[0], fwd_electric[1], fwd_electric[2])
    magnetic = (fwd_magnetic[0], fwd_magnetic[1], fwd_magnetic[2])
    snapshots = [electric]
    for index in range(STEPS):
        electric, magnetic = yee_step(electric, magnetic, keep, curl)
        sample = lax.dynamic_slice_in_dim(wavelet, start + index, 1)[0]
        electric = (electric[0], electric[1], electric[2].at[src_i, src_j, src_k].add(sample))
        snapshots.append(electric)
    window = lax.dynamic_slice(residuals, (zero_index, start), (residuals.shape[0], STEPS))
    adjoint = (adj_electric[0], adj_electric[1], adj_electric[2])
    adjoint_mag = (adj_magnetic[0], adj_magnetic[1], adj_magnetic[2])
    gradient = jnp.zeros(permittivity.shape, jnp.float32)
    for index in range(STEPS):
        adjoint, adjoint_mag = yee_step(adjoint, adjoint_mag, keep, curl)
        adjoint = (adjoint[0], adjoint[1], adjoint[2].at[rec_i, rec_j, rec_k].add(window[:, STEPS - 1 - index]))
        later = STEPS - index
        change = [snapshots[later][c] - snapshots[later - 1][c] for c in range(3)]
        gradient = gradient + (change[0] * adjoint[0] + change[1] * adjoint[1] + change[2] * adjoint[2])
    gradient = -gradient / permittivity
    grad_rms = jnp.sqrt(jnp.sum(gradient * gradient) / (NX * NY * NZ) + 1e-06)
    return (gradient / grad_rms, grad_rms)
```

```python
import functools

import jax
import jax.numpy as jnp
from jax import lax
from jax.experimental import pallas as pl
from jax.experimental.pallas import tpu as pltpu
from jax.sharding import PartitionSpec as P

STEPS = 4
MESH = pl.DeviceIdType.MESH
F32 = jnp.float32
BF16 = jnp.bfloat16

HALO = 4
OWNX = HALO
OWNY = 16
TOP = 8
ROWS = 48
FIRST = 8
COMPS = 14


def kernel(
    dims,
    perm_hbm,
    loss_hbm,
    fe_hbm,
    fm_hbm,
    ae_hbm,
    am_hbm,
    res_ref,
    cells_ref,
    wave_ref,
    source_ref,
    start_ref,
    out_ref,
    rms_ref,
    field,
    medium,
    ysend,
    yrecv,
    corner,
    pack,
    packedge,
    packrecv,
    packedgerecv,
    slab,
    snaps,
    grad,
    hrow,
    hslab,
    smask,
    sslab,
    onehot,
    inj,
    injslab,
    gather1,
    gather2,
    red1,
    red2,
    load_sem,
    halo_send,
    halo_recv,
    group_send,
    group_recv,
):
    ngx, ngy, ngz, nx, ny, nz, nrec = dims
    gx, gy, gz = lax.axis_index("gx"), lax.axis_index("gy"), lax.axis_index("gz")
    i1 = lax.rem(gy, 8) * 2 + gz
    i2 = gx * 2 + gy // 8
    own = (slice(OWNX, OWNX + nx), slice(OWNY, OWNY + ny))

    loads = []
    for k, (src, dst) in enumerate(
        (
            (perm_hbm, medium.at[0]),
            (loss_hbm, medium.at[1]),
            (fe_hbm, field.at[2:5, own[0], own[1]]),
            (fm_hbm, field.at[5:8, own[0], own[1]]),
            (ae_hbm, field.at[8:11, own[0], own[1]]),
            (am_hbm, field.at[11:14, own[0], own[1]]),
        )
    ):
        copy = pltpu.make_async_copy(src, dst, load_sem.at[k])
        copy.start()
        loads.append(copy)

    def there(dx, dy):
        ok = []
        if dx:
            ok.append((gx + dx >= 0) & (gx + dx < ngx))
        if dy:
            ok.append((gy + dy >= 0) & (gy + dy < ngy))
        if not ok:
            return None
        return functools.reduce(jnp.logical_and, ok)

    def guarded(cond, fn):
        if cond is None:
            fn()
        else:
            pl.when(cond)(fn)

    def clear_planes(low):
        def body(c, _):
            field[c, low : low + HALO, OWNY : OWNY + ny, :] = jnp.zeros((HALO, ny, nz), F32)
            return 0

        lax.fori_loop(0, COMPS, body, 0)

    pl.when(gx == 0)(lambda: clear_planes(0))
    pl.when(gx == ngx - 1)(lambda: clear_planes(OWNX + nx))

    def clear(ref):
        ref[...] = jnp.zeros(ref.shape, F32)

    def clear_loop(ref):
        def body(c, _):
            ref[c] = jnp.zeros(ref.shape[1:], F32)
            return 0

        lax.fori_loop(0, ref.shape[0], body, 0)

    for ys, dy in ((0, -1), (1, 1)):
        missing_y = (gy + dy < 0) | (gy + dy >= ngy)
        pl.when(missing_y)(lambda ys=ys: clear_loop(yrecv.at[ys]))
        for xs, dx in ((0, -1), (1, 1)):
            missing = missing_y | (gx + dx < 0) | (gx + dx >= ngx)
            pl.when(missing)(lambda xs=xs, ys=ys: clear_loop(corner.at[xs, ys]))
        for q, dx in ((0, -1), (1, 0), (2, 1)):
            missing = missing_y | (gx + dx < 0) | (gx + dx >= ngx) if dx else missing_y
            for z in range(2):
                pl.when(missing)(lambda z=z, q=q, ys=ys: clear(packedgerecv.at[z, q, ys]))
    for q, dx in ((0, -1), (2, 1)):
        missing = (gx + dx < 0) | (gx + dx >= ngx)
        for z in range(2):
            pl.when(missing)(lambda z=z, q=q: clear_loop(packrecv.at[z, q]))

    barrier = pltpu.get_barrier_semaphore()
    for dx in (-1, 0, 1):
        for dy in (-1, 0, 1):
            for dz in (0, 1):
                if dx or dy or dz:
                    peer = {"gx": gx + dx, "gy": gy + dy, "gz": gz if dz == 0 else 1 - gz}
                    guarded(
                        there(dx, dy),
                        lambda peer=peer: pl.semaphore_signal(
                            barrier, inc=1, device_id=peer, device_id_type=MESH
                        ),
                    )

    def member1(k):
        return {"gx": gx, "gy": (gy // 8) * 8 + k // 2, "gz": lax.rem(k, 2)}

    def member2(k):
        return {"gx": k // 2, "gy": lax.rem(k, 2) * 8 + lax.rem(gy, 8), "gz": gz}

    groups = ((i1, member1), (i2, member2))
    for mine, member in groups:
        for step in range(1, 16):
            pl.semaphore_signal(
                barrier, inc=1, device_id=member(lax.rem(mine + step, 16)), device_id_type=MESH
            )

    start = start_ref[0]
    lane8 = lax.broadcasted_iota(jnp.int32, (8, 128), 1)
    sub8 = lax.broadcasted_iota(jnp.int32, (8, 128), 0)

    time = lax.broadcasted_iota(jnp.int32, res_ref.shape, 1)
    rows = []
    for m in range(STEPS):
        column = jnp.sum(jnp.where(time == start + m, res_ref[...], 0.0), axis=1, keepdims=True)
        spread = jnp.where(lane8 - i1 * 8 == sub8, jnp.broadcast_to(column, (8, 128)), 0.0)
        rows.append(jnp.sum(spread, axis=0, keepdims=True))
    gather1[i1] = jnp.concatenate(rows, axis=0)

    count_x = 3 - (gx == 0).astype(jnp.int32) - (gx == ngx - 1).astype(jnp.int32)
    count_y = 3 - (gy == 0).astype(jnp.int32) - (gy == ngy - 1).astype(jnp.int32)
    pl.semaphore_wait(barrier, count_x * count_y * 2 - 1 + 30)

    def group_copy(round_, which, ref, step):
        mine, member = groups[which]
        peer = lax.rem(mine + step, 16)
        return pltpu.make_async_remote_copy(
            src_ref=ref.at[mine],
            dst_ref=ref.at[mine],
            send_sem=group_send.at[round_, step - 1],
            recv_sem=group_recv.at[round_, mine],
            device_id=member(peer),
            device_id_type=MESH,
        )

    def group_arrival(round_, which, ref, step):
        mine, member = groups[which]
        peer = lax.rem(mine + step, 16)
        return pltpu.make_async_remote_copy(
            src_ref=ref.at[mine],
            dst_ref=ref.at[peer],
            send_sem=group_send.at[round_, step - 1],
            recv_sem=group_recv.at[round_, peer],
            device_id=member(peer),
            device_id_type=MESH,
        )

    def group_start(round_, which, ref):
        for step in range(1, 16):
            group_copy(round_, which, ref, step).start()

    def group_wait(round_, which, ref):
        for step in range(1, 16):
            group_arrival(round_, which, ref, step).wait_recv()

    def group_drain(round_, which, ref):
        for step in range(1, 16):
            group_copy(round_, which, ref, step).wait_send()

    group_start(0, 0, gather1)

    loads[0].wait()
    loads[1].wait()

    def coefficients(i, _):
        loss = medium[1, i]
        field[0, OWNX + i, OWNY : OWNY + ny, :] = (1.0 - loss) / (1.0 + loss)
        field[1, OWNX + i, OWNY : OWNY + ny, :] = 0.5 / (medium[0, i] * (1.0 + loss))
        return 0

    lax.fori_loop(0, nx, coefficients, 0)
    loads[2].wait()
    loads[3].wait()

    sends = []
    number = [0]

    def remote(src, dst, dx, dy, dz, back):
        k = number[0]
        number[0] += 1

        def make(landing):
            return pltpu.make_async_remote_copy(
                src_ref=src,
                dst_ref=landing,
                send_sem=halo_send.at[k],
                recv_sem=halo_recv.at[k],
                device_id={"gx": gx + dx, "gy": gy + dy, "gz": gz if dz == 0 else 1 - gz},
                device_id_type=MESH,
            )

        guarded(there(dx, dy), lambda: make(dst).start())
        sends.append((there(dx, dy), make(dst)))
        return lambda: guarded(there(-dx, -dy), lambda: make(back).wait_recv())

    def side(d):
        return 0 if d == 1 else 1

    def start_halos(c0, c1):
        waits = []
        for dx in (1, -1):
            source = slice(OWNX + nx - HALO, OWNX + nx) if dx == 1 else slice(OWNX, OWNX + HALO)
            target = slice(0, HALO) if dx == 1 else slice(OWNX + nx, OWNX + nx + HALO)
            landing = field.at[c0:c1, target, OWNY : OWNY + ny]
            waits.append(
                remote(field.at[c0:c1, source, OWNY : OWNY + ny], landing, dx, 0, 0, landing)
            )
            cond, copy = sends.pop()
            waits.append(lambda cond=cond, copy=copy: guarded(cond, copy.wait_send))
        for dy in (1, -1):
            edge = 1 if dy == 1 else 0
            landing = yrecv.at[side(dy), c0:c1]
            waits.append(remote(ysend.at[edge, c0:c1], landing, 0, dy, 0, landing))
            for dx in (1, -1):
                part = slice(nx - HALO, nx) if dx == 1 else slice(0, HALO)
                landing = corner.at[side(dx), side(dy), c0:c1]
                waits.append(remote(ysend.at[edge, c0:c1, part], landing, dx, dy, 0, landing))
        return waits

    def start_slabs():
        waits = []
        for dz in (0, 1):
            for dx in (0, 1, -1):
                for dy in (0, 1, -1):
                    if not (dx or dy or dz):
                        continue
                    z_there = gz
                    z_here = gz if dz == 0 else 1 - gz
                    if dy == 0:
                        waits.append(
                            remote(
                                pack,
                                packrecv.at[z_there, 1 - dx],
                                dx,
                                dy,
                                dz,
                                packrecv.at[z_here, 1 - dx],
                            )
                        )
                    else:
                        edge = 1 if dy == 1 else 0
                        waits.append(
                            remote(
                                packedge.at[edge],
                                packedgerecv.at[z_there, 1 - dx, side(dy)],
                                dx,
                                dy,
                                dz,
                                packedgerecv.at[z_here, 1 - dx, side(dy)],
                            )
                        )
        return waits

    def pack_edges(c0, c1):
        def body(c, _):
            ysend[0, c] = field[c, own[0], OWNY : OWNY + HALO, :]
            ysend[1, c] = field[c, own[0], OWNY + ny - HALO : OWNY + ny, :]
            return 0

        lax.fori_loop(c0, c1, body, 0)

    lane32 = lax.broadcasted_iota(jnp.int32, (ny, 128), 1)
    quad = lane32 // 4
    lift = 4 * (1 - gz)

    def pack_slab(group):
        packed = jnp.zeros((ny, 128), F32)
        for part in range(4):
            comp = group * 4 + part
            if comp >= COMPS:
                continue
            for i in range(nx):
                base = (part // 2) * 64 + i * 8 + (part % 2) * 4
                moved = pltpu.roll(field[comp, OWNX + i, own[1], :], base + lift, axis=1)
                packed = jnp.where(quad == base // 4, moved, packed)
        pack[group] = packed
        packrecv[gz, 1, group] = packed
        packedge[0, group] = packed[0:HALO]
        packedge[1, group] = packed[ny - HALO : ny]

    pack_edges(0, FIRST)
    first_waits = start_halos(0, FIRST)
    loads[4].wait()
    loads[5].wait()
    for group in range(4):
        pack_slab(group)
    slab_waits = start_slabs()
    pack_edges(FIRST, COMPS)
    second_waits = start_halos(FIRST, COMPS)

    row = lax.broadcasted_iota(jnp.int32, (ROWS, 128), 0) + TOP
    lane = lax.broadcasted_iota(jnp.int32, (ROWS, 128), 1)
    row_y = row - OWNY + gy * ny
    hrow[...] = jnp.where(row_y >= 0, 0.5, 0.0)
    slab_x = lane // 8 - OWNX + gx * nx
    hslab[...] = jnp.where((row_y >= 0) & (slab_x >= 0), 0.5, 0.0)
    source = source_ref[0]
    total_y, total_z = ngy * ny, ngz * nz
    src_x = source // (total_y * total_z)
    src_y = lax.rem(source // total_z, total_y)
    src_z = lax.rem(source, total_z)
    in_row = row_y == src_y
    smask[...] = jnp.where(in_row & (lane + gz * nz == src_z), 1.0, 0.0)
    slab_z = lax.rem(lane, 8) + nz - HALO
    sslab[...] = jnp.where(in_row & (slab_x == src_x) & (slab_z == src_z), 1.0, 0.0)
    src_plane = src_x - gx * nx + OWNX

    cells = cells_ref[...]
    rec_x = cells // (total_y * total_z) - gx * nx + OWNX
    rec_y = lax.rem(cells // total_z, total_y) - gy * ny + OWNY - TOP
    rec_z = lax.rem(cells, total_z)
    in_x = (rec_x >= 0) & (rec_x < nx + 2 * HALO)
    in_y = (rec_y >= 0) & (rec_y < ROWS)
    rec_row = jnp.where(in_x & in_y, rec_x * ROWS + rec_y, -1)
    rec_lane = rec_z - gz * nz
    planes = nx + 2 * HALO - 2

    def build(i, _):
        ids = lax.broadcasted_iota(jnp.int32, (ROWS, nrec), 0) + (i + 1) * ROWS
        onehot[pl.ds(pl.multiple_of(i * ROWS, 16), ROWS), :] = jnp.where(ids == rec_row, 1.0, 0.0).astype(BF16)
        return 0

    lax.fori_loop(0, planes, build, 0)

    group_wait(0, 0, gather1)
    row_of_samples = gather1[0]
    for k in range(1, 16):
        row_of_samples = row_of_samples + gather1[k]
    gather2[i2] = row_of_samples
    group_start(1, 1, gather2)

    lane_r = lax.broadcasted_iota(jnp.int32, (ROWS, nz), 1)

    def assemble(c0, c1):
        zeros = jnp.zeros((HALO, nz), F32)

        def body(c, _):
            for i in range(nx + 2 * HALO):
                for ys in range(2):
                    if i < OWNX:
                        piece = corner[0, ys, c, i]
                    elif i < OWNX + nx:
                        piece = yrecv[ys, c, i - OWNX]
                    else:
                        piece = corner[1, ys, c, i - OWNX - nx]
                    if ys == 0:
                        field[c, i, TOP:OWNY, :] = jnp.concatenate([zeros, piece], axis=0)
                    else:
                        field[c, i, OWNY + ny : OWNY + ny + 8, :] = jnp.concatenate([piece, zeros], axis=0)
            return 0

        lax.fori_loop(c0, c1, body, 0)

    lane_p = lax.broadcasted_iota(jnp.int32, (ROWS, 128), 1)

    def assemble_slab(c0, c1):
        zeros = jnp.zeros((HALO, 128), F32)
        for group in range(c0 // 4, (c1 + 3) // 4):
            centre, beside = [], []
            for z in range(2):
                full = []
                for q in range(3):
                    full.append(
                        jnp.concatenate(
                            [
                                zeros,
                                packedgerecv[z, q, 0, group],
                                packrecv[z, q, group],
                                packedgerecv[z, q, 1, group],
                                zeros,
                            ],
                            axis=0,
                        )
                    )
                centre.append(full[1])
                beside.append(jnp.where(lax.rem(lane_p, 64) >= 32, full[0], full[2]))
            for part in range(4):
                comp = group * 4 + part
                if comp >= c1:
                    continue
                base = (part // 2) * 64 + (part % 2) * 4
                inner = [pltpu.roll(centre[z], (32 + 4 * z - base) % 128, axis=1) for z in range(2)]
                outer = [pltpu.roll(beside[z], (96 + 4 * z - base) % 128, axis=1) for z in range(2)]
                deep = lax.rem(lane_p, 8) >= 4
                inside = (lane_p >= 32) & (lane_p < 96)
                slab[comp, TOP : TOP + ROWS, :] = jnp.where(
                    inside, jnp.where(deep, inner[1], inner[0]), jnp.where(deep, outer[1], outer[0])
                )

    up_keep = jnp.where(gz == 0, 1.0, 0.0)
    down_keep = jnp.where(gz == 0, 0.0, 1.0)
    body_rows = slice(TOP, TOP + ROWS)
    rows_up = slice(TOP + 1, TOP + 1 + ROWS)
    rows_down = slice(TOP - 1, TOP - 1 + ROWS)

    def magnetic_half(b, step):
        def body(i, _):
            factor = hrow[...] * jnp.where(gx * nx + i - OWNX >= 0, 1.0, 0.0)
            ex, ey, ez = field[b, i, body_rows], field[b + 1, i, body_rows], field[b + 2, i, body_rows]
            turn = lax.rem(2 * 128 - 1 - HALO - 8 * i, 128)

            def deeper(value, comp):
                edge = pltpu.roll(slab[comp, body_rows], turn, axis=1) * up_keep
                return jnp.where(lane_r == nz - 1, edge, pltpu.roll(value, nz - 1, axis=1))

            field[b + 3, i, body_rows] = field[b + 3, i, body_rows] - factor * (
                (field[b + 2, i, rows_up] - ez) - (deeper(ey, b + 1) - ey)
            )
            field[b + 4, i, body_rows] = field[b + 4, i, body_rows] - factor * (
                (deeper(ex, b) - ex) - (field[b + 2, i + 1, body_rows] - ez)
            )
            field[b + 5, i, body_rows] = field[b + 5, i, body_rows] - factor * (
                (field[b + 1, i + 1, body_rows] - ey) - (field[b, i, rows_up] - ex)
            )
            return 0

        lax.fori_loop(step - 1, nx + 2 * HALO - step, body, 0)
        factor = hslab[...]
        ex, ey, ez = slab[b, body_rows], slab[b + 1, body_rows], slab[b + 2, body_rows]

        def along_x(value):
            return pltpu.roll(value, 120, axis=1)

        def along_z(value):
            return pltpu.roll(value, 127, axis=1)

        slab[b + 3, body_rows] = slab[b + 3, body_rows] - factor * (
            (slab[b + 2, rows_up] - ez) - (along_z(ey) - ey)
        )
        slab[b + 4, body_rows] = slab[b + 4, body_rows] - factor * (
            (along_z(ex) - ex) - (along_x(ez) - ez)
        )
        slab[b + 5, body_rows] = slab[b + 5, body_rows] - factor * (
            (along_x(ey) - ey) - (slab[b, rows_up] - ex)
        )

    def electric_half(b, step, extra, extra_slab):
        def body(i, _):
            keep, curl = field[0, i, body_rows], field[1, i, body_rows]
            hx, hy, hz = field[b + 3, i, body_rows], field[b + 4, i, body_rows], field[b + 5, i, body_rows]
            turn = lax.rem(2 * 128 - (HALO - 1) - 8 * i, 128)

            def shallower(value, comp):
                edge = pltpu.roll(slab[comp, body_rows], turn, axis=1) * down_keep
                return jnp.where(lane_r == 0, edge, pltpu.roll(value, 1, axis=1))

            field[b, i, body_rows] = keep * field[b, i, body_rows] + curl * (
                (hz - field[b + 5, i, rows_down]) - (hy - shallower(hy, b + 4))
            )
            field[b + 1, i, body_rows] = keep * field[b + 1, i, body_rows] + curl * (
                (hx - shallower(hx, b + 3)) - (hz - field[b + 5, i - 1, body_rows])
            )
            field[b + 2, i, body_rows] = (
                keep * field[b + 2, i, body_rows]
                + curl * ((hy - field[b + 4, i - 1, body_rows]) - (hx - field[b + 3, i, rows_down]))
                + extra(i)
            )
            return 0

        lax.fori_loop(step, nx + 2 * HALO - step, body, 0)
        if step == STEPS:
            return
        keep, curl = slab[0, body_rows], slab[1, body_rows]
        hx, hy, hz = slab[b + 3, body_rows], slab[b + 4, body_rows], slab[b + 5, body_rows]

        def along_x(value):
            return pltpu.roll(value, 8, axis=1)

        def along_z(value):
            return pltpu.roll(value, 1, axis=1)

        slab[b, body_rows] = keep * slab[b, body_rows] + curl * (
            (hz - slab[b + 5, rows_down]) - (hy - along_z(hy))
        )
        slab[b + 1, body_rows] = keep * slab[b + 1, body_rows] + curl * (
            (hx - along_z(hx)) - (hz - along_x(hz))
        )
        slab[b + 2, body_rows] = (
            keep * slab[b + 2, body_rows]
            + curl * ((hy - along_x(hy)) - (hx - slab[b + 3, rows_down]))
            + extra_slab()
        )

    def snapshot(n):
        def body(i, _):
            for c in range(3):
                snaps[n, c, i] = field[2 + c, OWNX + i, own[1], :]
            return 0

        lax.fori_loop(0, nx, body, 0)

    for wait in first_waits:
        wait()
    for wait in slab_waits:
        wait()
    snapshot(0)
    assemble(0, FIRST)
    assemble_slab(0, FIRST)
    for step in range(1, STEPS + 1):
        pulse = wave_ref[start + step - 1]
        magnetic_half(2, step)
        electric_half(
            2,
            step,
            lambda i: smask[...] * jnp.where(i == src_plane, pulse, 0.0),
            lambda: sslab[...] * pulse,
        )
        snapshot(step)

    group_wait(1, 1, gather2)
    samples = [
        jnp.concatenate([gather2[k][m : m + 1] for k in range(16)], axis=1) for m in range(STEPS)
    ]

    def split(value):
        high = value.astype(BF16).astype(F32)
        return high, value - high

    contract = (((1,), (1,)), ((), ()))
    lanes_of = lax.broadcasted_iota(jnp.int32, (nz, nrec), 0)
    at_lane = lanes_of == rec_lane
    for m in range(STEPS):
        high, low = split(samples[STEPS - 1 - m])
        weights = jnp.concatenate(
            [jnp.where(at_lane, high, 0.0).astype(BF16), jnp.where(at_lane, low, 0.0).astype(BF16)],
            axis=0,
        )
        count = planes - 2 * m
        both = lax.dot_general(
            onehot[m * ROWS : (m + count) * ROWS, :], weights, contract, preferred_element_type=F32
        )
        inj[m, 1 + m : 1 + m + count] = (both[:, :nz] + both[:, nz:]).reshape(count, ROWS, nz)
    rec_near = rec_x * 8 + rec_z - (nz - HALO)
    in_slab = in_x & (rec_z >= nz - HALO) & (rec_z < nz + HALO)
    slab_weights = jnp.where(lanes_of == jnp.where(in_slab, rec_near, -1), 1.0, 0.0).astype(BF16)
    at_row = lax.broadcasted_iota(jnp.int32, (ROWS, nrec), 0) == rec_y
    pieces = []
    for m in range(STEPS - 1):
        for value in split(samples[STEPS - 1 - m]):
            pieces.append(jnp.where(at_row, value, 0.0).astype(BF16))
    both = lax.dot_general(
        jnp.concatenate(pieces, axis=0), slab_weights, contract, preferred_element_type=F32
    )
    for m in range(STEPS - 1):
        at = 2 * m * ROWS
        injslab[m] = both[at : at + ROWS] + both[at + ROWS : at + 2 * ROWS]

    for wait in second_waits:
        wait()
    assemble(FIRST, COMPS)
    assemble_slab(FIRST, COMPS)
    for step in range(1, STEPS + 1):
        magnetic_half(8, step)
        electric_half(
            8, step, lambda i, m=step - 1: inj[m, i], lambda m=step - 1: injslab[m]
        )
        later = STEPS + 1 - step

        def correlate(i, square, step=step, later=later):
            term = None
            for c in range(3):
                change = snaps[later, c, i] - snaps[later - 1, c, i]
                product = change * field[8 + c, OWNX + i, own[1], :]
                term = product if term is None else term + product
            value = term if step == 1 else grad[i] + term
            if step == STEPS:
                value = -value / medium[0, i]
                square = square + value * value
            grad[i] = value
            return square

        square = lax.fori_loop(0, nx, correlate, jnp.zeros((ny, nz), F32))

    red1[i1] = jnp.sum(square, axis=0, keepdims=True)
    group_start(2, 0, red1)
    group_wait(2, 0, red1)
    total = red1[0]
    for k in range(1, 16):
        total = total + red1[k]
    red2[i2] = total
    group_start(3, 1, red2)
    group_wait(3, 1, red2)
    total = red2[0]
    for k in range(1, 16):
        total = total + red2[k]
    total = jnp.sum(total, axis=1, keepdims=True)
    cells_in_all = ngx * nx * ngy * ny * ngz * nz
    rms = jnp.sqrt(total / cells_in_all + 1e-06)
    rms_ref[...] = rms
    wide = jnp.broadcast_to(rms, (ny, nz))

    def scale(i, _):
        out_ref[i] = grad[i] / wide
        return 0

    lax.fori_loop(0, nx, scale, 0)
    for cond, copy in sends:
        guarded(cond, copy.wait_send)
    group_drain(0, 0, gather1)
    group_drain(1, 1, gather2)
    group_drain(2, 0, red1)
    group_drain(3, 1, red2)


def solution(mesh):
    ngx, ngy, ngz = mesh.shape["gx"], mesh.shape["gy"], mesh.shape["gz"]

    def per_device(
        permittivity,
        loss,
        fwd_electric,
        fwd_magnetic,
        adj_electric,
        adj_magnetic,
        wavelet,
        residuals,
        source_cell,
        receiver_cells,
        start_step,
    ):
        nx, ny, nz = permittivity.shape
        nrec = receiver_cells.shape[0]
        planes = nx + 2 * HALO
        dims = (ngx, ngy, ngz, nx, ny, nz, nrec)
        hbm = pl.BlockSpec(memory_space=pl.ANY)
        vmem = pl.BlockSpec(memory_space=pltpu.VMEM)
        smem = pl.BlockSpec(memory_space=pltpu.SMEM)
        direction, rms = pl.pallas_call(
            functools.partial(kernel, dims),
            out_shape=(
                jax.ShapeDtypeStruct((nx, ny, nz), F32),
                jax.ShapeDtypeStruct((1, 1), F32),
            ),
            in_specs=[hbm] * 6 + [vmem] * 2 + [smem] * 3,
            out_specs=(vmem, vmem),
            scratch_shapes=[
                pltpu.VMEM((COMPS, planes, 64, nz), F32),
                pltpu.VMEM((2, nx, ny, nz), F32),
                pltpu.VMEM((2, COMPS, nx, HALO, nz), F32),
                pltpu.VMEM((2, COMPS, nx, HALO, nz), F32),
                pltpu.VMEM((2, 2, COMPS, HALO, HALO, nz), F32),
                pltpu.VMEM((4, ny, 128), F32),
                pltpu.VMEM((2, 4, HALO, 128), F32),
                pltpu.VMEM((2, 3, 4, ny, 128), F32),
                pltpu.VMEM((2, 3, 2, 4, HALO, 128), F32),
                pltpu.VMEM((COMPS, 64, 128), F32),
                pltpu.VMEM((STEPS + 1, 3, nx, ny, nz), F32),
                pltpu.VMEM((nx, ny, nz), F32),
                pltpu.VMEM((ROWS, 128), F32),
                pltpu.VMEM((ROWS, 128), F32),
                pltpu.VMEM((ROWS, 128), F32),
                pltpu.VMEM((ROWS, 128), F32),
                pltpu.VMEM(((planes - 2) * ROWS, nrec), BF16),
                pltpu.VMEM((STEPS, planes, ROWS, nz), F32),
                pltpu.VMEM((STEPS - 1, ROWS, 128), F32),
                pltpu.VMEM((16, STEPS, 128), F32),
                pltpu.VMEM((16, STEPS, 128), F32),
                pltpu.VMEM((16, 1, 128), F32),
                pltpu.VMEM((16, 1, 128), F32),
                pltpu.SemaphoreType.DMA((6,)),
                pltpu.SemaphoreType.DMA((33,)),
                pltpu.SemaphoreType.DMA((33,)),
                pltpu.SemaphoreType.DMA((4, 15)),
                pltpu.SemaphoreType.DMA((4, 16)),
            ],
            compiler_params=pltpu.CompilerParams(
                collective_id=0, has_side_effects=True, vmem_limit_bytes=60 * 1024 * 1024
            ),
            name="window",
        )(
            permittivity,
            loss,
            fwd_electric,
            fwd_magnetic,
            adj_electric,
            adj_magnetic,
            residuals,
            receiver_cells.reshape(1, nrec),
            wavelet,
            source_cell,
            start_step,
        )
        return direction, rms.reshape(())

    field_spec = P(None, "gx", "gy", "gz")
    block_spec = P("gx", "gy", "gz")
    return jax.shard_map(
        per_device,
        mesh=mesh,
        in_specs=(
            block_spec,
            block_spec,
            field_spec,
            field_spec,
            field_spec,
            field_spec,
            P(),
            P(("gx", "gy", "gz"), None),
            P(),
            P(),
            P(),
        ),
        out_specs=(block_spec, P()),
        check_vma=False,
    )
```

```python
import functools

import jax
import jax.numpy as jnp
from jax import lax
from jax.experimental import pallas as pl
from jax.experimental.pallas import tpu as pltpu
from jax.sharding import PartitionSpec as P

STEPS = 4
MESH = pl.DeviceIdType.MESH
F32 = jnp.float32
BF16 = jnp.bfloat16

HALO = 4
OWNX = HALO
OWNY = 16
TOP = 8
ROWS = 48
FIRST = 8
COMPS = 14
GROUP = 16


def kernel(
    dims,
    perm_hbm,
    loss_hbm,
    fe_hbm,
    fm_hbm,
    ae_hbm,
    am_hbm,
    res_ref,
    cells_ref,
    wave_ref,
    source_ref,
    start_ref,
    out_ref,
    rms_ref,
    field,
    medium,
    ysend,
    yrecv,
    corner,
    pack,
    packedge,
    packrecv,
    packedgerecv,
    slab,
    snaps,
    grad,
    hrow,
    hslab,
    smask,
    sslab,
    onehot,
    inj,
    injslab,
    gather1,
    gather2,
    red1,
    red2,
    load_sem,
    halo_send,
    halo_recv,
    group_send,
    group_recv,
):
    ngx, ngy, ngz, nx, ny, nz, nrec = dims
    gx, gy, gz = lax.axis_index("gx"), lax.axis_index("gy"), lax.axis_index("gz")
    i1 = lax.rem(gy, 8) * 2 + gz
    i2 = gx * 2 + gy // 8
    own = (slice(OWNX, OWNX + nx), slice(OWNY, OWNY + ny))

    loads = []
    for k, (src, dst) in enumerate(
        (
            (perm_hbm, medium.at[0]),
            (loss_hbm, medium.at[1]),
            (fe_hbm, field.at[2:5, own[0], own[1]]),
            (fm_hbm, field.at[5:8, own[0], own[1]]),
            (ae_hbm, field.at[8:11, own[0], own[1]]),
            (am_hbm, field.at[11:14, own[0], own[1]]),
        )
    ):
        copy = pltpu.make_async_copy(src, dst, load_sem.at[k])
        copy.start()
        loads.append(copy)

    def there(dx, dy):
        ok = []
        if dx:
            ok.append((gx + dx >= 0) & (gx + dx < ngx))
        if dy:
            ok.append((gy + dy >= 0) & (gy + dy < ngy))
        if not ok:
            return None
        return functools.reduce(jnp.logical_and, ok)

    def guarded(cond, fn):
        if cond is None:
            fn()
        else:
            pl.when(cond)(fn)

    def clear_planes(low):
        def body(c, _):
            field[c, low : low + HALO, OWNY : OWNY + ny, :] = jnp.zeros((HALO, ny, nz), F32)
            return 0

        lax.fori_loop(0, COMPS, body, 0)

    pl.when(gx == 0)(lambda: clear_planes(0))
    pl.when(gx == ngx - 1)(lambda: clear_planes(OWNX + nx))

    def clear(ref):
        ref[...] = jnp.zeros(ref.shape, F32)

    def clear_loop(ref):
        def body(c, _):
            ref[c] = jnp.zeros(ref.shape[1:], F32)
            return 0

        lax.fori_loop(0, ref.shape[0], body, 0)

    for ys, dy in ((0, -1), (1, 1)):
        missing_y = (gy + dy < 0) | (gy + dy >= ngy)
        pl.when(missing_y)(lambda ys=ys: clear_loop(yrecv.at[ys]))
        for xs, dx in ((0, -1), (1, 1)):
            missing = missing_y | (gx + dx < 0) | (gx + dx >= ngx)
            pl.when(missing)(lambda xs=xs, ys=ys: clear_loop(corner.at[xs, ys]))
        for q, dx in ((0, -1), (1, 0), (2, 1)):
            missing = missing_y | (gx + dx < 0) | (gx + dx >= ngx) if dx else missing_y
            for z in range(2):
                pl.when(missing)(lambda z=z, q=q, ys=ys: clear(packedgerecv.at[z, q, ys]))
    for q, dx in ((0, -1), (2, 1)):
        missing = (gx + dx < 0) | (gx + dx >= ngx)
        for z in range(2):
            pl.when(missing)(lambda z=z, q=q: clear_loop(packrecv.at[z, q]))

    barrier = pltpu.get_barrier_semaphore()
    for dx in (-1, 0, 1):
        for dy in (-1, 0, 1):
            for dz in (0, 1):
                if dx or dy or dz:
                    peer = {"gx": gx + dx, "gy": gy + dy, "gz": gz if dz == 0 else 1 - gz}
                    guarded(
                        there(dx, dy),
                        lambda peer=peer: pl.semaphore_signal(
                            barrier, inc=1, device_id=peer, device_id_type=MESH
                        ),
                    )

    def member1(k):
        return {"gx": gx, "gy": (gy // 8) * 8 + k // 2, "gz": lax.rem(k, 2)}

    def member2(k):
        return {"gx": k // 2, "gy": lax.rem(k, 2) * 8 + lax.rem(gy, 8), "gz": gz}

    groups = ((i1, member1), (i2, member2))
    for mine, member in groups:
        for step in range(1, 16):
            pl.semaphore_signal(
                barrier, inc=1, device_id=member(lax.rem(mine + step, 16)), device_id_type=MESH
            )

    start = start_ref[0]
    lane8 = lax.broadcasted_iota(jnp.int32, (8, 128), 1)
    sub8 = lax.broadcasted_iota(jnp.int32, (8, 128), 0)

    time = lax.broadcasted_iota(jnp.int32, res_ref.shape, 1)
    rows = []
    for m in range(STEPS):
        column = jnp.sum(jnp.where(time == start + m, res_ref[...], 0.0), axis=1, keepdims=True)
        spread = jnp.where(lane8 - i1 * 8 == sub8, jnp.broadcast_to(column, (8, 128)), 0.0)
        rows.append(jnp.sum(spread, axis=0, keepdims=True))
    gather1[i1] = jnp.concatenate(rows, axis=0)

    count_x = 3 - (gx == 0).astype(jnp.int32) - (gx == ngx - 1).astype(jnp.int32)
    count_y = 3 - (gy == 0).astype(jnp.int32) - (gy == ngy - 1).astype(jnp.int32)
    pl.semaphore_wait(barrier, count_x * count_y * 2 - 1 + 30)

    def group_copy(round_, which, ref, step):
        mine, member = groups[which]
        peer = lax.rem(mine + step, 16)
        return pltpu.make_async_remote_copy(
            src_ref=ref.at[mine],
            dst_ref=ref.at[mine],
            send_sem=group_send.at[round_, step - 1],
            recv_sem=group_recv.at[round_, mine],
            device_id=member(peer),
            device_id_type=MESH,
        )

    def group_arrival(round_, which, ref, step):
        mine, member = groups[which]
        peer = lax.rem(mine + step, 16)
        return pltpu.make_async_remote_copy(
            src_ref=ref.at[mine],
            dst_ref=ref.at[peer],
            send_sem=group_send.at[round_, step - 1],
            recv_sem=group_recv.at[round_, peer],
            device_id=member(peer),
            device_id_type=MESH,
        )

    def group_start(round_, which, ref):
        for step in range(1, 16):
            group_copy(round_, which, ref, step).start()

    def group_wait(round_, which, ref):
        for step in range(1, 16):
            group_arrival(round_, which, ref, step).wait_recv()

    def group_drain(round_, which, ref):
        for step in range(1, 16):
            group_copy(round_, which, ref, step).wait_send()

    group_start(0, 0, gather1)

    loads[0].wait()
    loads[1].wait()

    def coefficients(i, _):
        loss = medium[1, i]
        field[0, OWNX + i, OWNY : OWNY + ny, :] = (1.0 - loss) / (1.0 + loss)
        field[1, OWNX + i, OWNY : OWNY + ny, :] = 0.5 / (medium[0, i] * (1.0 + loss))
        return 0

    lax.fori_loop(0, nx, coefficients, 0)
    loads[2].wait()
    loads[3].wait()

    sends = []
    number = [0]

    def remote(src, dst, dx, dy, dz, back):
        k = number[0]
        number[0] += 1

        def make(landing):
            return pltpu.make_async_remote_copy(
                src_ref=src,
                dst_ref=landing,
                send_sem=halo_send.at[k],
                recv_sem=halo_recv.at[k],
                device_id={"gx": gx + dx, "gy": gy + dy, "gz": gz if dz == 0 else 1 - gz},
                device_id_type=MESH,
            )

        guarded(there(dx, dy), lambda: make(dst).start())
        sends.append((there(dx, dy), make(dst)))
        return lambda: guarded(there(-dx, -dy), lambda: make(back).wait_recv())

    def side(d):
        return 0 if d == 1 else 1

    def start_halos(c0, c1):
        waits = []
        for dx in (1, -1):
            source = slice(OWNX + nx - HALO, OWNX + nx) if dx == 1 else slice(OWNX, OWNX + HALO)
            target = slice(0, HALO) if dx == 1 else slice(OWNX + nx, OWNX + nx + HALO)
            landing = field.at[c0:c1, target, OWNY : OWNY + ny]
            waits.append(
                remote(field.at[c0:c1, source, OWNY : OWNY + ny], landing, dx, 0, 0, landing)
            )
            cond, copy = sends.pop()
            waits.append(lambda cond=cond, copy=copy: guarded(cond, copy.wait_send))
        for dy in (1, -1):
            edge = 1 if dy == 1 else 0
            landing = yrecv.at[side(dy), c0:c1]
            waits.append(remote(ysend.at[edge, c0:c1], landing, 0, dy, 0, landing))
            for dx in (1, -1):
                part = slice(nx - HALO, nx) if dx == 1 else slice(0, HALO)
                landing = corner.at[side(dx), side(dy), c0:c1]
                waits.append(remote(ysend.at[edge, c0:c1, part], landing, dx, dy, 0, landing))
        return waits

    def start_slabs():
        waits = []
        for dz in (0, 1):
            for dx in (0, 1, -1):
                for dy in (0, 1, -1):
                    if not (dx or dy or dz):
                        continue
                    z_there = gz
                    z_here = gz if dz == 0 else 1 - gz
                    if dy == 0:
                        waits.append(
                            remote(
                                pack,
                                packrecv.at[z_there, 1 - dx],
                                dx,
                                dy,
                                dz,
                                packrecv.at[z_here, 1 - dx],
                            )
                        )
                    else:
                        edge = 1 if dy == 1 else 0
                        waits.append(
                            remote(
                                packedge.at[edge],
                                packedgerecv.at[z_there, 1 - dx, side(dy)],
                                dx,
                                dy,
                                dz,
                                packedgerecv.at[z_here, 1 - dx, side(dy)],
                            )
                        )
        return waits

    def pack_edges(c0, c1):
        def body(c, _):
            ysend[0, c] = field[c, own[0], OWNY : OWNY + HALO, :]
            ysend[1, c] = field[c, own[0], OWNY + ny - HALO : OWNY + ny, :]
            return 0

        lax.fori_loop(c0, c1, body, 0)

    lane32 = lax.broadcasted_iota(jnp.int32, (ny, 128), 1)
    quad = lane32 // 4
    lift = 4 * (1 - gz)

    def pack_slab(group):
        packed = jnp.zeros((ny, 128), F32)
        for part in range(4):
            comp = group * 4 + part
            if comp >= COMPS:
                continue
            for i in range(nx):
                base = (part // 2) * 64 + i * 8 + (part % 2) * 4
                moved = pltpu.roll(field[comp, OWNX + i, own[1], :], base + lift, axis=1)
                packed = jnp.where(quad == base // 4, moved, packed)
        pack[group] = packed
        packrecv[gz, 1, group] = packed
        packedge[0, group] = packed[0:HALO]
        packedge[1, group] = packed[ny - HALO : ny]

    pack_edges(0, FIRST)
    first_waits = start_halos(0, FIRST)
    loads[4].wait()
    loads[5].wait()
    for group in range(4):
        pack_slab(group)
    slab_waits = start_slabs()
    pack_edges(FIRST, COMPS)
    second_waits = start_halos(FIRST, COMPS)

    row = lax.broadcasted_iota(jnp.int32, (ROWS, 128), 0) + TOP
    lane = lax.broadcasted_iota(jnp.int32, (ROWS, 128), 1)
    row_y = row - OWNY + gy * ny
    hrow[...] = jnp.where(row_y >= 0, 0.5, 0.0)
    slab_x = lane // 8 - OWNX + gx * nx
    hslab[...] = jnp.where((row_y >= 0) & (slab_x >= 0), 0.5, 0.0)
    source = source_ref[0]
    total_y, total_z = ngy * ny, ngz * nz
    src_x = source // (total_y * total_z)
    src_y = lax.rem(source // total_z, total_y)
    src_z = lax.rem(source, total_z)
    in_row = row_y == src_y
    smask[...] = jnp.where(in_row & (lane + gz * nz == src_z), 1.0, 0.0)
    slab_z = lax.rem(lane, 8) + nz - HALO
    sslab[...] = jnp.where(in_row & (slab_x == src_x) & (slab_z == src_z), 1.0, 0.0)
    src_plane = src_x - gx * nx + OWNX

    cells = cells_ref[...]
    rec_x = cells // (total_y * total_z) - gx * nx + OWNX
    rec_y = lax.rem(cells // total_z, total_y) - gy * ny + OWNY - TOP
    rec_z = lax.rem(cells, total_z)
    in_x = (rec_x >= 0) & (rec_x < nx + 2 * HALO)
    in_y = (rec_y >= 0) & (rec_y < ROWS)
    rec_row = jnp.where(in_x & in_y, rec_x * ROWS + rec_y, -1)
    rec_lane = rec_z - gz * nz
    planes = nx + 2 * HALO - 2

    def build(i, _):
        ids = lax.broadcasted_iota(jnp.int32, (ROWS, nrec), 0) + (i + 1) * ROWS
        onehot[pl.ds(pl.multiple_of(i * ROWS, 16), ROWS), :] = jnp.where(ids == rec_row, 1.0, 0.0).astype(BF16)
        return 0

    lax.fori_loop(0, planes, build, 0)

    group_wait(0, 0, gather1)
    row_of_samples = gather1[0]
    for k in range(1, 16):
        row_of_samples = row_of_samples + gather1[k]
    gather2[i2] = row_of_samples
    group_start(1, 1, gather2)

    lane_r = lax.broadcasted_iota(jnp.int32, (ROWS, nz), 1)

    def assemble(c0, c1):
        zeros = jnp.zeros((HALO, nz), F32)

        def body(c, _):
            for i in range(nx + 2 * HALO):
                for ys in range(2):
                    if i < OWNX:
                        piece = corner[0, ys, c, i]
                    elif i < OWNX + nx:
                        piece = yrecv[ys, c, i - OWNX]
                    else:
                        piece = corner[1, ys, c, i - OWNX - nx]
                    if ys == 0:
                        field[c, i, TOP:OWNY, :] = jnp.concatenate([zeros, piece], axis=0)
                    else:
                        field[c, i, OWNY + ny : OWNY + ny + 8, :] = jnp.concatenate([piece, zeros], axis=0)
            return 0

        lax.fori_loop(c0, c1, body, 0)

    lane_p = lax.broadcasted_iota(jnp.int32, (ROWS, 128), 1)

    def assemble_slab(c0, c1):
        zeros = jnp.zeros((HALO, 128), F32)
        for group in range(c0 // 4, (c1 + 3) // 4):
            centre, beside = [], []
            for z in range(2):
                full = []
                for q in range(3):
                    full.append(
                        jnp.concatenate(
                            [
                                zeros,
                                packedgerecv[z, q, 0, group],
                                packrecv[z, q, group],
                                packedgerecv[z, q, 1, group],
                                zeros,
                            ],
                            axis=0,
                        )
                    )
                centre.append(full[1])
                beside.append(jnp.where(lax.rem(lane_p, 64) >= 32, full[0], full[2]))
            for part in range(4):
                comp = group * 4 + part
                if comp >= c1:
                    continue
                base = (part // 2) * 64 + (part % 2) * 4
                inner = [pltpu.roll(centre[z], (32 + 4 * z - base) % 128, axis=1) for z in range(2)]
                outer = [pltpu.roll(beside[z], (96 + 4 * z - base) % 128, axis=1) for z in range(2)]
                deep = lax.rem(lane_p, 8) >= 4
                inside = (lane_p >= 32) & (lane_p < 96)
                slab[comp, TOP : TOP + ROWS, :] = jnp.where(
                    inside, jnp.where(deep, inner[1], inner[0]), jnp.where(deep, outer[1], outer[0])
                )

    up_keep = jnp.where(gz == 0, 1.0, 0.0)
    down_keep = jnp.where(gz == 0, 0.0, 1.0)
    body_rows = slice(TOP, TOP + ROWS)
    rows_up = slice(TOP + 1, TOP + 1 + ROWS)
    rows_down = slice(TOP - 1, TOP - 1 + ROWS)

    def over_planes(low, high, body):
        count = (high - low) // GROUP

        def several(k, _):
            for j in range(GROUP):
                body(low + k * GROUP + j, 0)
            return 0

        if count:
            lax.fori_loop(0, count, several, 0)
        for i in range(low + count * GROUP, high):
            body(i, 0)

    def magnetic_half(b, step):
        def body(i, _):
            factor = hrow[...] * jnp.where(gx * nx + i - OWNX >= 0, 1.0, 0.0)
            ex, ey, ez = field[b, i, body_rows], field[b + 1, i, body_rows], field[b + 2, i, body_rows]
            turn = lax.rem(2 * 128 - 1 - HALO - 8 * i, 128)

            def deeper(value, comp):
                edge = pltpu.roll(slab[comp, body_rows], turn, axis=1) * up_keep
                return jnp.where(lane_r == nz - 1, edge, pltpu.roll(value, nz - 1, axis=1))

            field[b + 3, i, body_rows] = field[b + 3, i, body_rows] - factor * (
                (field[b + 2, i, rows_up] - ez) - (deeper(ey, b + 1) - ey)
            )
            field[b + 4, i, body_rows] = field[b + 4, i, body_rows] - factor * (
                (deeper(ex, b) - ex) - (field[b + 2, i + 1, body_rows] - ez)
            )
            field[b + 5, i, body_rows] = field[b + 5, i, body_rows] - factor * (
                (field[b + 1, i + 1, body_rows] - ey) - (field[b, i, rows_up] - ex)
            )
            return 0

        over_planes(step - 1, nx + 2 * HALO - step, body)
        factor = hslab[...]
        ex, ey, ez = slab[b, body_rows], slab[b + 1, body_rows], slab[b + 2, body_rows]

        def along_x(value):
            return pltpu.roll(value, 120, axis=1)

        def along_z(value):
            return pltpu.roll(value, 127, axis=1)

        slab[b + 3, body_rows] = slab[b + 3, body_rows] - factor * (
            (slab[b + 2, rows_up] - ez) - (along_z(ey) - ey)
        )
        slab[b + 4, body_rows] = slab[b + 4, body_rows] - factor * (
            (along_z(ex) - ex) - (along_x(ez) - ez)
        )
        slab[b + 5, body_rows] = slab[b + 5, body_rows] - factor * (
            (along_x(ey) - ey) - (slab[b, rows_up] - ex)
        )

    def electric_half(b, step, extra, extra_slab):
        def body(i, _):
            keep, curl = field[0, i, body_rows], field[1, i, body_rows]
            hx, hy, hz = field[b + 3, i, body_rows], field[b + 4, i, body_rows], field[b + 5, i, body_rows]
            turn = lax.rem(2 * 128 - (HALO - 1) - 8 * i, 128)

            def shallower(value, comp):
                edge = pltpu.roll(slab[comp, body_rows], turn, axis=1) * down_keep
                return jnp.where(lane_r == 0, edge, pltpu.roll(value, 1, axis=1))

            field[b, i, body_rows] = keep * field[b, i, body_rows] + curl * (
                (hz - field[b + 5, i, rows_down]) - (hy - shallower(hy, b + 4))
            )
            field[b + 1, i, body_rows] = keep * field[b + 1, i, body_rows] + curl * (
                (hx - shallower(hx, b + 3)) - (hz - field[b + 5, i - 1, body_rows])
            )
            field[b + 2, i, body_rows] = (
                keep * field[b + 2, i, body_rows]
                + curl * ((hy - field[b + 4, i - 1, body_rows]) - (hx - field[b + 3, i, rows_down]))
                + extra(i)
            )
            return 0

        over_planes(step, nx + 2 * HALO - step, body)
        if step == STEPS:
            return
        keep, curl = slab[0, body_rows], slab[1, body_rows]
        hx, hy, hz = slab[b + 3, body_rows], slab[b + 4, body_rows], slab[b + 5, body_rows]

        def along_x(value):
            return pltpu.roll(value, 8, axis=1)

        def along_z(value):
            return pltpu.roll(value, 1, axis=1)

        slab[b, body_rows] = keep * slab[b, body_rows] + curl * (
            (hz - slab[b + 5, rows_down]) - (hy - along_z(hy))
        )
        slab[b + 1, body_rows] = keep * slab[b + 1, body_rows] + curl * (
            (hx - along_z(hx)) - (hz - along_x(hz))
        )
        slab[b + 2, body_rows] = (
            keep * slab[b + 2, body_rows]
            + curl * ((hy - along_x(hy)) - (hx - slab[b + 3, rows_down]))
            + extra_slab()
        )

    def snapshot(n):
        def body(i, _):
            for c in range(3):
                snaps[n, c, i] = field[2 + c, OWNX + i, own[1], :]
            return 0

        lax.fori_loop(0, nx, body, 0)

    for wait in first_waits:
        wait()
    for wait in slab_waits:
        wait()
    snapshot(0)
    assemble(0, FIRST)
    assemble_slab(0, FIRST)
    for step in range(1, STEPS + 1):
        pulse = wave_ref[start + step - 1]
        magnetic_half(2, step)
        electric_half(
            2,
            step,
            lambda i: smask[...] * jnp.where(i == src_plane, pulse, 0.0),
            lambda: sslab[...] * pulse,
        )
        snapshot(step)

    group_wait(1, 1, gather2)
    samples = [
        jnp.concatenate([gather2[k][m : m + 1] for k in range(16)], axis=1) for m in range(STEPS)
    ]

    def split(value):
        high = value.astype(BF16).astype(F32)
        return high, value - high

    contract = (((1,), (1,)), ((), ()))
    lanes_of = lax.broadcasted_iota(jnp.int32, (nz, nrec), 0)
    at_lane = lanes_of == rec_lane
    for m in range(STEPS):
        high, low = split(samples[STEPS - 1 - m])
        weights = jnp.concatenate(
            [jnp.where(at_lane, high, 0.0).astype(BF16), jnp.where(at_lane, low, 0.0).astype(BF16)],
            axis=0,
        )
        count = planes - 2 * m
        both = lax.dot_general(
            onehot[m * ROWS : (m + count) * ROWS, :], weights, contract, preferred_element_type=F32
        )
        inj[m, 1 + m : 1 + m + count] = (both[:, :nz] + both[:, nz:]).reshape(count, ROWS, nz)
    rec_near = rec_x * 8 + rec_z - (nz - HALO)
    in_slab = in_x & (rec_z >= nz - HALO) & (rec_z < nz + HALO)
    slab_weights = jnp.where(lanes_of == jnp.where(in_slab, rec_near, -1), 1.0, 0.0).astype(BF16)
    at_row = lax.broadcasted_iota(jnp.int32, (ROWS, nrec), 0) == rec_y
    pieces = []
    for m in range(STEPS - 1):
        for value in split(samples[STEPS - 1 - m]):
            pieces.append(jnp.where(at_row, value, 0.0).astype(BF16))
    both = lax.dot_general(
        jnp.concatenate(pieces, axis=0), slab_weights, contract, preferred_element_type=F32
    )
    for m in range(STEPS - 1):
        at = 2 * m * ROWS
        injslab[m] = both[at : at + ROWS] + both[at + ROWS : at + 2 * ROWS]

    for wait in second_waits:
        wait()
    assemble(FIRST, COMPS)
    assemble_slab(FIRST, COMPS)
    for step in range(1, STEPS + 1):
        magnetic_half(8, step)
        electric_half(
            8, step, lambda i, m=step - 1: inj[m, i], lambda m=step - 1: injslab[m]
        )
        later = STEPS + 1 - step

        def correlate(i, square, step=step, later=later):
            term = None
            for c in range(3):
                change = snaps[later, c, i] - snaps[later - 1, c, i]
                product = change * field[8 + c, OWNX + i, own[1], :]
                term = product if term is None else term + product
            value = term if step == 1 else grad[i] + term
            if step == STEPS:
                value = -value / medium[0, i]
                square = square + value * value
            grad[i] = value
            return square

        square = lax.fori_loop(0, nx, correlate, jnp.zeros((ny, nz), F32))

    red1[i1] = jnp.sum(square, axis=0, keepdims=True)
    group_start(2, 0, red1)
    group_wait(2, 0, red1)
    total = red1[0]
    for k in range(1, 16):
        total = total + red1[k]
    red2[i2] = total
    group_start(3, 1, red2)
    group_wait(3, 1, red2)
    total = red2[0]
    for k in range(1, 16):
        total = total + red2[k]
    total = jnp.sum(total, axis=1, keepdims=True)
    cells_in_all = ngx * nx * ngy * ny * ngz * nz
    rms = jnp.sqrt(total / cells_in_all + 1e-06)
    rms_ref[...] = rms
    wide = jnp.broadcast_to(rms, (ny, nz))

    def scale(i, _):
        out_ref[i] = grad[i] / wide
        return 0

    lax.fori_loop(0, nx, scale, 0)
    for cond, copy in sends:
        guarded(cond, copy.wait_send)
    group_drain(0, 0, gather1)
    group_drain(1, 1, gather2)
    group_drain(2, 0, red1)
    group_drain(3, 1, red2)


def solution(mesh):
    ngx, ngy, ngz = mesh.shape["gx"], mesh.shape["gy"], mesh.shape["gz"]

    def per_device(
        permittivity,
        loss,
        fwd_electric,
        fwd_magnetic,
        adj_electric,
        adj_magnetic,
        wavelet,
        residuals,
        source_cell,
        receiver_cells,
        start_step,
    ):
        nx, ny, nz = permittivity.shape
        nrec = receiver_cells.shape[0]
        planes = nx + 2 * HALO
        dims = (ngx, ngy, ngz, nx, ny, nz, nrec)
        hbm = pl.BlockSpec(memory_space=pl.ANY)
        vmem = pl.BlockSpec(memory_space=pltpu.VMEM)
        smem = pl.BlockSpec(memory_space=pltpu.SMEM)
        direction, rms = pl.pallas_call(
            functools.partial(kernel, dims),
            out_shape=(
                jax.ShapeDtypeStruct((nx, ny, nz), F32),
                jax.ShapeDtypeStruct((1, 1), F32),
            ),
            in_specs=[hbm] * 6 + [vmem] * 2 + [smem] * 3,
            out_specs=(vmem, vmem),
            scratch_shapes=[
                pltpu.VMEM((COMPS, planes, 64, nz), F32),
                pltpu.VMEM((2, nx, ny, nz), F32),
                pltpu.VMEM((2, COMPS, nx, HALO, nz), F32),
                pltpu.VMEM((2, COMPS, nx, HALO, nz), F32),
                pltpu.VMEM((2, 2, COMPS, HALO, HALO, nz), F32),
                pltpu.VMEM((4, ny, 128), F32),
                pltpu.VMEM((2, 4, HALO, 128), F32),
                pltpu.VMEM((2, 3, 4, ny, 128), F32),
                pltpu.VMEM((2, 3, 2, 4, HALO, 128), F32),
                pltpu.VMEM((COMPS, 64, 128), F32),
                pltpu.VMEM((STEPS + 1, 3, nx, ny, nz), F32),
                pltpu.VMEM((nx, ny, nz), F32),
                pltpu.VMEM((ROWS, 128), F32),
                pltpu.VMEM((ROWS, 128), F32),
                pltpu.VMEM((ROWS, 128), F32),
                pltpu.VMEM((ROWS, 128), F32),
                pltpu.VMEM(((planes - 2) * ROWS, nrec), BF16),
                pltpu.VMEM((STEPS, planes, ROWS, nz), F32),
                pltpu.VMEM((STEPS - 1, ROWS, 128), F32),
                pltpu.VMEM((16, STEPS, 128), F32),
                pltpu.VMEM((16, STEPS, 128), F32),
                pltpu.VMEM((16, 1, 128), F32),
                pltpu.VMEM((16, 1, 128), F32),
                pltpu.SemaphoreType.DMA((6,)),
                pltpu.SemaphoreType.DMA((33,)),
                pltpu.SemaphoreType.DMA((33,)),
                pltpu.SemaphoreType.DMA((4, 15)),
                pltpu.SemaphoreType.DMA((4, 16)),
            ],
            compiler_params=pltpu.CompilerParams(
                collective_id=0, has_side_effects=True, vmem_limit_bytes=60 * 1024 * 1024
            ),
            name="window",
        )(
            permittivity,
            loss,
            fwd_electric,
            fwd_magnetic,
            adj_electric,
            adj_magnetic,
            residuals,
            receiver_cells.reshape(1, nrec),
            wavelet,
            source_cell,
            start_step,
        )
        return direction, rms.reshape(())

    field_spec = P(None, "gx", "gy", "gz")
    block_spec = P("gx", "gy", "gz")
    return jax.shard_map(
        per_device,
        mesh=mesh,
        in_specs=(
            block_spec,
            block_spec,
            field_spec,
            field_spec,
            field_spec,
            field_spec,
            P(),
            P(("gx", "gy", "gz"), None),
            P(),
            P(),
            P(),
        ),
        out_specs=(block_spec, P()),
        check_vma=False,
    )
```

```python
import functools

import jax
import jax.numpy as jnp
from jax import lax
from jax.experimental import pallas as pl
from jax.experimental.pallas import tpu as pltpu
from jax.sharding import PartitionSpec as P

STEPS = 4
MESH = pl.DeviceIdType.MESH
F32 = jnp.float32
BF16 = jnp.bfloat16

HALO = 4
OWNX = HALO
OWNY = 16
TOP = 8
ROWS = 48
KEEP, CURL = 6, 7
FIRST = 8
COMPS = 14


def kernel(
    dims,
    perm_hbm,
    loss_hbm,
    fe_hbm,
    fm_hbm,
    ae_hbm,
    am_hbm,
    res_hbm,
    cells_hbm,
    wave_hbm,
    source_hbm,
    start_hbm,
    out_ref,
    rms_ref,
    field,
    medium,
    ysend,
    yrecv,
    corner,
    res_ref,
    cells_ref,
    wave_ref,
    source_ref,
    start_ref,
    pack,
    packedge,
    packx,
    packxedge,
    packrecv,
    packedgerecv,
    packxrecv,
    packxedgerecv,
    slab,
    snaps,
    change,
    hrow,
    hslab,
    smask,
    sslab,
    onehot,
    inj,
    injslab,
    gather1,
    gather2,
    red1,
    red2,
    load_sem,
    halo_send,
    halo_recv,
    group_send,
    group_recv,
):
    ngx, ngy, ngz, nx, ny, nz, nrec = dims
    gx, gy, gz = lax.axis_index("gx"), lax.axis_index("gy"), lax.axis_index("gz")
    i1 = lax.rem(gy, 8) * 2 + gz
    i2 = gx * 2 + gy // 8
    own = (slice(OWNX, OWNX + nx), slice(OWNY, OWNY + ny))

    loads = {}
    for k, (name, src, dst) in enumerate(
        (
            ("fe", fe_hbm, field.at[0:3, own[0], own[1]]),
            ("fm", fm_hbm, field.at[3:6, own[0], own[1]]),
            ("perm", perm_hbm, medium.at[0]),
            ("loss", loss_hbm, medium.at[1]),
            ("start", start_hbm, start_ref),
            ("res", res_hbm, res_ref),
            ("ae", ae_hbm, field.at[8:11, own[0], own[1]]),
            ("am", am_hbm, field.at[11:14, own[0], own[1]]),
            ("source", source_hbm, source_ref),
            ("wave", wave_hbm, wave_ref),
            ("cells", cells_hbm, cells_ref),
        )
    ):
        loads[name] = pltpu.make_async_copy(src, dst, load_sem.at[k])
        loads[name].start()

    def there(dx, dy):
        ok = []
        if dx:
            ok.append((gx + dx >= 0) & (gx + dx < ngx))
        if dy:
            ok.append((gy + dy >= 0) & (gy + dy < ngy))
        if not ok:
            return None
        return functools.reduce(jnp.logical_and, ok)

    def guarded(cond, fn):
        if cond is None:
            fn()
        else:
            pl.when(cond)(fn)

    def clear_planes(low):
        def body(c, _):
            field[c, low : low + HALO, OWNY : OWNY + ny, :] = jnp.zeros((HALO, ny, nz), F32)
            return 0

        lax.fori_loop(0, COMPS, body, 0)

    pl.when(gx == 0)(lambda: clear_planes(0))
    pl.when(gx == ngx - 1)(lambda: clear_planes(OWNX + nx))

    def clear(ref):
        ref[...] = jnp.zeros(ref.shape, F32)

    def clear_loop(ref):
        def body(c, _):
            ref[c] = jnp.zeros(ref.shape[1:], F32)
            return 0

        lax.fori_loop(0, ref.shape[0], body, 0)

    for ys, dy in ((0, -1), (1, 1)):
        missing_y = (gy + dy < 0) | (gy + dy >= ngy)
        pl.when(missing_y)(lambda ys=ys: clear_loop(yrecv.at[ys]))
        for xs, dx in ((0, -1), (1, 1)):
            missing = missing_y | (gx + dx < 0) | (gx + dx >= ngx)
            pl.when(missing)(lambda xs=xs, ys=ys: clear_loop(corner.at[xs, ys]))
        for z in range(2):
            pl.when(missing_y)(lambda z=z, ys=ys: clear(packedgerecv.at[z, ys]))
            for xs, dx in ((0, -1), (1, 1)):
                missing = missing_y | (gx + dx < 0) | (gx + dx >= ngx)
                pl.when(missing)(lambda z=z, xs=xs, ys=ys: clear(packxedgerecv.at[z, xs, ys]))
    for xs, dx in ((0, -1), (1, 1)):
        missing = (gx + dx < 0) | (gx + dx >= ngx)
        for z in range(2):
            pl.when(missing)(lambda z=z, xs=xs: clear(packxrecv.at[z, xs]))

    barrier = pltpu.get_barrier_semaphore()
    for dx in (-1, 0, 1):
        for dy in (-1, 0, 1):
            for dz in (0, 1):
                if dx or dy or dz:
                    peer = {"gx": gx + dx, "gy": gy + dy, "gz": gz if dz == 0 else 1 - gz}
                    guarded(
                        there(dx, dy),
                        lambda peer=peer: pl.semaphore_signal(
                            barrier, inc=1, device_id=peer, device_id_type=MESH
                        ),
                    )

    def member1(k):
        return {"gx": gx, "gy": (gy // 8) * 8 + k // 2, "gz": lax.rem(k, 2)}

    def member2(k):
        return {"gx": k // 2, "gy": lax.rem(k, 2) * 8 + lax.rem(gy, 8), "gz": gz}

    groups = ((i1, member1), (i2, member2))
    for mine, member in groups:
        for step in range(1, 16):
            pl.semaphore_signal(
                barrier, inc=1, device_id=member(lax.rem(mine + step, 16)), device_id_type=MESH
            )

    loads["start"].wait()
    loads["res"].wait()
    start = start_ref[0]
    lane8 = lax.broadcasted_iota(jnp.int32, (8, 128), 1)
    sub8 = lax.broadcasted_iota(jnp.int32, (8, 128), 0)

    time = lax.broadcasted_iota(jnp.int32, res_ref.shape, 1)
    rows = []
    for m in range(STEPS):
        column = jnp.sum(jnp.where(time == start + m, res_ref[...], 0.0), axis=1, keepdims=True)
        spread = jnp.where(lane8 - i1 * 8 == sub8, jnp.broadcast_to(column, (8, 128)), 0.0)
        rows.append(jnp.sum(spread, axis=0, keepdims=True))
    gather1[i1] = jnp.concatenate(rows, axis=0)

    def group_copy(round_, which, ref, step):
        mine, member = groups[which]
        peer = lax.rem(mine + step, 16)
        return pltpu.make_async_remote_copy(
            src_ref=ref.at[mine],
            dst_ref=ref.at[mine],
            send_sem=group_send.at[round_, step - 1],
            recv_sem=group_recv.at[round_, mine],
            device_id=member(peer),
            device_id_type=MESH,
        )

    def group_arrival(round_, which, ref, step):
        mine, member = groups[which]
        peer = lax.rem(mine + step, 16)
        return pltpu.make_async_remote_copy(
            src_ref=ref.at[mine],
            dst_ref=ref.at[peer],
            send_sem=group_send.at[round_, step - 1],
            recv_sem=group_recv.at[round_, peer],
            device_id=member(peer),
            device_id_type=MESH,
        )

    def group_start(round_, which, ref):
        for step in range(1, 16):
            group_copy(round_, which, ref, step).start()

    def group_wait(round_, which, ref):
        for step in range(1, 16):
            group_arrival(round_, which, ref, step).wait_recv()

    def group_drain(round_, which, ref):
        for step in range(1, 16):
            group_copy(round_, which, ref, step).wait_send()

    sends = []
    number = [0]

    def remote(src, dst, dx, dy, dz, back):
        k = number[0]
        number[0] += 1

        def make(landing):
            return pltpu.make_async_remote_copy(
                src_ref=src,
                dst_ref=landing,
                send_sem=halo_send.at[k],
                recv_sem=halo_recv.at[k],
                device_id={"gx": gx + dx, "gy": gy + dy, "gz": gz if dz == 0 else 1 - gz},
                device_id_type=MESH,
            )

        guarded(there(dx, dy), lambda: make(dst).start())
        sends.append((there(dx, dy), make(dst)))
        return lambda: guarded(there(-dx, -dy), lambda: make(back).wait_recv())

    def side(d):
        return 0 if d == 1 else 1

    def span(low, count):
        return slice(low, low + count)

    def start_halos(c0, c1, low_parts, high_parts):
        waits, leaving = [], []
        rows_ = slice(OWNY, OWNY + ny)
        for dx, parts in ((1, low_parts), (-1, high_parts)):
            for first, last, depth in parts:
                if dx == 1:
                    source, target = span(OWNX + nx - depth, depth), span(HALO - depth, depth)
                else:
                    source, target = span(OWNX, depth), span(OWNX + nx, depth)
                landing = field.at[first:last, target, rows_]
                waits.append(remote(field.at[first:last, source, rows_], landing, dx, 0, 0, landing))
                cond, copy = sends.pop()
                leaving.append(lambda cond=cond, copy=copy: guarded(cond, copy.wait_send))
        for dy in (1, -1):
            edge = 1 if dy == 1 else 0
            landing = yrecv.at[side(dy), c0:c1]
            waits.append(remote(ysend.at[edge, c0:c1], landing, 0, dy, 0, landing))
            for dx in (1, -1):
                depth = HALO - 1 if dx == dy else HALO
                part = span(nx - depth, depth) if dx == 1 else span(0, depth)
                place = span(HALO - depth, depth) if dx == 1 else span(0, depth)
                landing = corner.at[side(dx), side(dy), c0:c1, place]
                waits.append(remote(ysend.at[edge, c0:c1, part], landing, dx, dy, 0, landing))
        return waits, leaving

    def start_slabs(chunk):
        waits = []
        groups_ = slice(2 * chunk, 2 * chunk + 2)
        for dz in (1, 0):
            there_z, here_z = gz, (gz if dz == 0 else 1 - gz)
            for dx in (0, 1, -1):
                for dy in (0, 1, -1):
                    if not (dx or dy or dz):
                        continue
                    edge = 1 if dy == 1 else 0
                    if dx == 0 and dy == 0:
                        src, land = pack.at[groups_], lambda z: packrecv.at[z, groups_]
                    elif dx == 0:
                        src = packedge.at[edge, groups_]
                        land = lambda z, dy=dy: packedgerecv.at[z, side(dy), groups_]
                    elif dy == 0:
                        src = packx.at[side(dx), chunk]
                        land = lambda z, dx=dx: packxrecv.at[z, side(dx), chunk]
                    else:
                        src = packxedge.at[side(dx), edge, chunk]
                        land = lambda z, dx=dx, dy=dy: packxedgerecv.at[z, side(dx), side(dy), chunk]
                    waits.append(remote(src, land(there_z), dx, dy, dz, land(here_z)))
        return waits

    def pack_edges(c0, c1):
        for c in range(c0, c1):
            ysend[0, c] = field[c, own[0], OWNY : OWNY + HALO, :]
            ysend[1, c] = field[c, own[0], OWNY + ny - HALO : OWNY + ny, :]

    lane32 = lax.broadcasted_iota(jnp.int32, (ny, 128), 1)
    quad = lane32 // 4
    upper32 = lax.rem(lane32, 64) >= 32
    lift = 4 * (1 - gz)

    def pack_slab(chunk):
        both = []
        for group in (2 * chunk, 2 * chunk + 1):
            packed = jnp.zeros((ny, 128), F32)
            for part in range(4):
                comp = group * 4 + part
                if comp >= COMPS:
                    continue
                for i in range(nx):
                    base = (part // 2) * 64 + i * 8 + (part % 2) * 4
                    moved = pltpu.roll(field[comp, OWNX + i, own[1], :], base + lift, axis=1)
                    packed = jnp.where(quad == base // 4, moved, packed)
            pack[group] = packed
            packrecv[gz, group] = packed
            packedge[0, group] = packed[0:HALO]
            packedge[1, group] = packed[ny - HALO : ny]
            both.append(packed)
        high = jnp.where(upper32, both[0], pltpu.roll(both[1], 96, axis=1))
        low = jnp.where(upper32, pltpu.roll(both[1], 32, axis=1), both[0])
        for k, value in ((0, high), (1, low)):
            packx[k, chunk] = value
            packxedge[k, 0, chunk] = value[0:HALO]
            packxedge[k, 1, chunk] = value[ny - HALO : ny]

    loads["perm"].wait()
    loads["loss"].wait()
    for i in range(nx):
        loss = medium[1, i]
        field[KEEP, OWNX + i, OWNY : OWNY + ny, :] = (1.0 - loss) / (1.0 + loss)
        field[CURL, OWNX + i, OWNY : OWNY + ny, :] = 0.5 / (medium[0, i] * (1.0 + loss))
    loads["fe"].wait()
    loads["fm"].wait()
    pack_slab(0)
    pack_edges(0, FIRST)
    count_x = 3 - (gx == 0).astype(jnp.int32) - (gx == ngx - 1).astype(jnp.int32)
    count_y = 3 - (gy == 0).astype(jnp.int32) - (gy == ngy - 1).astype(jnp.int32)
    pl.semaphore_wait(barrier, count_x * count_y * 2 - 1 + 30)
    group_start(0, 0, gather1)
    slab_waits = start_slabs(0)
    first_waits, first_leaving = start_halos(
        0, FIRST, ((0, 6, HALO), (KEEP, CURL + 1, HALO - 1)), ((0, 3, HALO), (3, FIRST, HALO - 1))
    )
    loads["ae"].wait()
    loads["am"].wait()
    pack_slab(1)
    pack_edges(FIRST, COMPS)
    loads["source"].wait()
    loads["wave"].wait()
    loads["cells"].wait()
    row = lax.broadcasted_iota(jnp.int32, (ROWS, 128), 0) + TOP
    lane = lax.broadcasted_iota(jnp.int32, (ROWS, 128), 1)
    row_y = row - OWNY + gy * ny
    hrow[...] = jnp.where(row_y >= 0, 0.5, 0.0)
    slab_x = lane // 8 - OWNX + gx * nx
    hslab[...] = jnp.where((row_y >= 0) & (slab_x >= 0), 0.5, 0.0)
    source = source_ref[0]
    total_y, total_z = ngy * ny, ngz * nz
    src_x = source // (total_y * total_z)
    src_y = lax.rem(source // total_z, total_y)
    src_z = lax.rem(source, total_z)
    in_row = row_y == src_y
    smask[...] = jnp.where(in_row & (lane + gz * nz == src_z), 1.0, 0.0)
    slab_z = lax.rem(lane, 8) + nz - HALO
    sslab[...] = jnp.where(in_row & (slab_x == src_x) & (slab_z == src_z), 1.0, 0.0)
    src_plane = src_x - gx * nx + OWNX

    cells = cells_ref[...]
    rec_x = cells // (total_y * total_z) - gx * nx + OWNX
    rec_y = lax.rem(cells // total_z, total_y) - gy * ny + OWNY - TOP
    rec_z = lax.rem(cells, total_z)
    in_x = (rec_x >= 0) & (rec_x < nx + 2 * HALO)
    in_y = (rec_y >= 0) & (rec_y < ROWS)
    rec_row = jnp.where(in_x & in_y, rec_x * ROWS + rec_y, -1)
    rec_lane = rec_z - gz * nz
    planes = nx + 2 * HALO - 2

    def build(i, _):
        ids = lax.broadcasted_iota(jnp.int32, (ROWS, nrec), 0) + (i + 1) * ROWS
        onehot[pl.ds(pl.multiple_of(i * ROWS, 16), ROWS), :] = jnp.where(ids == rec_row, 1.0, 0.0).astype(BF16)
        return 0

    lax.fori_loop(0, planes, build, 0)

    group_wait(0, 0, gather1)
    row_of_samples = gather1[0]
    for k in range(1, 16):
        row_of_samples = row_of_samples + gather1[k]
    gather2[i2] = row_of_samples
    group_start(1, 1, gather2)
    second_slab_waits = start_slabs(1)
    second_waits, second_leaving = start_halos(
        FIRST, COMPS, ((FIRST, COMPS, HALO),), ((8, 11, HALO), (11, COMPS, HALO - 1))
    )

    lane_r = lax.broadcasted_iota(jnp.int32, (ROWS, nz), 1)

    def assemble(c0, c1):
        zeros = jnp.zeros((HALO, nz), F32)
        for c in range(c0, c1):
            for i in range(nx + 2 * HALO):
                for ys in range(2):
                    if i < OWNX:
                        piece = corner[0, ys, c, i]
                    elif i < OWNX + nx:
                        piece = yrecv[ys, c, i - OWNX]
                    else:
                        piece = corner[1, ys, c, i - OWNX - nx]
                    if ys == 0:
                        field[c, i, TOP:OWNY, :] = jnp.concatenate([zeros, piece], axis=0)
                    else:
                        field[c, i, OWNY + ny : OWNY + ny + 8, :] = jnp.concatenate([piece, zeros], axis=0)

    lane_p = lax.broadcasted_iota(jnp.int32, (ROWS, 128), 1)
    deep = lax.rem(lane_p, 8) >= 4
    inside = (lane_p >= 32) & (lane_p < 96)
    upper = lax.rem(lane_p, 64) >= 32

    def assemble_slab(chunk):
        zeros = jnp.zeros((HALO, 128), F32)

        def column(low, middle, high):
            return jnp.concatenate([zeros, low, middle, high, zeros], axis=0)

        sides = [
            [
                column(
                    packxedgerecv[z, k, 0, chunk], packxrecv[z, k, chunk], packxedgerecv[z, k, 1, chunk]
                )
                for k in range(2)
            ]
            for z in range(2)
        ]
        for odd in range(2):
            group = 2 * chunk + odd
            centre, beside = [], []
            for z in range(2):
                centre.append(
                    column(packedgerecv[z, 0, group], packrecv[z, group], packedgerecv[z, 1, group])
                )
                low, high = sides[z]
                if odd:
                    low, high = pltpu.roll(low, 32, axis=1), pltpu.roll(high, 96, axis=1)
                beside.append(jnp.where(upper, low, high))
            for part in range(4):
                comp = group * 4 + part
                if comp >= COMPS:
                    continue
                base = (part // 2) * 64 + (part % 2) * 4
                inner = [pltpu.roll(centre[z], (32 + 4 * z - base) % 128, axis=1) for z in range(2)]
                outer = [pltpu.roll(beside[z], (96 + 4 * z - base) % 128, axis=1) for z in range(2)]
                slab[comp, TOP : TOP + ROWS, :] = jnp.where(
                    inside, jnp.where(deep, inner[1], inner[0]), jnp.where(deep, outer[1], outer[0])
                )

    up_keep = jnp.where(gz == 0, 1.0, 0.0)
    down_keep = jnp.where(gz == 0, 0.0, 1.0)
    def moved(window, by):
        return slice(window.start + by, window.stop + by)

    def magnetic_half(b, step):
        at = slice(TOP, TOP + ROWS) if step < STEPS else slice(TOP, OWNY + ny)
        mask_at = moved(at, -TOP)
        tall = at.stop - at.start
        last_lane = lax.broadcasted_iota(jnp.int32, (tall, nz), 1) == nz - 1
        for i in range(step - 1, nx + 2 * HALO - step):
            factor = hrow[mask_at] * jnp.where(gx * nx + i - OWNX >= 0, 1.0, 0.0)
            ex, ey, ez = field[b, i, at], field[b + 1, i, at], field[b + 2, i, at]
            turn = (nz - 1 - HALO - 8 * i) % 128

            def deeper(value, comp):
                edge = pltpu.roll(slab[comp, at], turn, axis=1) * up_keep
                return jnp.where(last_lane, edge, pltpu.roll(value, nz - 1, axis=1))

            field[b + 3, i, at] = field[b + 3, i, at] - factor * (
                (field[b + 2, i, moved(at, 1)] - ez) - (deeper(ey, b + 1) - ey)
            )
            field[b + 4, i, at] = field[b + 4, i, at] - factor * (
                (deeper(ex, b) - ex) - (field[b + 2, i + 1, at] - ez)
            )
            field[b + 5, i, at] = field[b + 5, i, at] - factor * (
                (field[b + 1, i + 1, at] - ey) - (field[b, i, moved(at, 1)] - ex)
            )
        factor = hslab[mask_at]
        ex, ey, ez = slab[b, at], slab[b + 1, at], slab[b + 2, at]

        def along_x(value):
            return pltpu.roll(value, 120, axis=1)

        def along_z(value):
            return pltpu.roll(value, 127, axis=1)

        slab[b + 3, at] = slab[b + 3, at] - factor * (
            (slab[b + 2, moved(at, 1)] - ez) - (along_z(ey) - ey)
        )
        slab[b + 4, at] = slab[b + 4, at] - factor * ((along_z(ex) - ex) - (along_x(ez) - ez))
        if step < STEPS:
            slab[b + 5, at] = slab[b + 5, at] - factor * (
                (along_x(ey) - ey) - (slab[b, moved(at, 1)] - ex)
            )

    def electric_half(b, step, extra, extra_slab):
        at = slice(TOP, TOP + ROWS) if step < STEPS else own[1]
        tall = at.stop - at.start
        first_lane = lax.broadcasted_iota(jnp.int32, (tall, nz), 1) == 0
        for i in range(step, nx + 2 * HALO - step):
            keep, curl = field[KEEP, i, at], field[CURL, i, at]
            hx, hy, hz = field[b + 3, i, at], field[b + 4, i, at], field[b + 5, i, at]
            turn = (1 - HALO - 8 * i) % 128

            def shallower(value, comp):
                edge = pltpu.roll(slab[comp, at], turn, axis=1) * down_keep
                return jnp.where(first_lane, edge, pltpu.roll(value, 1, axis=1))

            field[b, i, at] = keep * field[b, i, at] + curl * (
                (hz - field[b + 5, i, moved(at, -1)]) - (hy - shallower(hy, b + 4))
            )
            field[b + 1, i, at] = keep * field[b + 1, i, at] + curl * (
                (hx - shallower(hx, b + 3)) - (hz - field[b + 5, i - 1, at])
            )
            field[b + 2, i, at] = (
                keep * field[b + 2, i, at]
                + curl * ((hy - field[b + 4, i - 1, at]) - (hx - field[b + 3, i, moved(at, -1)]))
                + extra(i, moved(at, -TOP))
            )
        if step == STEPS:
            return
        keep, curl = slab[KEEP, at], slab[CURL, at]
        hx, hy, hz = slab[b + 3, at], slab[b + 4, at], slab[b + 5, at]

        def along_x(value):
            return pltpu.roll(value, 8, axis=1)

        def along_z(value):
            return pltpu.roll(value, 1, axis=1)

        slab[b, at] = keep * slab[b, at] + curl * ((hz - slab[b + 5, moved(at, -1)]) - (hy - along_z(hy)))
        slab[b + 1, at] = keep * slab[b + 1, at] + curl * ((hx - along_z(hx)) - (hz - along_x(hz)))
        slab[b + 2, at] = (
            keep * slab[b + 2, at]
            + curl * ((hy - along_x(hy)) - (hx - slab[b + 3, moved(at, -1)]))
            + extra_slab()
        )

    def snapshot(n):
        for c in range(3):
            for i in range(nx):
                value = field[c, OWNX + i, own[1], :]
                if n < STEPS:
                    snaps[n, c, i] = value
                if n:
                    change[n - 1, c, i] = value - snaps[n - 1, c, i]

    for wait in first_waits + slab_waits + first_leaving:
        wait()
    snapshot(0)
    assemble(0, FIRST)
    assemble_slab(0)

    def pulse(step):
        return wave_ref[start + step - 1]

    def forward_electric(step):
        electric_half(
            0,
            step,
            lambda i, at: smask[at] * jnp.where(i == src_plane, pulse(step), 0.0),
            lambda: sslab[...] * pulse(step),
        )
        snapshot(step)

    def split(value):
        high = value.astype(BF16).astype(F32)
        return high, value - high

    contract = (((1,), (1,)), ((), ()))

    def inject(m):
        high, low = split(samples[STEPS - 1 - m])
        weights = jnp.concatenate(
            [jnp.where(at_lane, high, 0.0).astype(BF16), jnp.where(at_lane, low, 0.0).astype(BF16)],
            axis=0,
        )
        count = planes - 2 * m
        both = lax.dot_general(
            onehot[m * ROWS : (m + count) * ROWS, :], weights, contract, preferred_element_type=F32
        )
        inj[m, 1 + m : 1 + m + count] = (both[:, :nz] + both[:, nz:]).reshape(count, ROWS, nz)

    def inject_slab():
        rec_near = rec_x * 8 + rec_z - (nz - HALO)
        in_slab = in_x & (rec_z >= nz - HALO) & (rec_z < nz + HALO)
        slab_weights = jnp.where(lanes_of == jnp.where(in_slab, rec_near, -1), 1.0, 0.0).astype(BF16)
        at_row = lax.broadcasted_iota(jnp.int32, (ROWS, nrec), 0) == rec_y
        pieces = []
        for m in range(STEPS - 1):
            for value in split(samples[STEPS - 1 - m]):
                pieces.append(jnp.where(at_row, value, 0.0).astype(BF16))
        both = lax.dot_general(
            jnp.concatenate(pieces, axis=0), slab_weights, contract, preferred_element_type=F32
        )
        for m in range(STEPS - 1):
            at = 2 * m * ROWS
            injslab[m] = both[at : at + ROWS] + both[at + ROWS : at + 2 * ROWS]

    for step in (1, 2):
        magnetic_half(0, step)
        forward_electric(step)
    group_wait(1, 1, gather2)
    samples = [
        jnp.concatenate([gather2[k][m : m + 1] for k in range(16)], axis=1) for m in range(STEPS)
    ]
    lanes_of = lax.broadcasted_iota(jnp.int32, (nz, nrec), 0)
    at_lane = lanes_of == rec_lane
    inject(0)
    magnetic_half(0, 3)
    inject(1)
    forward_electric(3)
    inject(2)
    magnetic_half(0, 4)
    inject(3)
    inject_slab()
    forward_electric(4)

    for wait in second_waits + second_slab_waits + second_leaving:
        wait()
    assemble(FIRST, COMPS)
    assemble_slab(1)
    for step in range(1, STEPS + 1):
        magnetic_half(FIRST, step)
        electric_half(
            FIRST,
            step,
            lambda i, at, m=step - 1: inj[m, i, at],
            lambda m=step - 1: injslab[m],
        )
        square = jnp.zeros((ny, nz), F32)
        for i in range(nx):
            term = None
            for c in range(3):
                product = change[STEPS - step, c, i] * field[FIRST + c, OWNX + i, own[1], :]
                term = product if term is None else term + product
            value = term if step == 1 else out_ref[i] + term
            if step == STEPS:
                value = -value / medium[0, i]
                square = square + value * value
            out_ref[i] = value
    red1[i1] = jnp.sum(square, axis=0, keepdims=True)
    group_start(2, 0, red1)
    group_wait(2, 0, red1)
    total = red1[0]
    for k in range(1, 16):
        total = total + red1[k]
    red2[i2] = total
    group_start(3, 1, red2)
    group_wait(3, 1, red2)
    total = red2[0]
    for k in range(1, 16):
        total = total + red2[k]
    total = jnp.sum(total, axis=1, keepdims=True)
    cells_in_all = ngx * nx * ngy * ny * ngz * nz
    rms = jnp.sqrt(total / cells_in_all + 1e-06)
    rms_ref[...] = rms
    for cond, copy in sends:
        guarded(cond, copy.wait_send)
    group_drain(0, 0, gather1)
    group_drain(1, 1, gather2)
    group_drain(2, 0, red1)
    group_drain(3, 1, red2)


def solution(mesh):
    ngx, ngy, ngz = mesh.shape["gx"], mesh.shape["gy"], mesh.shape["gz"]

    def per_device(
        permittivity,
        loss,
        fwd_electric,
        fwd_magnetic,
        adj_electric,
        adj_magnetic,
        wavelet,
        residuals,
        source_cell,
        receiver_cells,
        start_step,
    ):
        nx, ny, nz = permittivity.shape
        nrec, trace = receiver_cells.shape[0], residuals.shape[1]
        planes = nx + 2 * HALO
        dims = (ngx, ngy, ngz, nx, ny, nz, nrec)
        hbm = pl.BlockSpec(memory_space=pltpu.HBM)
        vmem = pl.BlockSpec(memory_space=pltpu.VMEM)
        gradient, rms = pl.pallas_call(
            functools.partial(kernel, dims),
            out_shape=(
                jax.ShapeDtypeStruct((nx, ny, nz), F32),
                jax.ShapeDtypeStruct((1, 1), F32),
            ),
            in_specs=[hbm] * 11,
            out_specs=(vmem, vmem),
            scratch_shapes=[
                pltpu.VMEM((COMPS, planes, 64, nz), F32),
                pltpu.VMEM((2, nx, ny, nz), F32),
                pltpu.VMEM((2, COMPS, nx, HALO, nz), F32),
                pltpu.VMEM((2, COMPS, nx, HALO, nz), F32),
                pltpu.VMEM((2, 2, COMPS, HALO, HALO, nz), F32),
                pltpu.VMEM((nrec // (ngx * ngy * ngz), trace), F32),
                pltpu.VMEM((1, nrec), jnp.int32),
                pltpu.SMEM((trace,), F32),
                pltpu.SMEM((1,), jnp.int32),
                pltpu.SMEM((1,), jnp.int32),
                pltpu.VMEM((4, ny, 128), F32),
                pltpu.VMEM((2, 4, HALO, 128), F32),
                pltpu.VMEM((2, 2, ny, 128), F32),
                pltpu.VMEM((2, 2, 2, HALO, 128), F32),
                pltpu.VMEM((2, 4, ny, 128), F32),
                pltpu.VMEM((2, 2, 4, HALO, 128), F32),
                pltpu.VMEM((2, 2, 2, ny, 128), F32),
                pltpu.VMEM((2, 2, 2, 2, HALO, 128), F32),
                pltpu.VMEM((COMPS, 64, 128), F32),
                pltpu.VMEM((STEPS, 3, nx, ny, nz), F32),
                pltpu.VMEM((STEPS, 3, nx, ny, nz), F32),
                pltpu.VMEM((ROWS, 128), F32),
                pltpu.VMEM((ROWS, 128), F32),
                pltpu.VMEM((ROWS, 128), F32),
                pltpu.VMEM((ROWS, 128), F32),
                pltpu.VMEM(((planes - 2) * ROWS, nrec), BF16),
                pltpu.VMEM((STEPS, planes, ROWS, nz), F32),
                pltpu.VMEM((STEPS - 1, ROWS, 128), F32),
                pltpu.VMEM((16, STEPS, 128), F32),
                pltpu.VMEM((16, STEPS, 128), F32),
                pltpu.VMEM((16, 1, 128), F32),
                pltpu.VMEM((16, 1, 128), F32),
                pltpu.SemaphoreType.DMA((11,)),
                pltpu.SemaphoreType.DMA((53,)),
                pltpu.SemaphoreType.DMA((53,)),
                pltpu.SemaphoreType.DMA((4, 15)),
                pltpu.SemaphoreType.DMA((4, 16)),
            ],
            compiler_params=pltpu.CompilerParams(
                collective_id=0, has_side_effects=True, vmem_limit_bytes=60 * 1024 * 1024
            ),
            name="window",
        )(
            permittivity,
            loss,
            fwd_electric,
            fwd_magnetic,
            adj_electric,
            adj_magnetic,
            residuals,
            receiver_cells.reshape(1, nrec),
            wavelet,
            source_cell,
            start_step,
        )
        rms = rms.reshape(())
        return gradient / rms, rms

    field_spec = P(None, "gx", "gy", "gz")
    block_spec = P("gx", "gy", "gz")
    return jax.shard_map(
        per_device,
        mesh=mesh,
        in_specs=(
            block_spec,
            block_spec,
            field_spec,
            field_spec,
            field_spec,
            field_spec,
            P(),
            P(("gx", "gy", "gz"), None),
            P(),
            P(),
            P(),
        ),
        out_specs=(block_spec, P()),
        check_vma=False,
    )
```

```python
import functools

import jax
import jax.numpy as jnp
from jax import lax
from jax.experimental import pallas as pl
from jax.experimental.pallas import tpu as pltpu
from jax.sharding import PartitionSpec as P

STEPS = 4
MESH = pl.DeviceIdType.MESH
F32 = jnp.float32
BF16 = jnp.bfloat16

HALO = 4
OWNX = HALO
OWNY = 16
TOP = 8
ROWS = 48
KEEP, CURL = 6, 7
FIRST = 8
COMPS = 14


def kernel(
    dims,
    perm_hbm,
    loss_hbm,
    fe_hbm,
    fm_hbm,
    ae_hbm,
    am_hbm,
    res_hbm,
    cells_hbm,
    wave_hbm,
    source_hbm,
    start_hbm,
    out_ref,
    rms_ref,
    field,
    medium,
    ysend,
    yrecv,
    corner,
    res_ref,
    cells_ref,
    wave_ref,
    source_ref,
    start_ref,
    pack,
    packedge,
    packx,
    packxedge,
    packrecv,
    packedgerecv,
    packxrecv,
    packxedgerecv,
    slab,
    snaps,
    change,
    hrow,
    hslab,
    smask,
    sslab,
    onehot,
    inj,
    injslab,
    gather1,
    gather2,
    red1,
    red2,
    load_sem,
    halo_send,
    halo_recv,
    group_send,
    group_recv,
):
    ngx, ngy, ngz, nx, ny, nz, nrec = dims
    gx, gy, gz = lax.axis_index("gx"), lax.axis_index("gy"), lax.axis_index("gz")
    own = (slice(OWNX, OWNX + nx), slice(OWNY, OWNY + ny))

    loads = {}
    for k, (name, src, dst) in enumerate(
        (
            ("fe", fe_hbm, field.at[0:3, own[0], own[1]]),
            ("fm", fm_hbm, field.at[3:6, own[0], own[1]]),
            ("perm", perm_hbm, medium.at[0]),
            ("loss", loss_hbm, medium.at[1]),
            ("start", start_hbm, start_ref),
            ("res", res_hbm, res_ref),
            ("ae", ae_hbm, field.at[8:11, own[0], own[1]]),
            ("am", am_hbm, field.at[11:14, own[0], own[1]]),
            ("source", source_hbm, source_ref),
            ("wave", wave_hbm, wave_ref),
            ("cells", cells_hbm, cells_ref),
        )
    ):
        loads[name] = pltpu.make_async_copy(src, dst, load_sem.at[k])
        loads[name].start()

    def there(dx, dy):
        ok = []
        if dx:
            ok.append((gx + dx >= 0) & (gx + dx < ngx))
        if dy:
            ok.append((gy + dy >= 0) & (gy + dy < ngy))
        if not ok:
            return None
        return functools.reduce(jnp.logical_and, ok)

    def guarded(cond, fn):
        if cond is None:
            fn()
        else:
            pl.when(cond)(fn)

    x_low, z_chip = gy // 8, lax.rem(gy, 8)
    y_chip, core = gx // 2, lax.rem(gx, 2)

    def device(z, x_hi, y, core, x_lo):
        return {"gx": y * 2 + core, "gy": x_lo * 8 + z, "gz": x_hi}

    groups = (
        (z_chip * 2 + gz, lambda k: device(k // 2, lax.rem(k, 2), y_chip, core, x_low)),
        (gx * 2 + x_low, lambda k: device(z_chip, gz, k // 4, lax.rem(k // 2, 2), lax.rem(k, 2))),
        (
            (gz * 2 + x_low) * 4 + y_chip,
            lambda k: device(z_chip, k // 8, lax.rem(k, 4), core, lax.rem(k // 4, 2)),
        ),
        (z_chip * 2 + core, lambda k: device(k // 2, gz, y_chip, lax.rem(k, 2), x_low)),
    )
    i1, i2 = groups[0][0], groups[1][0]

    barrier = pltpu.get_barrier_semaphore()
    apart = sorted(
        {(dz, dh, 0, 0, 0) for dz in range(8) for dh in range(2)}
        | {(0, 0, dy, dc, dl) for dy in range(4) for dc in range(2) for dl in range(2)}
        | {(0, dh, dy, 0, dl) for dh in range(2) for dy in range(4) for dl in range(2)}
        | {(dz, 0, 0, dc, 0) for dz in range(8) for dc in range(2)}
    )[1:]
    for dz, dh, dy, dc, dl in apart:
        pl.semaphore_signal(
            barrier,
            inc=1,
            device_id=device(
                lax.rem(z_chip + dz, 8),
                lax.rem(gz + dh, 2),
                lax.rem(y_chip + dy, 4),
                lax.rem(core + dc, 2),
                lax.rem(x_low + dl, 2),
            ),
            device_id_type=MESH,
        )
    for dx in (-1, 0, 1):
        for dy in (-1, 0, 1):
            for dz in (0, 1):
                if dx or dy or dz:
                    peer = {"gx": gx + dx, "gy": gy + dy, "gz": gz if dz == 0 else 1 - gz}
                    guarded(
                        there(dx, dy),
                        lambda peer=peer: pl.semaphore_signal(
                            barrier, inc=1, device_id=peer, device_id_type=MESH
                        ),
                    )

    def clear_planes(low):
        def body(c, _):
            field[c, low : low + HALO, OWNY : OWNY + ny, :] = jnp.zeros((HALO, ny, nz), F32)
            return 0

        lax.fori_loop(0, COMPS, body, 0)

    pl.when(gx == 0)(lambda: clear_planes(0))
    pl.when(gx == ngx - 1)(lambda: clear_planes(OWNX + nx))

    def clear(ref):
        ref[...] = jnp.zeros(ref.shape, F32)

    def clear_loop(ref):
        def body(c, _):
            ref[c] = jnp.zeros(ref.shape[1:], F32)
            return 0

        lax.fori_loop(0, ref.shape[0], body, 0)

    for ys, dy in ((0, -1), (1, 1)):
        missing_y = (gy + dy < 0) | (gy + dy >= ngy)
        pl.when(missing_y)(lambda ys=ys: clear_loop(yrecv.at[ys]))
        for xs, dx in ((0, -1), (1, 1)):
            missing = missing_y | (gx + dx < 0) | (gx + dx >= ngx)
            pl.when(missing)(lambda xs=xs, ys=ys: clear_loop(corner.at[xs, ys]))
        for z in range(2):
            pl.when(missing_y)(lambda z=z, ys=ys: clear(packedgerecv.at[z, ys]))
            for xs, dx in ((0, -1), (1, 1)):
                missing = missing_y | (gx + dx < 0) | (gx + dx >= ngx)
                pl.when(missing)(lambda z=z, xs=xs, ys=ys: clear(packxedgerecv.at[z, xs, ys]))
    for xs, dx in ((0, -1), (1, 1)):
        missing = (gx + dx < 0) | (gx + dx >= ngx)
        for z in range(2):
            pl.when(missing)(lambda z=z, xs=xs: clear(packxrecv.at[z, xs]))

    loads["start"].wait()
    loads["res"].wait()
    start = start_ref[0]
    lane8 = lax.broadcasted_iota(jnp.int32, (8, 128), 1)
    sub8 = lax.broadcasted_iota(jnp.int32, (8, 128), 0)

    time = lax.broadcasted_iota(jnp.int32, res_ref.shape, 1)
    rows = []
    for m in range(STEPS):
        column = jnp.sum(jnp.where(time == start + m, res_ref[...], 0.0), axis=1, keepdims=True)
        spread = jnp.where(lane8 - i1 * 8 == sub8, jnp.broadcast_to(column, (8, 128)), 0.0)
        rows.append(jnp.sum(spread, axis=0, keepdims=True))
    gather1[i1] = jnp.concatenate(rows, axis=0)

    def group_copy(round_, which, ref, step):
        mine, member = groups[which]
        peer = lax.rem(mine + step, 16)
        return pltpu.make_async_remote_copy(
            src_ref=ref.at[mine],
            dst_ref=ref.at[mine],
            send_sem=group_send.at[round_, step - 1],
            recv_sem=group_recv.at[round_, mine],
            device_id=member(peer),
            device_id_type=MESH,
        )

    def group_arrival(round_, which, ref, step):
        mine, member = groups[which]
        peer = lax.rem(mine + step, 16)
        return pltpu.make_async_remote_copy(
            src_ref=ref.at[mine],
            dst_ref=ref.at[peer],
            send_sem=group_send.at[round_, step - 1],
            recv_sem=group_recv.at[round_, peer],
            device_id=member(peer),
            device_id_type=MESH,
        )

    def group_start(round_, which, ref):
        for step in range(1, 16):
            group_copy(round_, which, ref, step).start()

    def group_wait(round_, which, ref):
        for step in range(1, 16):
            group_arrival(round_, which, ref, step).wait_recv()

    def group_drain(round_, which, ref):
        for step in range(1, 16):
            group_copy(round_, which, ref, step).wait_send()

    sends = []
    number = [0]

    def remote(src, dst, dx, dy, dz, back, also=None):
        k = number[0]
        number[0] += 1

        def make(landing):
            return pltpu.make_async_remote_copy(
                src_ref=src,
                dst_ref=landing,
                send_sem=halo_send.at[k],
                recv_sem=halo_recv.at[k],
                device_id={"gx": gx + dx, "gy": gy + dy, "gz": gz if dz == 0 else 1 - gz},
                device_id_type=MESH,
            )

        go, come = there(dx, dy), there(-dx, -dy)
        if also is not None:
            go, come = go & also, come & also
        guarded(go, lambda: make(dst).start())
        sends.append((go, make(dst)))
        return lambda: guarded(come, lambda: make(back).wait_recv())

    def side(d):
        return 0 if d == 1 else 1

    def span(low, count):
        return slice(low, low + count)

    def start_along_x(low_parts, high_parts):
        waits, leaving = [], []
        rows_ = slice(OWNY, OWNY + ny)
        for dx, parts in ((1, low_parts), (-1, high_parts)):
            for first, last, depth in parts:
                if dx == 1:
                    source, target = span(OWNX + nx - depth, depth), span(HALO - depth, depth)
                else:
                    source, target = span(OWNX, depth), span(OWNX + nx, depth)
                landing = field.at[first:last, target, rows_]
                waits.append(remote(field.at[first:last, source, rows_], landing, dx, 0, 0, landing))
                cond, copy = sends.pop()
                leaving.append(lambda cond=cond, copy=copy: guarded(cond, copy.wait_send))
        return waits, leaving

    def start_along_y(c0, c1):
        waits = []
        for dy in (1, -1):
            landing = yrecv.at[side(dy), c0:c1]
            waits.append(remote(ysend.at[1 if dy == 1 else 0, c0:c1], landing, 0, dy, 0, landing))
        return waits

    def relay_corners(c0, c1):
        waits = []
        for ys, dy in ((0, -1), (1, 1)):
            for dx in (1, -1):
                depth = HALO - 1 if dx == -dy else HALO
                part = span(nx - depth, depth) if dx == 1 else span(0, depth)
                place = span(HALO - depth, depth) if dx == 1 else span(0, depth)
                landing = corner.at[side(dx), ys, c0:c1, place]
                waits.append(
                    remote(yrecv.at[ys, c0:c1, part], landing, dx, 0, 0, landing, there(0, dy))
                )
        return waits

    def start_along_z(chunk):
        groups_ = span(2 * chunk, 2)
        return remote(pack.at[groups_], packrecv.at[gz, groups_], 0, 0, 1, packrecv.at[1 - gz, groups_])

    def start_slabs(chunk, which):
        z = gz if which == 0 else 1 - gz
        waits = []
        groups_ = span(2 * chunk, 2)
        for dx in (0, 1, -1):
            for dy in (0, 1, -1):
                if not (dx or dy):
                    continue
                edge = 1 if dy == 1 else 0
                if dx == 0:
                    src, land = packedge.at[which, edge, groups_], packedgerecv.at[z, side(dy), groups_]
                elif dy == 0:
                    src, land = packx.at[which, side(dx), chunk], packxrecv.at[z, side(dx), chunk]
                else:
                    src = packxedge.at[which, side(dx), edge, chunk]
                    land = packxedgerecv.at[z, side(dx), side(dy), chunk]
                waits.append(remote(src, land, dx, dy, 0, land))
        return waits

    def share_slab(chunk, which, both):
        for k in range(2):
            packedge[which, 0, 2 * chunk + k] = both[k][0:HALO]
            packedge[which, 1, 2 * chunk + k] = both[k][ny - HALO : ny]
        high = jnp.where(upper32, both[0], pltpu.roll(both[1], 96, axis=1))
        low = jnp.where(upper32, pltpu.roll(both[1], 32, axis=1), both[0])
        for k, value in ((0, high), (1, low)):
            packx[which, k, chunk] = value
            packxedge[which, k, 0, chunk] = value[0:HALO]
            packxedge[which, k, 1, chunk] = value[ny - HALO : ny]

    def relay_slabs(chunk):
        share_slab(chunk, 1, [packrecv[1 - gz, 2 * chunk + k] for k in range(2)])
        return start_slabs(chunk, 1)

    def pack_edges(c0, c1):
        for c in range(c0, c1):
            ysend[0, c] = field[c, own[0], OWNY : OWNY + HALO, :]
            ysend[1, c] = field[c, own[0], OWNY + ny - HALO : OWNY + ny, :]

    lane32 = lax.broadcasted_iota(jnp.int32, (ny, 128), 1)
    quad = lane32 // 4
    upper32 = lax.rem(lane32, 64) >= 32
    lift = 4 * (1 - gz)

    def pack_slab(chunk):
        both = []
        for group in (2 * chunk, 2 * chunk + 1):
            packed = jnp.zeros((ny, 128), F32)
            for part in range(4):
                comp = group * 4 + part
                if comp >= COMPS:
                    continue
                for i in range(nx):
                    base = (part // 2) * 64 + i * 8 + (part % 2) * 4
                    moved = pltpu.roll(field[comp, OWNX + i, own[1], :], base + lift, axis=1)
                    packed = jnp.where(quad == base // 4, moved, packed)
            pack[group] = packed
            packrecv[gz, group] = packed
            both.append(packed)
        share_slab(chunk, 0, both)

    loads["perm"].wait()
    loads["loss"].wait()
    for i in range(nx):
        loss = medium[1, i]
        field[KEEP, OWNX + i, OWNY : OWNY + ny, :] = (1.0 - loss) / (1.0 + loss)
        field[CURL, OWNX + i, OWNY : OWNY + ny, :] = 0.5 / (medium[0, i] * (1.0 + loss))
    loads["fe"].wait()
    loads["fm"].wait()
    pack_slab(0)
    pack_edges(0, FIRST)
    count_x = 3 - (gx == 0).astype(jnp.int32) - (gx == ngx - 1).astype(jnp.int32)
    count_y = 3 - (gy == 0).astype(jnp.int32) - (gy == ngy - 1).astype(jnp.int32)
    pl.semaphore_wait(barrier, count_x * count_y * 2 - 1 + len(apart))
    group_start(0, 0, gather1)
    first_z = start_along_z(0)
    first_waits, first_leaving = start_along_x(
        ((0, 3, HALO), (3, 4, HALO - 1), (4, 6, HALO), (KEEP, CURL + 1, HALO - 1)),
        ((0, 1, HALO - 1), (1, 3, HALO), (3, FIRST, HALO - 1)),
    )
    first_y = start_along_y(0, FIRST)
    first_waits += start_slabs(0, 0)
    loads["ae"].wait()
    loads["am"].wait()
    pack_slab(1)
    pack_edges(FIRST, COMPS)
    second_z = start_along_z(1)
    second_y = start_along_y(FIRST, COMPS)
    second_waits = start_slabs(1, 0)
    loads["source"].wait()
    loads["wave"].wait()
    loads["cells"].wait()
    row = lax.broadcasted_iota(jnp.int32, (ROWS, 128), 0) + TOP
    lane = lax.broadcasted_iota(jnp.int32, (ROWS, 128), 1)
    row_y = row - OWNY + gy * ny
    hrow[...] = jnp.where(row_y >= 0, 0.5, 0.0)
    slab_x = lane // 8 - OWNX + gx * nx
    hslab[...] = jnp.where((row_y >= 0) & (slab_x >= 0), 0.5, 0.0)
    source = source_ref[0]
    total_y, total_z = ngy * ny, ngz * nz
    src_x = source // (total_y * total_z)
    src_y = lax.rem(source // total_z, total_y)
    src_z = lax.rem(source, total_z)
    in_row = row_y == src_y
    smask[...] = jnp.where(in_row & (lane + gz * nz == src_z), 1.0, 0.0)
    slab_z = lax.rem(lane, 8) + nz - HALO
    sslab[...] = jnp.where(in_row & (slab_x == src_x) & (slab_z == src_z), 1.0, 0.0)
    src_plane = src_x - gx * nx + OWNX

    cells = cells_ref[...]
    rec_x = cells // (total_y * total_z) - gx * nx + OWNX
    rec_y = lax.rem(cells // total_z, total_y) - gy * ny + OWNY - TOP
    rec_z = lax.rem(cells, total_z)
    in_x = (rec_x >= 0) & (rec_x < nx + 2 * HALO)
    in_y = (rec_y >= 0) & (rec_y < ROWS)
    rec_row = jnp.where(in_x & in_y, rec_x * ROWS + rec_y, -1)
    rec_lane = rec_z - gz * nz
    planes = nx + 2 * HALO - 2

    def build(i, _):
        ids = lax.broadcasted_iota(jnp.int32, (ROWS, nrec), 0) + (i + 1) * ROWS
        onehot[pl.ds(pl.multiple_of(i * ROWS, 16), ROWS), :] = jnp.where(ids == rec_row, 1.0, 0.0).astype(BF16)
        return 0

    lax.fori_loop(0, planes, build, 0)

    group_wait(0, 0, gather1)
    row_of_samples = gather1[0]
    for k in range(1, 16):
        row_of_samples = row_of_samples + gather1[k]
    gather2[i2] = row_of_samples
    group_start(1, 1, gather2)
    first_z()
    first_waits += relay_slabs(0)
    for wait in first_y:
        wait()
    first_waits += relay_corners(0, FIRST)
    second_x, second_leaving = start_along_x(
        ((8, 11, HALO), (11, 12, HALO - 1), (12, COMPS, HALO)),
        ((8, 9, HALO - 1), (9, 11, HALO), (11, COMPS, HALO - 1)),
    )
    second_waits += second_x

    lane_r = lax.broadcasted_iota(jnp.int32, (ROWS, nz), 1)

    def assemble(c0, c1):
        zeros = jnp.zeros((HALO, nz), F32)
        for c in range(c0, c1):
            for i in range(nx + 2 * HALO):
                for ys in range(2):
                    if i < OWNX:
                        piece = corner[0, ys, c, i]
                    elif i < OWNX + nx:
                        piece = yrecv[ys, c, i - OWNX]
                    else:
                        piece = corner[1, ys, c, i - OWNX - nx]
                    if ys == 0:
                        field[c, i, TOP:OWNY, :] = jnp.concatenate([zeros, piece], axis=0)
                    else:
                        field[c, i, OWNY + ny : OWNY + ny + 8, :] = jnp.concatenate([piece, zeros], axis=0)

    lane_p = lax.broadcasted_iota(jnp.int32, (ROWS, 128), 1)
    deep = lax.rem(lane_p, 8) >= 4
    inside = (lane_p >= 32) & (lane_p < 96)
    upper = lax.rem(lane_p, 64) >= 32

    def assemble_slab(chunk):
        zeros = jnp.zeros((HALO, 128), F32)

        def column(low, middle, high):
            return jnp.concatenate([zeros, low, middle, high, zeros], axis=0)

        sides = [
            [
                column(
                    packxedgerecv[z, k, 0, chunk], packxrecv[z, k, chunk], packxedgerecv[z, k, 1, chunk]
                )
                for k in range(2)
            ]
            for z in range(2)
        ]
        for odd in range(2):
            group = 2 * chunk + odd
            centre, beside = [], []
            for z in range(2):
                centre.append(
                    column(packedgerecv[z, 0, group], packrecv[z, group], packedgerecv[z, 1, group])
                )
                low, high = sides[z]
                if odd:
                    low, high = pltpu.roll(low, 32, axis=1), pltpu.roll(high, 96, axis=1)
                beside.append(jnp.where(upper, low, high))
            for part in range(4):
                comp = group * 4 + part
                if comp >= COMPS:
                    continue
                base = (part // 2) * 64 + (part % 2) * 4
                inner = [pltpu.roll(centre[z], (32 + 4 * z - base) % 128, axis=1) for z in range(2)]
                outer = [pltpu.roll(beside[z], (96 + 4 * z - base) % 128, axis=1) for z in range(2)]
                slab[comp, TOP : TOP + ROWS, :] = jnp.where(
                    inside, jnp.where(deep, inner[1], inner[0]), jnp.where(deep, outer[1], outer[0])
                )

    up_keep = jnp.where(gz == 0, 1.0, 0.0)
    down_keep = jnp.where(gz == 0, 0.0, 1.0)
    def moved(window, by):
        return slice(window.start + by, window.stop + by)

    def magnetic_half(b, step):
        at = slice(TOP, TOP + ROWS) if step < STEPS else slice(TOP, OWNY + ny)
        mask_at = moved(at, -TOP)
        tall = at.stop - at.start
        last_lane = lax.broadcasted_iota(jnp.int32, (tall, nz), 1) == nz - 1
        for i in range(step - 1, nx + 2 * HALO - step):
            factor = hrow[mask_at]
            if i < OWNX:
                factor = factor * jnp.where(gx > 0, 1.0, 0.0)
            ex, ey, ez = field[b, i, at], field[b + 1, i, at], field[b + 2, i, at]
            turn = (nz - 1 - HALO - 8 * i) % 128

            def deeper(value, comp):
                edge = pltpu.roll(slab[comp, at], turn, axis=1) * up_keep
                return jnp.where(last_lane, edge, pltpu.roll(value, nz - 1, axis=1))

            field[b + 3, i, at] = field[b + 3, i, at] - factor * (
                (field[b + 2, i, moved(at, 1)] - ez) - (deeper(ey, b + 1) - ey)
            )
            field[b + 4, i, at] = field[b + 4, i, at] - factor * (
                (deeper(ex, b) - ex) - (field[b + 2, i + 1, at] - ez)
            )
            field[b + 5, i, at] = field[b + 5, i, at] - factor * (
                (field[b + 1, i + 1, at] - ey) - (field[b, i, moved(at, 1)] - ex)
            )
        factor = hslab[mask_at]
        ex, ey, ez = slab[b, at], slab[b + 1, at], slab[b + 2, at]

        def along_x(value):
            return pltpu.roll(value, 120, axis=1)

        def along_z(value):
            return pltpu.roll(value, 127, axis=1)

        slab[b + 3, at] = slab[b + 3, at] - factor * (
            (slab[b + 2, moved(at, 1)] - ez) - (along_z(ey) - ey)
        )
        slab[b + 4, at] = slab[b + 4, at] - factor * ((along_z(ex) - ex) - (along_x(ez) - ez))
        if step < STEPS:
            slab[b + 5, at] = slab[b + 5, at] - factor * (
                (along_x(ey) - ey) - (slab[b, moved(at, 1)] - ex)
            )

    def electric_half(b, step, extra, extra_slab):
        at = slice(TOP, TOP + ROWS) if step < STEPS else own[1]
        tall = at.stop - at.start
        first_lane = lax.broadcasted_iota(jnp.int32, (tall, nz), 1) == 0
        for i in range(step, nx + 2 * HALO - step):
            keep, curl = field[KEEP, i, at], field[CURL, i, at]
            hx, hy, hz = field[b + 3, i, at], field[b + 4, i, at], field[b + 5, i, at]
            turn = (1 - HALO - 8 * i) % 128

            def shallower(value, comp):
                edge = pltpu.roll(slab[comp, at], turn, axis=1) * down_keep
                return jnp.where(first_lane, edge, pltpu.roll(value, 1, axis=1))

            field[b, i, at] = keep * field[b, i, at] + curl * (
                (hz - field[b + 5, i, moved(at, -1)]) - (hy - shallower(hy, b + 4))
            )
            field[b + 1, i, at] = keep * field[b + 1, i, at] + curl * (
                (hx - shallower(hx, b + 3)) - (hz - field[b + 5, i - 1, at])
            )
            field[b + 2, i, at] = (
                keep * field[b + 2, i, at]
                + curl * ((hy - field[b + 4, i - 1, at]) - (hx - field[b + 3, i, moved(at, -1)]))
                + extra(i, moved(at, -TOP))
            )
        if step == STEPS:
            return
        keep, curl = slab[KEEP, at], slab[CURL, at]
        hx, hy, hz = slab[b + 3, at], slab[b + 4, at], slab[b + 5, at]

        def along_x(value):
            return pltpu.roll(value, 8, axis=1)

        def along_z(value):
            return pltpu.roll(value, 1, axis=1)

        slab[b, at] = keep * slab[b, at] + curl * ((hz - slab[b + 5, moved(at, -1)]) - (hy - along_z(hy)))
        slab[b + 1, at] = keep * slab[b + 1, at] + curl * ((hx - along_z(hx)) - (hz - along_x(hz)))
        slab[b + 2, at] = (
            keep * slab[b + 2, at]
            + curl * ((hy - along_x(hy)) - (hx - slab[b + 3, moved(at, -1)]))
            + extra_slab()
        )

    def snapshot(n):
        for c in range(3):
            for i in range(nx):
                value = field[c, OWNX + i, own[1], :]
                if n < STEPS:
                    snaps[n, c, i] = value
                if n:
                    change[n - 1, c, i] = value - snaps[n - 1, c, i]

    for wait in first_waits + first_leaving:
        wait()
    snapshot(0)
    assemble(0, FIRST)
    assemble_slab(0)

    def pulse(step):
        return wave_ref[start + step - 1]

    def forward_electric(step):
        electric_half(
            0,
            step,
            lambda i, at: smask[at] * jnp.where(i == src_plane, pulse(step), 0.0),
            lambda: sslab[...] * pulse(step),
        )
        snapshot(step)

    def split(value):
        high = value.astype(BF16).astype(F32)
        return high, value - high

    contract = (((1,), (1,)), ((), ()))

    def inject(m):
        high, low = split(samples[STEPS - 1 - m])
        weights = jnp.concatenate(
            [jnp.where(at_lane, high, 0.0).astype(BF16), jnp.where(at_lane, low, 0.0).astype(BF16)],
            axis=0,
        )
        count = planes - 2 * m
        both = lax.dot_general(
            onehot[m * ROWS : (m + count) * ROWS, :], weights, contract, preferred_element_type=F32
        )
        inj[m, 1 + m : 1 + m + count] = (both[:, :nz] + both[:, nz:]).reshape(count, ROWS, nz)

    def inject_slab():
        rec_near = rec_x * 8 + rec_z - (nz - HALO)
        in_slab = in_x & (rec_z >= nz - HALO) & (rec_z < nz + HALO)
        slab_weights = jnp.where(lanes_of == jnp.where(in_slab, rec_near, -1), 1.0, 0.0).astype(BF16)
        at_row = lax.broadcasted_iota(jnp.int32, (ROWS, nrec), 0) == rec_y
        pieces = []
        for m in range(STEPS - 1):
            for value in split(samples[STEPS - 1 - m]):
                pieces.append(jnp.where(at_row, value, 0.0).astype(BF16))
        both = lax.dot_general(
            jnp.concatenate(pieces, axis=0), slab_weights, contract, preferred_element_type=F32
        )
        for m in range(STEPS - 1):
            at = 2 * m * ROWS
            injslab[m] = both[at : at + ROWS] + both[at + ROWS : at + 2 * ROWS]

    for step in (1, 2):
        magnetic_half(0, step)
        forward_electric(step)
    second_z()
    second_waits += relay_slabs(1)
    for wait in second_y:
        wait()
    second_waits += relay_corners(FIRST, COMPS)
    group_wait(1, 1, gather2)
    samples = [
        jnp.concatenate([gather2[k][m : m + 1] for k in range(16)], axis=1) for m in range(STEPS)
    ]
    lanes_of = lax.broadcasted_iota(jnp.int32, (nz, nrec), 0)
    at_lane = lanes_of == rec_lane
    inject(0)
    magnetic_half(0, 3)
    inject(1)
    forward_electric(3)
    inject(2)
    magnetic_half(0, 4)
    inject(3)
    inject_slab()
    forward_electric(4)

    for wait in second_waits + second_leaving:
        wait()
    assemble(FIRST, COMPS)
    assemble_slab(1)
    for step in range(1, STEPS + 1):
        magnetic_half(FIRST, step)
        electric_half(
            FIRST,
            step,
            lambda i, at, m=step - 1: inj[m, i, at],
            lambda m=step - 1: injslab[m],
        )
        square = jnp.zeros((ny, nz), F32)
        for i in range(nx):
            term = None
            for c in range(3):
                product = change[STEPS - step, c, i] * field[FIRST + c, OWNX + i, own[1], :]
                term = product if term is None else term + product
            value = term if step == 1 else out_ref[i] + term
            if step == STEPS:
                value = -value / medium[0, i]
                square = square + value * value
            out_ref[i] = value
    red1[groups[2][0]] = jnp.sum(square, axis=0, keepdims=True)
    group_start(2, 2, red1)
    group_wait(2, 2, red1)
    total = red1[0]
    for k in range(1, 16):
        total = total + red1[k]
    red2[groups[3][0]] = total
    group_start(3, 3, red2)
    group_wait(3, 3, red2)
    total = red2[0]
    for k in range(1, 16):
        total = total + red2[k]
    total = jnp.sum(total, axis=1, keepdims=True)
    cells_in_all = ngx * nx * ngy * ny * ngz * nz
    rms = jnp.sqrt(total / cells_in_all + 1e-06)
    rms_ref[...] = rms
    wide = jnp.broadcast_to(rms, (ny, nz))
    for i in range(nx):
        out_ref[i] = out_ref[i] / wide
    for cond, copy in sends:
        guarded(cond, copy.wait_send)
    group_drain(0, 0, gather1)
    group_drain(1, 1, gather2)
    group_drain(2, 2, red1)
    group_drain(3, 3, red2)


def solution(mesh):
    ngx, ngy, ngz = mesh.shape["gx"], mesh.shape["gy"], mesh.shape["gz"]

    def per_device(
        permittivity,
        loss,
        fwd_electric,
        fwd_magnetic,
        adj_electric,
        adj_magnetic,
        wavelet,
        residuals,
        source_cell,
        receiver_cells,
        start_step,
    ):
        nx, ny, nz = permittivity.shape
        nrec, trace = receiver_cells.shape[0], residuals.shape[1]
        planes = nx + 2 * HALO
        dims = (ngx, ngy, ngz, nx, ny, nz, nrec)
        hbm = pl.BlockSpec(memory_space=pltpu.HBM)
        vmem = pl.BlockSpec(memory_space=pltpu.VMEM)
        direction, rms = pl.pallas_call(
            functools.partial(kernel, dims),
            out_shape=(
                jax.ShapeDtypeStruct((nx, ny, nz), F32),
                jax.ShapeDtypeStruct((1, 1), F32),
            ),
            in_specs=[hbm] * 11,
            out_specs=(vmem, vmem),
            scratch_shapes=[
                pltpu.VMEM((COMPS, planes, 64, nz), F32),
                pltpu.VMEM((2, nx, ny, nz), F32),
                pltpu.VMEM((2, COMPS, nx, HALO, nz), F32),
                pltpu.VMEM((2, COMPS, nx, HALO, nz), F32),
                pltpu.VMEM((2, 2, COMPS, HALO, HALO, nz), F32),
                pltpu.VMEM((nrec // (ngx * ngy * ngz), trace), F32),
                pltpu.VMEM((1, nrec), jnp.int32),
                pltpu.SMEM((trace,), F32),
                pltpu.SMEM((1,), jnp.int32),
                pltpu.SMEM((1,), jnp.int32),
                pltpu.VMEM((4, ny, 128), F32),
                pltpu.VMEM((2, 2, 4, HALO, 128), F32),
                pltpu.VMEM((2, 2, 2, ny, 128), F32),
                pltpu.VMEM((2, 2, 2, 2, HALO, 128), F32),
                pltpu.VMEM((2, 4, ny, 128), F32),
                pltpu.VMEM((2, 2, 4, HALO, 128), F32),
                pltpu.VMEM((2, 2, 2, ny, 128), F32),
                pltpu.VMEM((2, 2, 2, 2, HALO, 128), F32),
                pltpu.VMEM((COMPS, 64, 128), F32),
                pltpu.VMEM((STEPS, 3, nx, ny, nz), F32),
                pltpu.VMEM((STEPS, 3, nx, ny, nz), F32),
                pltpu.VMEM((ROWS, 128), F32),
                pltpu.VMEM((ROWS, 128), F32),
                pltpu.VMEM((ROWS, 128), F32),
                pltpu.VMEM((ROWS, 128), F32),
                pltpu.VMEM(((planes - 2) * ROWS, nrec), BF16),
                pltpu.VMEM((STEPS, planes, ROWS, nz), F32),
                pltpu.VMEM((STEPS - 1, ROWS, 128), F32),
                pltpu.VMEM((16, STEPS, 128), F32),
                pltpu.VMEM((16, STEPS, 128), F32),
                pltpu.VMEM((16, 1, 128), F32),
                pltpu.VMEM((16, 1, 128), F32),
                pltpu.SemaphoreType.DMA((11,)),
                pltpu.SemaphoreType.DMA((59,)),
                pltpu.SemaphoreType.DMA((59,)),
                pltpu.SemaphoreType.DMA((4, 15)),
                pltpu.SemaphoreType.DMA((4, 16)),
            ],
            compiler_params=pltpu.CompilerParams(
                collective_id=0, has_side_effects=True, vmem_limit_bytes=60 * 1024 * 1024
            ),
            name="window",
        )(
            permittivity,
            loss,
            fwd_electric,
            fwd_magnetic,
            adj_electric,
            adj_magnetic,
            residuals,
            receiver_cells.reshape(1, nrec),
            wavelet,
            source_cell,
            start_step,
        )
        return direction, rms.reshape(())

    field_spec = P(None, "gx", "gy", "gz")
    block_spec = P("gx", "gy", "gz")
    return jax.shard_map(
        per_device,
        mesh=mesh,
        in_specs=(
            block_spec,
            block_spec,
            field_spec,
            field_spec,
            field_spec,
            field_spec,
            P(),
            P(("gx", "gy", "gz"), None),
            P(),
            P(),
            P(),
        ),
        out_specs=(block_spec, P()),
        check_vma=False,
    )
```

```python
import functools

import jax
import jax.numpy as jnp
from jax import lax
from jax.experimental import pallas as pl
from jax.experimental.pallas import tpu as pltpu
from jax.sharding import PartitionSpec as P

STEPS = 4
MESH = pl.DeviceIdType.MESH
F32 = jnp.float32
BF16 = jnp.bfloat16

HALO = 4
OWNX = HALO
OWNY = 16
TOP = 8
ROWS = 48
KEEP, CURL = 6, 7
FIRST = 8
COMPS = 14


def kernel(
    dims,
    perm_hbm,
    loss_hbm,
    fe_hbm,
    fm_hbm,
    ae_hbm,
    am_hbm,
    res_hbm,
    cells_hbm,
    wave_hbm,
    source_hbm,
    start_hbm,
    out_ref,
    rms_ref,
    field,
    medium,
    ysend,
    yrecv,
    corner,
    res_ref,
    cells_ref,
    wave_ref,
    source_ref,
    start_ref,
    pack,
    packedge,
    packx,
    packxedge,
    packrecv,
    packedgerecv,
    packxrecv,
    packxedgerecv,
    slab,
    snaps,
    change,
    hrow,
    hslab,
    smask,
    sslab,
    onehot,
    inj,
    injslab,
    gather1,
    gather2,
    red1,
    red2,
    load_sem,
    halo_send,
    halo_recv,
    group_send,
    group_recv,
):
    ngx, ngy, ngz, nx, ny, nz, nrec = dims
    gx, gy, gz = lax.axis_index("gx"), lax.axis_index("gy"), lax.axis_index("gz")
    own = (slice(OWNX, OWNX + nx), slice(OWNY, OWNY + ny))

    loads = {}
    for k, (name, src, dst) in enumerate(
        (
            ("fe", fe_hbm, field.at[0:3, own[0], own[1]]),
            ("fm", fm_hbm, field.at[3:6, own[0], own[1]]),
            ("perm", perm_hbm, medium.at[0]),
            ("loss", loss_hbm, medium.at[1]),
            ("start", start_hbm, start_ref),
            ("res", res_hbm, res_ref),
            ("ae", ae_hbm, field.at[8:11, own[0], own[1]]),
            ("am", am_hbm, field.at[11:14, own[0], own[1]]),
            ("source", source_hbm, source_ref),
            ("wave", wave_hbm, wave_ref),
            ("cells", cells_hbm, cells_ref),
        )
    ):
        loads[name] = pltpu.make_async_copy(src, dst, load_sem.at[k])
        loads[name].start()

    def there(dx, dy):
        ok = []
        if dx:
            ok.append((gx + dx >= 0) & (gx + dx < ngx))
        if dy:
            ok.append((gy + dy >= 0) & (gy + dy < ngy))
        if not ok:
            return None
        return functools.reduce(jnp.logical_and, ok)

    def guarded(cond, fn):
        if cond is None:
            fn()
        else:
            pl.when(cond)(fn)

    x_low, z_chip = gy // 8, lax.rem(gy, 8)
    y_chip, core = gx // 2, lax.rem(gx, 2)

    def device(z, x_hi, y, core, x_lo):
        return {"gx": y * 2 + core, "gy": x_lo * 8 + z, "gz": x_hi}

    groups = (
        (z_chip * 2 + gz, lambda k: device(k // 2, lax.rem(k, 2), y_chip, core, x_low)),
        (gx * 2 + x_low, lambda k: device(z_chip, gz, k // 4, lax.rem(k // 2, 2), lax.rem(k, 2))),
        (
            (gz * 2 + x_low) * 4 + y_chip,
            lambda k: device(z_chip, k // 8, lax.rem(k, 4), core, lax.rem(k // 4, 2)),
        ),
        (z_chip * 2 + core, lambda k: device(k // 2, gz, y_chip, lax.rem(k, 2), x_low)),
    )
    i1, i2 = groups[0][0], groups[1][0]

    barrier = pltpu.get_barrier_semaphore()
    apart = sorted(
        {(dz, dh, 0, 0, 0) for dz in range(8) for dh in range(2)}
        | {(0, 0, dy, dc, dl) for dy in range(4) for dc in range(2) for dl in range(2)}
        | {(0, dh, dy, 0, dl) for dh in range(2) for dy in range(4) for dl in range(2)}
        | {(dz, 0, 0, dc, 0) for dz in range(8) for dc in range(2)}
    )[1:]
    for dz, dh, dy, dc, dl in apart:
        pl.semaphore_signal(
            barrier,
            inc=1,
            device_id=device(
                lax.rem(z_chip + dz, 8),
                lax.rem(gz + dh, 2),
                lax.rem(y_chip + dy, 4),
                lax.rem(core + dc, 2),
                lax.rem(x_low + dl, 2),
            ),
            device_id_type=MESH,
        )
    for dx in (-1, 0, 1):
        for dy in (-1, 0, 1):
            for dz in (0, 1):
                if dx or dy or dz:
                    peer = {"gx": gx + dx, "gy": gy + dy, "gz": gz if dz == 0 else 1 - gz}
                    guarded(
                        there(dx, dy),
                        lambda peer=peer: pl.semaphore_signal(
                            barrier, inc=1, device_id=peer, device_id_type=MESH
                        ),
                    )

    def clear_planes(low):
        def body(c, _):
            field[c, low : low + HALO, OWNY : OWNY + ny, :] = jnp.zeros((HALO, ny, nz), F32)
            return 0

        lax.fori_loop(0, COMPS, body, 0)

    pl.when(gx == 0)(lambda: clear_planes(0))
    pl.when(gx == ngx - 1)(lambda: clear_planes(OWNX + nx))

    def clear(ref):
        ref[...] = jnp.zeros(ref.shape, F32)

    def clear_loop(ref):
        def body(c, _):
            ref[c] = jnp.zeros(ref.shape[1:], F32)
            return 0

        lax.fori_loop(0, ref.shape[0], body, 0)

    for ys, dy in ((0, -1), (1, 1)):
        missing_y = (gy + dy < 0) | (gy + dy >= ngy)
        pl.when(missing_y)(lambda ys=ys: clear_loop(yrecv.at[ys]))
        for xs, dx in ((0, -1), (1, 1)):
            missing = missing_y | (gx + dx < 0) | (gx + dx >= ngx)
            pl.when(missing)(lambda xs=xs, ys=ys: clear_loop(corner.at[xs, ys]))
        for z in range(2):
            pl.when(missing_y)(lambda z=z, ys=ys: clear(packedgerecv.at[z, ys]))
            for xs, dx in ((0, -1), (1, 1)):
                missing = missing_y | (gx + dx < 0) | (gx + dx >= ngx)
                pl.when(missing)(lambda z=z, xs=xs, ys=ys: clear(packxedgerecv.at[z, xs, ys]))
    for xs, dx in ((0, -1), (1, 1)):
        missing = (gx + dx < 0) | (gx + dx >= ngx)
        for z in range(2):
            pl.when(missing)(lambda z=z, xs=xs: clear(packxrecv.at[z, xs]))

    loads["start"].wait()
    loads["res"].wait()
    start = start_ref[0]
    lane8 = lax.broadcasted_iota(jnp.int32, (8, 128), 1)
    sub8 = lax.broadcasted_iota(jnp.int32, (8, 128), 0)

    time = lax.broadcasted_iota(jnp.int32, res_ref.shape, 1)
    rows = []
    for m in range(STEPS):
        column = jnp.sum(jnp.where(time == start + m, res_ref[...], 0.0), axis=1, keepdims=True)
        spread = jnp.where(lane8 - i1 * 8 == sub8, jnp.broadcast_to(column, (8, 128)), 0.0)
        rows.append(jnp.sum(spread, axis=0, keepdims=True))
    gather1[i1] = jnp.concatenate(rows, axis=0)

    def group_copy(round_, which, ref, step):
        mine, member = groups[which]
        peer = lax.rem(mine + step, 16)
        return pltpu.make_async_remote_copy(
            src_ref=ref.at[mine],
            dst_ref=ref.at[mine],
            send_sem=group_send.at[round_, step - 1],
            recv_sem=group_recv.at[round_, mine],
            device_id=member(peer),
            device_id_type=MESH,
        )

    def group_arrival(round_, which, ref, step):
        mine, member = groups[which]
        peer = lax.rem(mine + step, 16)
        return pltpu.make_async_remote_copy(
            src_ref=ref.at[mine],
            dst_ref=ref.at[peer],
            send_sem=group_send.at[round_, step - 1],
            recv_sem=group_recv.at[round_, peer],
            device_id=member(peer),
            device_id_type=MESH,
        )

    def group_start(round_, which, ref):
        for step in range(1, 16):
            group_copy(round_, which, ref, step).start()

    def group_wait(round_, which, ref):
        for step in range(1, 16):
            group_arrival(round_, which, ref, step).wait_recv()

    def group_drain(round_, which, ref):
        for step in range(1, 16):
            group_copy(round_, which, ref, step).wait_send()

    sends = []
    number = [0]

    def remote(src, dst, dx, dy, dz, back, also=None):
        k = number[0]
        number[0] += 1

        def make(landing):
            return pltpu.make_async_remote_copy(
                src_ref=src,
                dst_ref=landing,
                send_sem=halo_send.at[k],
                recv_sem=halo_recv.at[k],
                device_id={"gx": gx + dx, "gy": gy + dy, "gz": gz if dz == 0 else 1 - gz},
                device_id_type=MESH,
            )

        go, come = there(dx, dy), there(-dx, -dy)
        if also is not None:
            go, come = go & also, come & also
        guarded(go, lambda: make(dst).start())
        sends.append((go, make(dst)))
        return lambda: guarded(come, lambda: make(back).wait_recv())

    def side(d):
        return 0 if d == 1 else 1

    def span(low, count):
        return slice(low, low + count)

    def start_along_x(low_parts, high_parts):
        waits, leaving = [], []
        rows_ = slice(OWNY, OWNY + ny)
        for dx, parts in ((1, low_parts), (-1, high_parts)):
            for first, last, depth in parts:
                if dx == 1:
                    source, target = span(OWNX + nx - depth, depth), span(HALO - depth, depth)
                else:
                    source, target = span(OWNX, depth), span(OWNX + nx, depth)
                landing = field.at[first:last, target, rows_]
                waits.append(remote(field.at[first:last, source, rows_], landing, dx, 0, 0, landing))
                cond, copy = sends.pop()
                leaving.append(lambda cond=cond, copy=copy: guarded(cond, copy.wait_send))
        return waits, leaving

    def start_along_y(c0, c1):
        waits = []
        for dy in (1, -1):
            landing = yrecv.at[side(dy), c0:c1]
            waits.append(remote(ysend.at[1 if dy == 1 else 0, c0:c1], landing, 0, dy, 0, landing))
        return waits

    def relay_corners(c0, c1):
        waits = []
        for ys, dy in ((0, -1), (1, 1)):
            for dx in (1, -1):
                depth = HALO - 1 if dx == -dy else HALO
                part = span(nx - depth, depth) if dx == 1 else span(0, depth)
                place = span(HALO - depth, depth) if dx == 1 else span(0, depth)
                landing = corner.at[side(dx), ys, c0:c1, place]
                waits.append(
                    remote(yrecv.at[ys, c0:c1, part], landing, dx, 0, 0, landing, there(0, dy))
                )
        return waits

    def start_along_z(chunk):
        groups_ = span(2 * chunk, 2)
        return remote(pack.at[groups_], packrecv.at[gz, groups_], 0, 0, 1, packrecv.at[1 - gz, groups_])

    def start_slabs(chunk, which):
        z = gz if which == 0 else 1 - gz
        edges, sides = [], []
        groups_ = span(2 * chunk, 2)
        for dx in (0, 1, -1):
            for dy in (0, 1, -1):
                if not (dx or dy):
                    continue
                edge = 1 if dy == 1 else 0
                if dx == 0:
                    src, land = packedge.at[which, edge, groups_], packedgerecv.at[z, side(dy), groups_]
                elif dy == 0:
                    src, land = packx.at[which, side(dx), chunk], packxrecv.at[z, side(dx), chunk]
                else:
                    src = packxedge.at[which, side(dx), edge, chunk]
                    land = packxedgerecv.at[z, side(dx), side(dy), chunk]
                (sides if dx else edges).append(remote(src, land, dx, dy, 0, land))
        return edges, sides

    def share_slab(chunk, which, both):
        for k in range(2):
            packedge[which, 0, 2 * chunk + k] = both[k][0:HALO]
            packedge[which, 1, 2 * chunk + k] = both[k][ny - HALO : ny]
        high = jnp.where(upper32, both[0], pltpu.roll(both[1], 96, axis=1))
        low = jnp.where(upper32, pltpu.roll(both[1], 32, axis=1), both[0])
        for k, value in ((0, high), (1, low)):
            packx[which, k, chunk] = value
            packxedge[which, k, 0, chunk] = value[0:HALO]
            packxedge[which, k, 1, chunk] = value[ny - HALO : ny]

    def relay_slabs(chunk):
        share_slab(chunk, 1, [packrecv[1 - gz, 2 * chunk + k] for k in range(2)])
        return start_slabs(chunk, 1)

    def pack_edges(c0, c1):
        for c in range(c0, c1):
            ysend[0, c] = field[c, own[0], OWNY : OWNY + HALO, :]
            ysend[1, c] = field[c, own[0], OWNY + ny - HALO : OWNY + ny, :]

    lane32 = lax.broadcasted_iota(jnp.int32, (ny, 128), 1)
    quad = lane32 // 4
    upper32 = lax.rem(lane32, 64) >= 32
    lift = 4 * (1 - gz)

    def pack_slab(chunk):
        both = []
        for group in (2 * chunk, 2 * chunk + 1):
            packed = jnp.zeros((ny, 128), F32)
            for part in range(4):
                comp = group * 4 + part
                if comp >= COMPS:
                    continue
                for i in range(nx):
                    base = (part // 2) * 64 + i * 8 + (part % 2) * 4
                    moved = pltpu.roll(field[comp, OWNX + i, own[1], :], base + lift, axis=1)
                    packed = jnp.where(quad == base // 4, moved, packed)
            pack[group] = packed
            packrecv[gz, group] = packed
            both.append(packed)
        share_slab(chunk, 0, both)

    loads["perm"].wait()
    loads["loss"].wait()
    for i in range(nx):
        loss = medium[1, i]
        field[KEEP, OWNX + i, OWNY : OWNY + ny, :] = (1.0 - loss) / (1.0 + loss)
        field[CURL, OWNX + i, OWNY : OWNY + ny, :] = 0.5 / (medium[0, i] * (1.0 + loss))
    loads["fe"].wait()
    loads["fm"].wait()
    pack_slab(0)
    pack_edges(0, FIRST)
    count_x = 3 - (gx == 0).astype(jnp.int32) - (gx == ngx - 1).astype(jnp.int32)
    count_y = 3 - (gy == 0).astype(jnp.int32) - (gy == ngy - 1).astype(jnp.int32)
    pl.semaphore_wait(barrier, count_x * count_y * 2 - 1 + len(apart))
    group_start(0, 0, gather1)
    first_z = start_along_z(0)
    first_waits, first_leaving = start_along_x(
        ((0, 3, HALO), (3, 4, HALO - 1), (4, 6, HALO), (KEEP, CURL + 1, HALO - 1)),
        ((0, 1, HALO - 1), (1, 3, HALO), (3, FIRST, HALO - 1)),
    )
    first_y = start_along_y(0, FIRST)
    first_slabs = start_slabs(0, 0)
    loads["ae"].wait()
    loads["am"].wait()
    pack_slab(1)
    pack_edges(FIRST, COMPS)
    loads["source"].wait()
    loads["wave"].wait()
    loads["cells"].wait()
    row = lax.broadcasted_iota(jnp.int32, (ROWS, 128), 0) + TOP
    lane = lax.broadcasted_iota(jnp.int32, (ROWS, 128), 1)
    row_y = row - OWNY + gy * ny
    hrow[...] = jnp.where(row_y >= 0, 0.5, 0.0)
    slab_x = lane // 8 - OWNX + gx * nx
    hslab[...] = jnp.where((row_y >= 0) & (slab_x >= 0), 0.5, 0.0)
    source = source_ref[0]
    total_y, total_z = ngy * ny, ngz * nz
    src_x = source // (total_y * total_z)
    src_y = lax.rem(source // total_z, total_y)
    src_z = lax.rem(source, total_z)
    in_row = row_y == src_y
    smask[...] = jnp.where(in_row & (lane + gz * nz == src_z), 1.0, 0.0)
    slab_z = lax.rem(lane, 8) + nz - HALO
    sslab[...] = jnp.where(in_row & (slab_x == src_x) & (slab_z == src_z), 1.0, 0.0)
    src_plane = src_x - gx * nx + OWNX

    cells = cells_ref[...]
    rec_x = cells // (total_y * total_z) - gx * nx + OWNX
    rec_y = lax.rem(cells // total_z, total_y) - gy * ny + OWNY - TOP
    rec_z = lax.rem(cells, total_z)
    in_x = (rec_x >= 0) & (rec_x < nx + 2 * HALO)
    in_y = (rec_y >= 0) & (rec_y < ROWS)
    rec_row = jnp.where(in_x & in_y, rec_x * ROWS + rec_y, -1)
    rec_lane = rec_z - gz * nz
    planes = nx + 2 * HALO - 2

    def build(i, _):
        ids = lax.broadcasted_iota(jnp.int32, (ROWS, nrec), 0) + (i + 1) * ROWS
        onehot[pl.ds(pl.multiple_of(i * ROWS, 16), ROWS), :] = jnp.where(ids == rec_row, 1.0, 0.0).astype(BF16)
        return 0

    lax.fori_loop(0, planes, build, 0)

    first_z()
    first_edges, first_sides = first_slabs
    edges_, sides_ = relay_slabs(0)
    first_edges, first_waits = first_edges + edges_, first_waits + first_sides + sides_
    for wait in first_y:
        wait()
    first_waits += relay_corners(0, FIRST)

    group_wait(0, 0, gather1)
    row_of_samples = gather1[0]
    for k in range(1, 16):
        row_of_samples = row_of_samples + gather1[k]
    gather2[i2] = row_of_samples
    group_start(1, 1, gather2)
    second_z = start_along_z(1)
    second_y = start_along_y(FIRST, COMPS)
    second_edges, second_waits = start_slabs(1, 0)
    second_x, second_leaving = start_along_x(
        ((8, 11, HALO), (11, 12, HALO - 1), (12, COMPS, HALO)),
        ((8, 9, HALO - 1), (9, 11, HALO), (11, COMPS, HALO - 1)),
    )
    second_waits += second_x

    lane_r = lax.broadcasted_iota(jnp.int32, (ROWS, nz), 1)

    def assemble(c0, c1, planes_):
        zeros = jnp.zeros((HALO, nz), F32)
        for c in range(c0, c1):
            for i in planes_:
                for ys in range(2):
                    if i < OWNX:
                        piece = corner[0, ys, c, i]
                    elif i < OWNX + nx:
                        piece = yrecv[ys, c, i - OWNX]
                    else:
                        piece = corner[1, ys, c, i - OWNX - nx]
                    if ys == 0:
                        field[c, i, TOP:OWNY, :] = jnp.concatenate([zeros, piece], axis=0)
                    else:
                        field[c, i, OWNY + ny : OWNY + ny + 8, :] = jnp.concatenate([piece, zeros], axis=0)

    every = list(range(nx + 2 * HALO))
    middle = every[OWNX : OWNX + nx]
    outside = every[:OWNX] + every[OWNX + nx :]

    lane_p = lax.broadcasted_iota(jnp.int32, (ROWS, 128), 1)
    deep = lax.rem(lane_p, 8) >= 4
    inside = (lane_p >= 32) & (lane_p < 96)
    upper = lax.rem(lane_p, 64) >= 32

    def assemble_slab(chunk, with_sides=True):
        zeros = jnp.zeros((HALO, 128), F32)

        def column(low, middle, high):
            return jnp.concatenate([zeros, low, middle, high, zeros], axis=0)

        sides = with_sides and [
            [
                column(
                    packxedgerecv[z, k, 0, chunk], packxrecv[z, k, chunk], packxedgerecv[z, k, 1, chunk]
                )
                for k in range(2)
            ]
            for z in range(2)
        ]
        for odd in range(2):
            group = 2 * chunk + odd
            centre, beside = [], []
            for z in range(2):
                centre.append(
                    column(packedgerecv[z, 0, group], packrecv[z, group], packedgerecv[z, 1, group])
                )
                if with_sides:
                    low, high = sides[z]
                    if odd:
                        low, high = pltpu.roll(low, 32, axis=1), pltpu.roll(high, 96, axis=1)
                    beside.append(jnp.where(upper, low, high))
            for part in range(4):
                comp = group * 4 + part
                if comp >= COMPS:
                    continue
                base = (part // 2) * 64 + (part % 2) * 4
                inner = [pltpu.roll(centre[z], (32 + 4 * z - base) % 128, axis=1) for z in range(2)]
                near = jnp.where(deep, inner[1], inner[0])
                far = 0.0
                if with_sides:
                    outer = [pltpu.roll(beside[z], (96 + 4 * z - base) % 128, axis=1) for z in range(2)]
                    far = jnp.where(deep, outer[1], outer[0])
                slab[comp, TOP : TOP + ROWS, :] = jnp.where(inside, near, far)

    up_keep = jnp.where(gz == 0, 1.0, 0.0)
    down_keep = jnp.where(gz == 0, 0.0, 1.0)
    def moved(window, by):
        return slice(window.start + by, window.stop + by)

    def magnetic_half(b, step, planes_):
        at = slice(TOP, TOP + ROWS) if step < STEPS else slice(TOP, OWNY + ny)
        mask_at = moved(at, -TOP)
        tall = at.stop - at.start
        last_lane = lax.broadcasted_iota(jnp.int32, (tall, nz), 1) == nz - 1
        for i in planes_:
            factor = hrow[mask_at]
            if i < OWNX:
                factor = factor * jnp.where(gx > 0, 1.0, 0.0)
            ex, ey, ez = field[b, i, at], field[b + 1, i, at], field[b + 2, i, at]
            turn = (nz - 1 - HALO - 8 * i) % 128

            def deeper(value, comp):
                edge = pltpu.roll(slab[comp, at], turn, axis=1) * up_keep
                return jnp.where(last_lane, edge, pltpu.roll(value, nz - 1, axis=1))

            field[b + 3, i, at] = field[b + 3, i, at] - factor * (
                (field[b + 2, i, moved(at, 1)] - ez) - (deeper(ey, b + 1) - ey)
            )
            field[b + 4, i, at] = field[b + 4, i, at] - factor * (
                (deeper(ex, b) - ex) - (field[b + 2, i + 1, at] - ez)
            )
            field[b + 5, i, at] = field[b + 5, i, at] - factor * (
                (field[b + 1, i + 1, at] - ey) - (field[b, i, moved(at, 1)] - ex)
            )
        factor = hslab[mask_at]
        ex, ey, ez = slab[b, at], slab[b + 1, at], slab[b + 2, at]

        def along_x(value):
            return pltpu.roll(value, 120, axis=1)

        def along_z(value):
            return pltpu.roll(value, 127, axis=1)

        slab[b + 3, at] = slab[b + 3, at] - factor * (
            (slab[b + 2, moved(at, 1)] - ez) - (along_z(ey) - ey)
        )
        slab[b + 4, at] = slab[b + 4, at] - factor * ((along_z(ex) - ex) - (along_x(ez) - ez))
        if step < STEPS:
            slab[b + 5, at] = slab[b + 5, at] - factor * (
                (along_x(ey) - ey) - (slab[b, moved(at, 1)] - ex)
            )

    def electric_half(b, step, planes_, extra, extra_slab):
        at = slice(TOP, TOP + ROWS) if step < STEPS else own[1]
        tall = at.stop - at.start
        first_lane = lax.broadcasted_iota(jnp.int32, (tall, nz), 1) == 0
        for i in planes_:
            keep, curl = field[KEEP, i, at], field[CURL, i, at]
            hx, hy, hz = field[b + 3, i, at], field[b + 4, i, at], field[b + 5, i, at]
            turn = (1 - HALO - 8 * i) % 128

            def shallower(value, comp):
                edge = pltpu.roll(slab[comp, at], turn, axis=1) * down_keep
                return jnp.where(first_lane, edge, pltpu.roll(value, 1, axis=1))

            field[b, i, at] = keep * field[b, i, at] + curl * (
                (hz - field[b + 5, i, moved(at, -1)]) - (hy - shallower(hy, b + 4))
            )
            field[b + 1, i, at] = keep * field[b + 1, i, at] + curl * (
                (hx - shallower(hx, b + 3)) - (hz - field[b + 5, i - 1, at])
            )
            field[b + 2, i, at] = (
                keep * field[b + 2, i, at]
                + curl * ((hy - field[b + 4, i - 1, at]) - (hx - field[b + 3, i, moved(at, -1)]))
                + extra(i, moved(at, -TOP))
            )
        if step == STEPS:
            return
        keep, curl = slab[KEEP, at], slab[CURL, at]
        hx, hy, hz = slab[b + 3, at], slab[b + 4, at], slab[b + 5, at]

        def along_x(value):
            return pltpu.roll(value, 8, axis=1)

        def along_z(value):
            return pltpu.roll(value, 1, axis=1)

        slab[b, at] = keep * slab[b, at] + curl * ((hz - slab[b + 5, moved(at, -1)]) - (hy - along_z(hy)))
        slab[b + 1, at] = keep * slab[b + 1, at] + curl * ((hx - along_z(hx)) - (hz - along_x(hz)))
        slab[b + 2, at] = (
            keep * slab[b + 2, at]
            + curl * ((hy - along_x(hy)) - (hx - slab[b + 3, moved(at, -1)]))
            + extra_slab()
        )

    def snapshot(n, planes_):
        for i in planes_:
            if i not in middle:
                continue
            k = i - OWNX
            for c in range(3):
                value = field[c, i, own[1], :]
                if n < STEPS:
                    snaps[n, c, k] = value
                if n:
                    change[n - 1, c, k] = value - snaps[n - 1, c, k]

    for wait in first_edges + first_leaving:
        wait()

    def pulse(step):
        return wave_ref[start + step - 1]

    def magnetic_planes(step):
        return every[step - 1 : nx + 2 * HALO - step]

    def electric_planes(step):
        return every[step : nx + 2 * HALO - step]

    def magnetic_inner(step):
        return middle[step - 1 : nx - step]

    def electric_inner(step):
        return middle[step : nx - step]

    def forward_electric(step, planes_):
        electric_half(
            0,
            step,
            planes_,
            lambda i, at: smask[at] * jnp.where(i == src_plane, pulse(step), 0.0),
            lambda: sslab[...] * pulse(step),
        )
        snapshot(step, planes_)

    def split(value):
        high = value.astype(BF16).astype(F32)
        return high, value - high

    contract = (((1,), (1,)), ((), ()))

    def inject(m):
        high, low = split(samples[STEPS - 1 - m])
        weights = jnp.concatenate(
            [jnp.where(at_lane, high, 0.0).astype(BF16), jnp.where(at_lane, low, 0.0).astype(BF16)],
            axis=0,
        )
        count = planes - 2 * m
        both = lax.dot_general(
            onehot[m * ROWS : (m + count) * ROWS, :], weights, contract, preferred_element_type=F32
        )
        inj[m, 1 + m : 1 + m + count] = (both[:, :nz] + both[:, nz:]).reshape(count, ROWS, nz)

    def inject_slab():
        rec_near = rec_x * 8 + rec_z - (nz - HALO)
        in_slab = in_x & (rec_z >= nz - HALO) & (rec_z < nz + HALO)
        slab_weights = jnp.where(lanes_of == jnp.where(in_slab, rec_near, -1), 1.0, 0.0).astype(BF16)
        at_row = lax.broadcasted_iota(jnp.int32, (ROWS, nrec), 0) == rec_y
        pieces = []
        for m in range(STEPS - 1):
            for value in split(samples[STEPS - 1 - m]):
                pieces.append(jnp.where(at_row, value, 0.0).astype(BF16))
        both = lax.dot_general(
            jnp.concatenate(pieces, axis=0), slab_weights, contract, preferred_element_type=F32
        )
        for m in range(STEPS - 1):
            at = 2 * m * ROWS
            injslab[m] = both[at : at + ROWS] + both[at + ROWS : at + 2 * ROWS]

    snapshot(0, middle)
    assemble(0, FIRST, middle)
    assemble_slab(0, False)
    for step in range(1, STEPS + 1):
        magnetic_half(0, step, magnetic_inner(step))
        forward_electric(step, electric_inner(step))
    for wait in first_waits:
        wait()
    assemble(0, FIRST, outside)
    assemble_slab(0)

    def magnetic_outer(step):
        magnetic_half(0, step, [i for i in magnetic_planes(step) if i not in magnetic_inner(step)])

    def electric_outer(step):
        forward_electric(step, [i for i in electric_planes(step) if i not in electric_inner(step)])

    for step in (1, 2):
        magnetic_outer(step)
        electric_outer(step)
    second_z()
    edges_, sides_ = relay_slabs(1)
    second_edges += edges_
    second_waits += sides_
    for wait in second_y:
        wait()
    second_waits += relay_corners(FIRST, COMPS)
    group_wait(1, 1, gather2)
    samples = [
        jnp.concatenate([gather2[k][m : m + 1] for k in range(16)], axis=1) for m in range(STEPS)
    ]
    lanes_of = lax.broadcasted_iota(jnp.int32, (nz, nrec), 0)
    at_lane = lanes_of == rec_lane
    inject(0)
    magnetic_outer(3)
    inject(1)
    electric_outer(3)
    inject(2)
    magnetic_outer(4)
    inject(3)
    inject_slab()
    electric_outer(4)

    square = [jnp.zeros((ny, nz), F32)]

    def adjoint_step(step, magnetic_at, electric_at):
        magnetic_half(FIRST, step, magnetic_at)
        electric_half(
            FIRST,
            step,
            electric_at,
            lambda i, at: inj[step - 1, i, at],
            lambda: injslab[step - 1],
        )
        for i in electric_at:
            if i not in middle:
                continue
            k = i - OWNX
            term = None
            for c in range(3):
                product = change[STEPS - step, c, k] * field[FIRST + c, i, own[1], :]
                term = product if term is None else term + product
            value = term if step == 1 else out_ref[k] + term
            if step == STEPS:
                value = -value / medium[0, k]
                square[0] = square[0] + value * value
            out_ref[k] = value

    for wait in second_edges + second_waits + second_leaving:
        wait()
    assemble(FIRST, COMPS, every)
    assemble_slab(1)
    for step in range(1, STEPS + 1):
        adjoint_step(step, magnetic_planes(step), electric_planes(step))
    square = square[0]
    red1[groups[2][0]] = jnp.sum(square, axis=0, keepdims=True)
    group_start(2, 2, red1)
    group_wait(2, 2, red1)
    total = red1[0]
    for k in range(1, 16):
        total = total + red1[k]
    red2[groups[3][0]] = total
    group_start(3, 3, red2)
    group_wait(3, 3, red2)
    total = red2[0]
    for k in range(1, 16):
        total = total + red2[k]
    total = jnp.sum(total, axis=1, keepdims=True)
    cells_in_all = ngx * nx * ngy * ny * ngz * nz
    rms = jnp.sqrt(total / cells_in_all + 1e-06)
    rms_ref[...] = rms
    wide = jnp.broadcast_to(rms, (ny, nz))
    for i in range(nx):
        out_ref[i] = out_ref[i] / wide
    for cond, copy in sends:
        guarded(cond, copy.wait_send)
    group_drain(0, 0, gather1)
    group_drain(1, 1, gather2)
    group_drain(2, 2, red1)
    group_drain(3, 3, red2)


def solution(mesh):
    ngx, ngy, ngz = mesh.shape["gx"], mesh.shape["gy"], mesh.shape["gz"]

    def per_device(
        permittivity,
        loss,
        fwd_electric,
        fwd_magnetic,
        adj_electric,
        adj_magnetic,
        wavelet,
        residuals,
        source_cell,
        receiver_cells,
        start_step,
    ):
        nx, ny, nz = permittivity.shape
        nrec, trace = receiver_cells.shape[0], residuals.shape[1]
        planes = nx + 2 * HALO
        dims = (ngx, ngy, ngz, nx, ny, nz, nrec)
        hbm = pl.BlockSpec(memory_space=pltpu.HBM)
        vmem = pl.BlockSpec(memory_space=pltpu.VMEM)
        direction, rms = pl.pallas_call(
            functools.partial(kernel, dims),
            out_shape=(
                jax.ShapeDtypeStruct((nx, ny, nz), F32),
                jax.ShapeDtypeStruct((1, 1), F32),
            ),
            in_specs=[hbm] * 11,
            out_specs=(vmem, vmem),
            scratch_shapes=[
                pltpu.VMEM((COMPS, planes, 64, nz), F32),
                pltpu.VMEM((2, nx, ny, nz), F32),
                pltpu.VMEM((2, COMPS, nx, HALO, nz), F32),
                pltpu.VMEM((2, COMPS, nx, HALO, nz), F32),
                pltpu.VMEM((2, 2, COMPS, HALO, HALO, nz), F32),
                pltpu.VMEM((nrec // (ngx * ngy * ngz), trace), F32),
                pltpu.VMEM((1, nrec), jnp.int32),
                pltpu.SMEM((trace,), F32),
                pltpu.SMEM((1,), jnp.int32),
                pltpu.SMEM((1,), jnp.int32),
                pltpu.VMEM((4, ny, 128), F32),
                pltpu.VMEM((2, 2, 4, HALO, 128), F32),
                pltpu.VMEM((2, 2, 2, ny, 128), F32),
                pltpu.VMEM((2, 2, 2, 2, HALO, 128), F32),
                pltpu.VMEM((2, 4, ny, 128), F32),
                pltpu.VMEM((2, 2, 4, HALO, 128), F32),
                pltpu.VMEM((2, 2, 2, ny, 128), F32),
                pltpu.VMEM((2, 2, 2, 2, HALO, 128), F32),
                pltpu.VMEM((COMPS, 64, 128), F32),
                pltpu.VMEM((STEPS, 3, nx, ny, nz), F32),
                pltpu.VMEM((STEPS, 3, nx, ny, nz), F32),
                pltpu.VMEM((ROWS, 128), F32),
                pltpu.VMEM((ROWS, 128), F32),
                pltpu.VMEM((ROWS, 128), F32),
                pltpu.VMEM((ROWS, 128), F32),
                pltpu.VMEM(((planes - 2) * ROWS, nrec), BF16),
                pltpu.VMEM((STEPS, planes, ROWS, nz), F32),
                pltpu.VMEM((STEPS - 1, ROWS, 128), F32),
                pltpu.VMEM((16, STEPS, 128), F32),
                pltpu.VMEM((16, STEPS, 128), F32),
                pltpu.VMEM((16, 1, 128), F32),
                pltpu.VMEM((16, 1, 128), F32),
                pltpu.SemaphoreType.DMA((11,)),
                pltpu.SemaphoreType.DMA((59,)),
                pltpu.SemaphoreType.DMA((59,)),
                pltpu.SemaphoreType.DMA((4, 15)),
                pltpu.SemaphoreType.DMA((4, 16)),
            ],
            compiler_params=pltpu.CompilerParams(
                collective_id=0, has_side_effects=True, vmem_limit_bytes=60 * 1024 * 1024
            ),
            name="window",
        )(
            permittivity,
            loss,
            fwd_electric,
            fwd_magnetic,
            adj_electric,
            adj_magnetic,
            residuals,
            receiver_cells.reshape(1, nrec),
            wavelet,
            source_cell,
            start_step,
        )
        return direction, rms.reshape(())

    field_spec = P(None, "gx", "gy", "gz")
    block_spec = P("gx", "gy", "gz")
    return jax.shard_map(
        per_device,
        mesh=mesh,
        in_specs=(
            block_spec,
            block_spec,
            field_spec,
            field_spec,
            field_spec,
            field_spec,
            P(),
            P(("gx", "gy", "gz"), None),
            P(),
            P(),
            P(),
        ),
        out_specs=(block_spec, P()),
        check_vma=False,
    )
```

```python
import functools

import jax
import jax.numpy as jnp
from jax import lax
from jax.experimental import pallas as pl
from jax.experimental.pallas import tpu as pltpu
from jax.sharding import PartitionSpec as P

STEPS = 4
MESH = pl.DeviceIdType.MESH
F32 = jnp.float32
BF16 = jnp.bfloat16

HALO = 4
OWNX = HALO
OWNY = 16
TOP = 8
ROWS = 48
KEEP, CURL = 6, 7
FIRST = 8
COMPS = 14


def kernel(
    dims,
    perm_hbm,
    loss_hbm,
    fe_hbm,
    fm_hbm,
    ae_hbm,
    am_hbm,
    res_hbm,
    cells_hbm,
    wave_hbm,
    source_hbm,
    start_hbm,
    out_ref,
    rms_ref,
    field,
    medium,
    ysend,
    yrecv,
    corner,
    res_ref,
    cells_ref,
    wave_ref,
    source_ref,
    start_ref,
    pack,
    packedge,
    packx,
    packxedge,
    packrecv,
    packedgerecv,
    packxrecv,
    packxedgerecv,
    slab,
    snaps,
    change,
    hrow,
    hslab,
    smask,
    sslab,
    onehot,
    inj,
    injslab,
    gather1,
    gather2,
    red1,
    red2,
    load_sem,
    halo_send,
    halo_recv,
    group_send,
    group_recv,
):
    ngx, ngy, ngz, nx, ny, nz, nrec = dims
    gx, gy, gz = lax.axis_index("gx"), lax.axis_index("gy"), lax.axis_index("gz")
    own = (slice(OWNX, OWNX + nx), slice(OWNY, OWNY + ny))

    loads = {}
    for k, (name, src, dst) in enumerate(
        (
            ("fe", fe_hbm, field.at[0:3, own[0], own[1]]),
            ("fm", fm_hbm, field.at[3:6, own[0], own[1]]),
            ("perm", perm_hbm, medium.at[0]),
            ("loss", loss_hbm, medium.at[1]),
            ("start", start_hbm, start_ref),
            ("res", res_hbm, res_ref),
            ("ae", ae_hbm, field.at[8:11, own[0], own[1]]),
            ("am", am_hbm, field.at[11:14, own[0], own[1]]),
            ("source", source_hbm, source_ref),
            ("wave", wave_hbm, wave_ref),
            ("cells", cells_hbm, cells_ref),
        )
    ):
        loads[name] = pltpu.make_async_copy(src, dst, load_sem.at[k])
        loads[name].start()

    def there(dx, dy):
        ok = []
        if dx:
            ok.append((gx + dx >= 0) & (gx + dx < ngx))
        if dy:
            ok.append((gy + dy >= 0) & (gy + dy < ngy))
        if not ok:
            return None
        return functools.reduce(jnp.logical_and, ok)

    def guarded(cond, fn):
        if cond is None:
            fn()
        else:
            pl.when(cond)(fn)

    x_low, z_chip = gy // 8, lax.rem(gy, 8)
    y_chip, core = gx // 2, lax.rem(gx, 2)

    def device(z, x_hi, y, core, x_lo):
        return {"gx": y * 2 + core, "gy": x_lo * 8 + z, "gz": x_hi}

    groups = (
        (z_chip * 2 + gz, lambda k: device(k // 2, lax.rem(k, 2), y_chip, core, x_low)),
        (gx * 2 + x_low, lambda k: device(z_chip, gz, k // 4, lax.rem(k // 2, 2), lax.rem(k, 2))),
        (
            (gz * 2 + x_low) * 4 + y_chip,
            lambda k: device(z_chip, k // 8, lax.rem(k, 4), core, lax.rem(k // 4, 2)),
        ),
        (z_chip * 2 + core, lambda k: device(k // 2, gz, y_chip, lax.rem(k, 2), x_low)),
    )
    i1, i2 = groups[0][0], groups[1][0]
    hops = (
        lambda k: min(k // 2, 8 - k // 2) + 2 * (k % 2),
        lambda k: min(k // 4, 4 - k // 4) + k % 2,
        lambda k: min(k // 4, 4 - k // 4) + min(k % 4, 4 - k % 4),
        lambda k: min(k // 2, 8 - k // 2),
    )
    orders = [sorted(range(1, 16), key=lambda k, far=far: -far(k)) for far in hops]

    barrier = pltpu.get_barrier_semaphore()
    apart = sorted(
        {(dz, dh, 0, 0, 0) for dz in range(8) for dh in range(2)}
        | {(0, 0, dy, dc, dl) for dy in range(4) for dc in range(2) for dl in range(2)}
        | {(0, dh, dy, 0, dl) for dh in range(2) for dy in range(4) for dl in range(2)}
        | {(dz, 0, 0, dc, 0) for dz in range(8) for dc in range(2)}
    )[1:]
    apart.sort(key=lambda o: -(min(o[0], 8 - o[0]) + 2 * o[1] + min(o[2], 4 - o[2]) + o[4]))
    for dz, dh, dy, dc, dl in apart:
        pl.semaphore_signal(
            barrier,
            inc=1,
            device_id=device(
                lax.rem(z_chip + dz, 8),
                lax.rem(gz + dh, 2),
                lax.rem(y_chip + dy, 4),
                lax.rem(core + dc, 2),
                lax.rem(x_low + dl, 2),
            ),
            device_id_type=MESH,
        )
    for dx in (-1, 0, 1):
        for dy in (-1, 0, 1):
            for dz in (0, 1):
                if dx or dy or dz:
                    peer = {"gx": gx + dx, "gy": gy + dy, "gz": gz if dz == 0 else 1 - gz}
                    guarded(
                        there(dx, dy),
                        lambda peer=peer: pl.semaphore_signal(
                            barrier, inc=1, device_id=peer, device_id_type=MESH
                        ),
                    )

    def clear_planes(low):
        def body(c, _):
            field[c, low : low + HALO, OWNY : OWNY + ny, :] = jnp.zeros((HALO, ny, nz), F32)
            return 0

        lax.fori_loop(0, COMPS, body, 0)

    pl.when(gx == 0)(lambda: clear_planes(0))
    pl.when(gx == ngx - 1)(lambda: clear_planes(OWNX + nx))

    def clear(ref):
        ref[...] = jnp.zeros(ref.shape, F32)

    def clear_loop(ref):
        def body(c, _):
            ref[c] = jnp.zeros(ref.shape[1:], F32)
            return 0

        lax.fori_loop(0, ref.shape[0], body, 0)

    for ys, dy in ((0, -1), (1, 1)):
        missing_y = (gy + dy < 0) | (gy + dy >= ngy)
        pl.when(missing_y)(lambda ys=ys: clear_loop(yrecv.at[ys]))
        for xs, dx in ((0, -1), (1, 1)):
            missing = missing_y | (gx + dx < 0) | (gx + dx >= ngx)
            pl.when(missing)(lambda xs=xs, ys=ys: clear_loop(corner.at[xs, ys]))
        for z in range(2):
            pl.when(missing_y)(lambda z=z, ys=ys: clear(packedgerecv.at[z, ys]))
            for xs, dx in ((0, -1), (1, 1)):
                missing = missing_y | (gx + dx < 0) | (gx + dx >= ngx)
                pl.when(missing)(lambda z=z, xs=xs, ys=ys: clear(packxedgerecv.at[z, xs, ys]))
    for xs, dx in ((0, -1), (1, 1)):
        missing = (gx + dx < 0) | (gx + dx >= ngx)
        for z in range(2):
            pl.when(missing)(lambda z=z, xs=xs: clear(packxrecv.at[z, xs]))

    loads["start"].wait()
    loads["res"].wait()
    start = start_ref[0]
    lane8 = lax.broadcasted_iota(jnp.int32, (8, 128), 1)
    sub8 = lax.broadcasted_iota(jnp.int32, (8, 128), 0)

    time = lax.broadcasted_iota(jnp.int32, res_ref.shape, 1)
    rows = []
    for m in range(STEPS):
        column = jnp.sum(jnp.where(time == start + m, res_ref[...], 0.0), axis=1, keepdims=True)
        spread = jnp.where(lane8 - i1 * 8 == sub8, jnp.broadcast_to(column, (8, 128)), 0.0)
        rows.append(jnp.sum(spread, axis=0, keepdims=True))
    gather1[i1] = jnp.concatenate(rows, axis=0)

    def group_copy(round_, which, ref, step):
        mine, member = groups[which]
        peer = lax.rem(mine + step, 16)
        return pltpu.make_async_remote_copy(
            src_ref=ref.at[mine],
            dst_ref=ref.at[mine],
            send_sem=group_send.at[round_, step - 1],
            recv_sem=group_recv.at[round_, mine],
            device_id=member(peer),
            device_id_type=MESH,
        )

    def group_arrival(round_, which, ref, step):
        mine, member = groups[which]
        peer = lax.rem(mine + step, 16)
        return pltpu.make_async_remote_copy(
            src_ref=ref.at[mine],
            dst_ref=ref.at[peer],
            send_sem=group_send.at[round_, step - 1],
            recv_sem=group_recv.at[round_, peer],
            device_id=member(peer),
            device_id_type=MESH,
        )

    def group_start(round_, which, ref):
        for step in orders[which]:
            group_copy(round_, which, ref, step).start()

    def group_wait(round_, which, ref):
        for step in range(1, 16):
            group_arrival(round_, which, ref, step).wait_recv()

    def group_drain(round_, which, ref):
        for step in range(1, 16):
            group_copy(round_, which, ref, step).wait_send()

    sends = []
    number = [0]

    def remote(src, dst, dx, dy, dz, back, also=None):
        k = number[0]
        number[0] += 1

        def make(landing):
            return pltpu.make_async_remote_copy(
                src_ref=src,
                dst_ref=landing,
                send_sem=halo_send.at[k],
                recv_sem=halo_recv.at[k],
                device_id={"gx": gx + dx, "gy": gy + dy, "gz": gz if dz == 0 else 1 - gz},
                device_id_type=MESH,
            )

        go, come = there(dx, dy), there(-dx, -dy)
        if also is not None:
            go, come = go & also, come & also
        guarded(go, lambda: make(dst).start())
        sends.append((go, make(dst)))
        return lambda: guarded(come, lambda: make(back).wait_recv())

    def side(d):
        return 0 if d == 1 else 1

    def span(low, count):
        return slice(low, low + count)

    def start_along_x(low_parts, high_parts):
        waits, leaving = [], []
        rows_ = slice(OWNY, OWNY + ny)
        for dx, parts in ((1, low_parts), (-1, high_parts)):
            for first, last, depth in parts:
                if dx == 1:
                    source, target = span(OWNX + nx - depth, depth), span(HALO - depth, depth)
                else:
                    source, target = span(OWNX, depth), span(OWNX + nx, depth)
                landing = field.at[first:last, target, rows_]
                waits.append(remote(field.at[first:last, source, rows_], landing, dx, 0, 0, landing))
                cond, copy = sends.pop()
                leaving.append(lambda cond=cond, copy=copy: guarded(cond, copy.wait_send))
        return waits, leaving

    def start_along_y(c0, c1):
        waits = []
        for dy in (1, -1):
            landing = yrecv.at[side(dy), c0:c1]
            waits.append(remote(ysend.at[1 if dy == 1 else 0, c0:c1], landing, 0, dy, 0, landing))
        return waits

    def relay_corners(c0, c1):
        waits = []
        for ys, dy in ((0, -1), (1, 1)):
            for dx in (1, -1):
                depth = HALO - 1 if dx == -dy else HALO
                part = span(nx - depth, depth) if dx == 1 else span(0, depth)
                place = span(HALO - depth, depth) if dx == 1 else span(0, depth)
                landing = corner.at[side(dx), ys, c0:c1, place]
                waits.append(
                    remote(yrecv.at[ys, c0:c1, part], landing, dx, 0, 0, landing, there(0, dy))
                )
        return waits

    def start_along_z(chunk):
        groups_ = span(2 * chunk, 2)
        return remote(pack.at[groups_], packrecv.at[gz, groups_], 0, 0, 1, packrecv.at[1 - gz, groups_])

    def start_slabs(chunk, which):
        z = gz if which == 0 else 1 - gz
        edges, sides = [], []
        groups_ = span(2 * chunk, 2)
        for dx in (0, 1, -1):
            for dy in (0, 1, -1):
                if not (dx or dy):
                    continue
                edge = 1 if dy == 1 else 0
                if dx == 0:
                    src, land = packedge.at[which, edge, groups_], packedgerecv.at[z, side(dy), groups_]
                elif dy == 0:
                    src, land = packx.at[which, side(dx), chunk], packxrecv.at[z, side(dx), chunk]
                else:
                    src = packxedge.at[which, side(dx), edge, chunk]
                    land = packxedgerecv.at[z, side(dx), side(dy), chunk]
                (sides if dx else edges).append(remote(src, land, dx, dy, 0, land))
        return edges, sides

    def share_slab(chunk, which, both):
        for k in range(2):
            packedge[which, 0, 2 * chunk + k] = both[k][0:HALO]
            packedge[which, 1, 2 * chunk + k] = both[k][ny - HALO : ny]
        high = jnp.where(upper32, both[0], pltpu.roll(both[1], 96, axis=1))
        low = jnp.where(upper32, pltpu.roll(both[1], 32, axis=1), both[0])
        for k, value in ((0, high), (1, low)):
            packx[which, k, chunk] = value
            packxedge[which, k, 0, chunk] = value[0:HALO]
            packxedge[which, k, 1, chunk] = value[ny - HALO : ny]

    def relay_slabs(chunk):
        share_slab(chunk, 1, [packrecv[1 - gz, 2 * chunk + k] for k in range(2)])
        return start_slabs(chunk, 1)

    def pack_edges(c0, c1):
        for c in range(c0, c1):
            ysend[0, c] = field[c, own[0], OWNY : OWNY + HALO, :]
            ysend[1, c] = field[c, own[0], OWNY + ny - HALO : OWNY + ny, :]

    lane32 = lax.broadcasted_iota(jnp.int32, (ny, 128), 1)
    quad = lane32 // 4
    upper32 = lax.rem(lane32, 64) >= 32
    lift = 4 * (1 - gz)

    def pack_slab(chunk):
        both = []
        for group in (2 * chunk, 2 * chunk + 1):
            packed = jnp.zeros((ny, 128), F32)
            for part in range(4):
                comp = group * 4 + part
                if comp >= COMPS:
                    continue
                for i in range(nx):
                    base = (part // 2) * 64 + i * 8 + (part % 2) * 4
                    turn = lax.rem(base + lift, 128)
                    moved = pltpu.roll(field[comp, OWNX + i, own[1], :], turn, axis=1)
                    packed = jnp.where(quad == base // 4, moved, packed)
            pack[group] = packed
            packrecv[gz, group] = packed
            both.append(packed)
        share_slab(chunk, 0, both)

    loads["perm"].wait()
    loads["loss"].wait()
    for i in range(nx):
        loss = medium[1, i]
        field[KEEP, OWNX + i, OWNY : OWNY + ny, :] = (1.0 - loss) / (1.0 + loss)
        field[CURL, OWNX + i, OWNY : OWNY + ny, :] = 0.5 / (medium[0, i] * (1.0 + loss))
    loads["fe"].wait()
    loads["fm"].wait()
    pack_slab(0)
    pack_edges(0, FIRST)
    count_x = 3 - (gx == 0).astype(jnp.int32) - (gx == ngx - 1).astype(jnp.int32)
    count_y = 3 - (gy == 0).astype(jnp.int32) - (gy == ngy - 1).astype(jnp.int32)
    pl.semaphore_wait(barrier, count_x * count_y * 2 - 1 + len(apart))
    group_start(0, 0, gather1)
    first_z = start_along_z(0)
    first_waits, first_leaving = start_along_x(
        ((0, 3, HALO), (3, 4, HALO - 1), (4, 6, HALO), (KEEP, CURL + 1, HALO - 1)),
        ((0, 1, HALO - 1), (1, 3, HALO), (3, FIRST, HALO - 1)),
    )
    first_y = start_along_y(0, FIRST)
    first_slabs = start_slabs(0, 0)
    loads["ae"].wait()
    loads["am"].wait()
    pack_slab(1)
    pack_edges(FIRST, COMPS)
    loads["source"].wait()
    loads["wave"].wait()
    loads["cells"].wait()
    row = lax.broadcasted_iota(jnp.int32, (ROWS, 128), 0) + TOP
    lane = lax.broadcasted_iota(jnp.int32, (ROWS, 128), 1)
    row_y = row - OWNY + gy * ny
    hrow[...] = jnp.where(row_y >= 0, 0.5, 0.0)
    slab_x = lane // 8 - OWNX + gx * nx
    hslab[...] = jnp.where((row_y >= 0) & (slab_x >= 0), 0.5, 0.0)
    source = source_ref[0]
    total_y, total_z = ngy * ny, ngz * nz
    src_x = source // (total_y * total_z)
    src_y = lax.rem(source // total_z, total_y)
    src_z = lax.rem(source, total_z)
    in_row = row_y == src_y
    smask[...] = jnp.where(in_row & (lane + gz * nz == src_z), 1.0, 0.0)
    slab_z = lax.rem(lane, 8) + nz - HALO
    sslab[...] = jnp.where(in_row & (slab_x == src_x) & (slab_z == src_z), 1.0, 0.0)
    src_plane = src_x - gx * nx + OWNX

    cells = cells_ref[...]
    rec_x = cells // (total_y * total_z) - gx * nx + OWNX
    rec_y = lax.rem(cells // total_z, total_y) - gy * ny + OWNY - TOP
    rec_z = lax.rem(cells, total_z)
    in_x = (rec_x >= 0) & (rec_x < nx + 2 * HALO)
    in_y = (rec_y >= 0) & (rec_y < ROWS)
    rec_row = jnp.where(in_x & in_y, rec_x * ROWS + rec_y, -1)
    rec_lane = rec_z - gz * nz
    planes = nx + 2 * HALO - 2

    def build(i, _):
        ids = lax.broadcasted_iota(jnp.int32, (ROWS, nrec), 0) + (i + 1) * ROWS
        onehot[pl.ds(pl.multiple_of(i * ROWS, 16), ROWS), :] = jnp.where(ids == rec_row, 1.0, 0.0).astype(BF16)
        return 0

    lax.fori_loop(0, planes, build, 0)

    first_z()
    first_edges, first_sides = first_slabs
    edges_, sides_ = relay_slabs(0)
    first_edges, first_waits = first_edges + edges_, first_waits + first_sides + sides_
    for wait in first_y:
        wait()
    first_waits += relay_corners(0, FIRST)

    group_wait(0, 0, gather1)
    row_of_samples = gather1[0]
    for k in range(1, 16):
        row_of_samples = row_of_samples + gather1[k]
    gather2[i2] = row_of_samples
    group_start(1, 1, gather2)
    second_z = start_along_z(1)
    second_y = start_along_y(FIRST, COMPS)
    second_edges, second_waits = start_slabs(1, 0)
    second_x, second_leaving = start_along_x(
        ((8, 11, HALO), (11, 12, HALO - 1), (12, COMPS, HALO)),
        ((8, 9, HALO - 1), (9, 11, HALO), (11, COMPS, HALO - 1)),
    )
    second_waits += second_x

    lane_r = lax.broadcasted_iota(jnp.int32, (ROWS, nz), 1)

    def assemble(c0, c1, planes_):
        zeros = jnp.zeros((HALO, nz), F32)
        for c in range(c0, c1):
            for i in planes_:
                for ys in range(2):
                    if i < OWNX:
                        piece = corner[0, ys, c, i]
                    elif i < OWNX + nx:
                        piece = yrecv[ys, c, i - OWNX]
                    else:
                        piece = corner[1, ys, c, i - OWNX - nx]
                    if ys == 0:
                        field[c, i, TOP:OWNY, :] = jnp.concatenate([zeros, piece], axis=0)
                    else:
                        field[c, i, OWNY + ny : OWNY + ny + 8, :] = jnp.concatenate([piece, zeros], axis=0)

    every = list(range(nx + 2 * HALO))
    middle = every[OWNX : OWNX + nx]
    outside = every[:OWNX] + every[OWNX + nx :]

    lane_p = lax.broadcasted_iota(jnp.int32, (ROWS, 128), 1)
    deep = lax.rem(lane_p, 8) >= 4
    inside = (lane_p >= 32) & (lane_p < 96)
    upper = lax.rem(lane_p, 64) >= 32

    def assemble_slab(chunk, with_sides=True):
        zeros = jnp.zeros((HALO, 128), F32)

        def column(low, middle, high):
            return jnp.concatenate([zeros, low, middle, high, zeros], axis=0)

        sides = with_sides and [
            [
                column(
                    packxedgerecv[z, k, 0, chunk], packxrecv[z, k, chunk], packxedgerecv[z, k, 1, chunk]
                )
                for k in range(2)
            ]
            for z in range(2)
        ]
        for odd in range(2):
            group = 2 * chunk + odd
            centre, beside = [], []
            for z in range(2):
                centre.append(
                    column(packedgerecv[z, 0, group], packrecv[z, group], packedgerecv[z, 1, group])
                )
                if with_sides:
                    low, high = sides[z]
                    if odd:
                        low, high = pltpu.roll(low, 32, axis=1), pltpu.roll(high, 96, axis=1)
                    beside.append(jnp.where(upper, low, high))
            for part in range(4):
                comp = group * 4 + part
                if comp >= COMPS:
                    continue
                base = (part // 2) * 64 + (part % 2) * 4
                inner = [pltpu.roll(centre[z], (32 + 4 * z - base) % 128, axis=1) for z in range(2)]
                near = jnp.where(deep, inner[1], inner[0])
                far = 0.0
                if with_sides:
                    outer = [pltpu.roll(beside[z], (96 + 4 * z - base) % 128, axis=1) for z in range(2)]
                    far = jnp.where(deep, outer[1], outer[0])
                slab[comp, TOP : TOP + ROWS, :] = jnp.where(inside, near, far)

    up_keep = jnp.where(gz == 0, 1.0, 0.0)
    down_keep = jnp.where(gz == 0, 0.0, 1.0)
    def moved(window, by):
        return slice(window.start + by, window.stop + by)

    def magnetic_half(b, step, planes_):
        at = slice(TOP, TOP + ROWS) if step < STEPS else slice(TOP, OWNY + ny)
        mask_at = moved(at, -TOP)
        tall = at.stop - at.start
        last_lane = lax.broadcasted_iota(jnp.int32, (tall, nz), 1) == nz - 1
        for i in planes_:
            factor = hrow[mask_at]
            if i < OWNX:
                factor = factor * jnp.where(gx > 0, 1.0, 0.0)
            ex, ey, ez = field[b, i, at], field[b + 1, i, at], field[b + 2, i, at]
            turn = (nz - 1 - HALO - 8 * i) % 128

            def deeper(value, comp):
                edge = pltpu.roll(slab[comp, at], turn, axis=1) * up_keep
                return jnp.where(last_lane, edge, pltpu.roll(value, nz - 1, axis=1))

            field[b + 3, i, at] = field[b + 3, i, at] - factor * (
                (field[b + 2, i, moved(at, 1)] - ez) - (deeper(ey, b + 1) - ey)
            )
            field[b + 4, i, at] = field[b + 4, i, at] - factor * (
                (deeper(ex, b) - ex) - (field[b + 2, i + 1, at] - ez)
            )
            field[b + 5, i, at] = field[b + 5, i, at] - factor * (
                (field[b + 1, i + 1, at] - ey) - (field[b, i, moved(at, 1)] - ex)
            )
        factor = hslab[mask_at]
        ex, ey, ez = slab[b, at], slab[b + 1, at], slab[b + 2, at]

        def along_x(value):
            return pltpu.roll(value, 120, axis=1)

        def along_z(value):
            return pltpu.roll(value, 127, axis=1)

        slab[b + 3, at] = slab[b + 3, at] - factor * (
            (slab[b + 2, moved(at, 1)] - ez) - (along_z(ey) - ey)
        )
        slab[b + 4, at] = slab[b + 4, at] - factor * ((along_z(ex) - ex) - (along_x(ez) - ez))
        if step < STEPS:
            slab[b + 5, at] = slab[b + 5, at] - factor * (
                (along_x(ey) - ey) - (slab[b, moved(at, 1)] - ex)
            )

    def electric_half(b, step, planes_, extra, extra_slab):
        at = slice(TOP, TOP + ROWS) if step < STEPS else own[1]
        tall = at.stop - at.start
        first_lane = lax.broadcasted_iota(jnp.int32, (tall, nz), 1) == 0
        for i in planes_:
            keep, curl = field[KEEP, i, at], field[CURL, i, at]
            hx, hy, hz = field[b + 3, i, at], field[b + 4, i, at], field[b + 5, i, at]
            turn = (1 - HALO - 8 * i) % 128

            def shallower(value, comp):
                edge = pltpu.roll(slab[comp, at], turn, axis=1) * down_keep
                return jnp.where(first_lane, edge, pltpu.roll(value, 1, axis=1))

            field[b, i, at] = keep * field[b, i, at] + curl * (
                (hz - field[b + 5, i, moved(at, -1)]) - (hy - shallower(hy, b + 4))
            )
            field[b + 1, i, at] = keep * field[b + 1, i, at] + curl * (
                (hx - shallower(hx, b + 3)) - (hz - field[b + 5, i - 1, at])
            )
            field[b + 2, i, at] = (
                keep * field[b + 2, i, at]
                + curl * ((hy - field[b + 4, i - 1, at]) - (hx - field[b + 3, i, moved(at, -1)]))
                + extra(i, moved(at, -TOP))
            )
        if step == STEPS:
            return
        keep, curl = slab[KEEP, at], slab[CURL, at]
        hx, hy, hz = slab[b + 3, at], slab[b + 4, at], slab[b + 5, at]

        def along_x(value):
            return pltpu.roll(value, 8, axis=1)

        def along_z(value):
            return pltpu.roll(value, 1, axis=1)

        slab[b, at] = keep * slab[b, at] + curl * ((hz - slab[b + 5, moved(at, -1)]) - (hy - along_z(hy)))
        slab[b + 1, at] = keep * slab[b + 1, at] + curl * ((hx - along_z(hx)) - (hz - along_x(hz)))
        slab[b + 2, at] = (
            keep * slab[b + 2, at]
            + curl * ((hy - along_x(hy)) - (hx - slab[b + 3, moved(at, -1)]))
            + extra_slab()
        )

    def snapshot(n, planes_):
        for i in planes_:
            if i not in middle:
                continue
            k = i - OWNX
            for c in range(3):
                value = field[c, i, own[1], :]
                if n < STEPS:
                    snaps[n, c, k] = value
                if n:
                    change[n - 1, c, k] = value - snaps[n - 1, c, k]

    for wait in first_edges + first_leaving:
        wait()

    def pulse(step):
        return wave_ref[start + step - 1]

    def magnetic_planes(step):
        return every[step - 1 : nx + 2 * HALO - step]

    def electric_planes(step):
        return every[step : nx + 2 * HALO - step]

    def magnetic_inner(step):
        return middle[step - 1 : nx - step]

    def electric_inner(step):
        return middle[step : nx - step]

    def forward_electric(step, planes_):
        electric_half(
            0,
            step,
            planes_,
            lambda i, at: smask[at] * jnp.where(i == src_plane, pulse(step), 0.0),
            lambda: sslab[...] * pulse(step),
        )
        snapshot(step, planes_)

    def split(value):
        high = value.astype(BF16).astype(F32)
        return high, value - high

    contract = (((1,), (1,)), ((), ()))

    def inject(m):
        high, low = split(samples[STEPS - 1 - m])
        weights = jnp.concatenate(
            [jnp.where(at_lane, high, 0.0).astype(BF16), jnp.where(at_lane, low, 0.0).astype(BF16)],
            axis=0,
        )
        count = planes - 2 * m
        both = lax.dot_general(
            onehot[m * ROWS : (m + count) * ROWS, :], weights, contract, preferred_element_type=F32
        )
        inj[m, 1 + m : 1 + m + count] = (both[:, :nz] + both[:, nz:]).reshape(count, ROWS, nz)

    def inject_slab():
        rec_near = rec_x * 8 + rec_z - (nz - HALO)
        in_slab = in_x & (rec_z >= nz - HALO) & (rec_z < nz + HALO)
        slab_weights = jnp.where(lanes_of == jnp.where(in_slab, rec_near, -1), 1.0, 0.0).astype(BF16)
        at_row = lax.broadcasted_iota(jnp.int32, (ROWS, nrec), 0) == rec_y
        pieces = []
        for m in range(STEPS - 1):
            for value in split(samples[STEPS - 1 - m]):
                pieces.append(jnp.where(at_row, value, 0.0).astype(BF16))
        both = lax.dot_general(
            jnp.concatenate(pieces, axis=0), slab_weights, contract, preferred_element_type=F32
        )
        for m in range(STEPS - 1):
            at = 2 * m * ROWS
            injslab[m] = both[at : at + ROWS] + both[at + ROWS : at + 2 * ROWS]

    snapshot(0, middle)
    assemble(0, FIRST, middle)
    assemble_slab(0, False)
    for step in range(1, STEPS + 1):
        magnetic_half(0, step, magnetic_inner(step))
        forward_electric(step, electric_inner(step))
    for wait in first_waits:
        wait()
    assemble(0, FIRST, outside)
    assemble_slab(0)

    def magnetic_outer(step):
        magnetic_half(0, step, [i for i in magnetic_planes(step) if i not in magnetic_inner(step)])

    def electric_outer(step):
        forward_electric(step, [i for i in electric_planes(step) if i not in electric_inner(step)])

    for step in (1, 2):
        magnetic_outer(step)
        electric_outer(step)
    second_z()
    edges_, sides_ = relay_slabs(1)
    second_edges += edges_
    second_waits += sides_
    for wait in second_y:
        wait()
    second_waits += relay_corners(FIRST, COMPS)
    group_wait(1, 1, gather2)
    samples = [
        jnp.concatenate([gather2[k][m : m + 1] for k in range(16)], axis=1) for m in range(STEPS)
    ]
    lanes_of = lax.broadcasted_iota(jnp.int32, (nz, nrec), 0)
    at_lane = lanes_of == rec_lane
    inject(0)
    magnetic_outer(3)
    inject(1)
    electric_outer(3)
    inject(2)
    magnetic_outer(4)
    inject(3)
    inject_slab()
    electric_outer(4)

    square = [jnp.zeros((ny, nz), F32)]

    def adjoint_step(step, magnetic_at, electric_at):
        magnetic_half(FIRST, step, magnetic_at)
        electric_half(
            FIRST,
            step,
            electric_at,
            lambda i, at: inj[step - 1, i, at],
            lambda: injslab[step - 1],
        )
        for i in electric_at:
            if i not in middle:
                continue
            k = i - OWNX
            term = None
            for c in range(3):
                product = change[STEPS - step, c, k] * field[FIRST + c, i, own[1], :]
                term = product if term is None else term + product
            value = term if step == 1 else out_ref[k] + term
            if step == STEPS:
                value = -value / medium[0, k]
                square[0] = square[0] + value * value
            out_ref[k] = value

    for wait in second_edges + second_waits + second_leaving:
        wait()
    assemble(FIRST, COMPS, every)
    assemble_slab(1)
    for step in range(1, STEPS + 1):
        adjoint_step(step, magnetic_planes(step), electric_planes(step))
    square = square[0]
    red1[groups[2][0]] = jnp.sum(square, axis=0, keepdims=True)
    group_start(2, 2, red1)
    group_wait(2, 2, red1)
    total = red1[0]
    for k in range(1, 16):
        total = total + red1[k]
    red2[groups[3][0]] = total
    group_start(3, 3, red2)
    group_wait(3, 3, red2)
    total = red2[0]
    for k in range(1, 16):
        total = total + red2[k]
    total = jnp.sum(total, axis=1, keepdims=True)
    cells_in_all = ngx * nx * ngy * ny * ngz * nz
    rms = jnp.sqrt(total / cells_in_all + 1e-06)
    rms_ref[...] = rms
    wide = jnp.broadcast_to(rms, (ny, nz))
    for i in range(nx):
        out_ref[i] = out_ref[i] / wide
    for cond, copy in sends:
        guarded(cond, copy.wait_send)
    group_drain(0, 0, gather1)
    group_drain(1, 1, gather2)
    group_drain(2, 2, red1)
    group_drain(3, 3, red2)


def solution(mesh):
    ngx, ngy, ngz = mesh.shape["gx"], mesh.shape["gy"], mesh.shape["gz"]

    def per_device(
        permittivity,
        loss,
        fwd_electric,
        fwd_magnetic,
        adj_electric,
        adj_magnetic,
        wavelet,
        residuals,
        source_cell,
        receiver_cells,
        start_step,
    ):
        nx, ny, nz = permittivity.shape
        nrec, trace = receiver_cells.shape[0], residuals.shape[1]
        planes = nx + 2 * HALO
        dims = (ngx, ngy, ngz, nx, ny, nz, nrec)
        hbm = pl.BlockSpec(memory_space=pltpu.HBM)
        vmem = pl.BlockSpec(memory_space=pltpu.VMEM)
        direction, rms = pl.pallas_call(
            functools.partial(kernel, dims),
            out_shape=(
                jax.ShapeDtypeStruct((nx, ny, nz), F32),
                jax.ShapeDtypeStruct((1, 1), F32),
            ),
            in_specs=[hbm] * 11,
            out_specs=(vmem, vmem),
            scratch_shapes=[
                pltpu.VMEM((COMPS, planes, 64, nz), F32),
                pltpu.VMEM((2, nx, ny, nz), F32),
                pltpu.VMEM((2, COMPS, nx, HALO, nz), F32),
                pltpu.VMEM((2, COMPS, nx, HALO, nz), F32),
                pltpu.VMEM((2, 2, COMPS, HALO, HALO, nz), F32),
                pltpu.VMEM((nrec // (ngx * ngy * ngz), trace), F32),
                pltpu.VMEM((1, nrec), jnp.int32),
                pltpu.SMEM((trace,), F32),
                pltpu.SMEM((1,), jnp.int32),
                pltpu.SMEM((1,), jnp.int32),
                pltpu.VMEM((4, ny, 128), F32),
                pltpu.VMEM((2, 2, 4, HALO, 128), F32),
                pltpu.VMEM((2, 2, 2, ny, 128), F32),
                pltpu.VMEM((2, 2, 2, 2, HALO, 128), F32),
                pltpu.VMEM((2, 4, ny, 128), F32),
                pltpu.VMEM((2, 2, 4, HALO, 128), F32),
                pltpu.VMEM((2, 2, 2, ny, 128), F32),
                pltpu.VMEM((2, 2, 2, 2, HALO, 128), F32),
                pltpu.VMEM((COMPS, 64, 128), F32),
                pltpu.VMEM((STEPS, 3, nx, ny, nz), F32),
                pltpu.VMEM((STEPS, 3, nx, ny, nz), F32),
                pltpu.VMEM((ROWS, 128), F32),
                pltpu.VMEM((ROWS, 128), F32),
                pltpu.VMEM((ROWS, 128), F32),
                pltpu.VMEM((ROWS, 128), F32),
                pltpu.VMEM(((planes - 2) * ROWS, nrec), BF16),
                pltpu.VMEM((STEPS, planes, ROWS, nz), F32),
                pltpu.VMEM((STEPS - 1, ROWS, 128), F32),
                pltpu.VMEM((16, STEPS, 128), F32),
                pltpu.VMEM((16, STEPS, 128), F32),
                pltpu.VMEM((16, 1, 128), F32),
                pltpu.VMEM((16, 1, 128), F32),
                pltpu.SemaphoreType.DMA((11,)),
                pltpu.SemaphoreType.DMA((59,)),
                pltpu.SemaphoreType.DMA((59,)),
                pltpu.SemaphoreType.DMA((4, 15)),
                pltpu.SemaphoreType.DMA((4, 16)),
            ],
            compiler_params=pltpu.CompilerParams(
                collective_id=0, has_side_effects=True, vmem_limit_bytes=60 * 1024 * 1024
            ),
            name="window",
        )(
            permittivity,
            loss,
            fwd_electric,
            fwd_magnetic,
            adj_electric,
            adj_magnetic,
            residuals,
            receiver_cells.reshape(1, nrec),
            wavelet,
            source_cell,
            start_step,
        )
        return direction, rms.reshape(())

    field_spec = P(None, "gx", "gy", "gz")
    block_spec = P("gx", "gy", "gz")
    return jax.shard_map(
        per_device,
        mesh=mesh,
        in_specs=(
            block_spec,
            block_spec,
            field_spec,
            field_spec,
            field_spec,
            field_spec,
            P(),
            P(("gx", "gy", "gz"), None),
            P(),
            P(),
            P(),
        ),
        out_specs=(block_spec, P()),
        check_vma=False,
    )
```
